16 devices in a mesh: data: 16 (over z, y, x, core).
Axes of the slice: x: 2, y: 2, z: 2, core: 2. Of those that a mesh axis runs over, the one named last changes fastest.
Arguments:
- z_one: bfloat16 [512, 128], P('data')
- z_two: bfloat16 [512, 128], P('data')
- z_small: bfloat16 [6, 512, 128], P(None, 'data')
- protos: bfloat16 [30000, 128], replicated
- live_mask: int32 [512], P('data')
Outputs:
- output 1: float32 [512, 30000], P('data')
- output 2: float32 [512, 30000], P('data')
- output 3: float32 [], replicated
- output 4: float32 [512, 128], P('data')
- output 5: float32 [512, 128], P('data')
- output 6: float32 [6, 512, 128], P(None, 'data')
- output 7: float32 [30000, 128], replicated
All inputs are finite; a program needn't handle non-finite values.
Results may differ from the reference program's by a relative error of at most 0.001.
Values are sent between devices in bfloat16 or wider.
A program may use at most 1 GiB of HBM per device.

```python
import jax
import jax.numpy as jnp
from jax import lax

ROWS_DEV = 32
NUM_GROUPS = 16
NUM_PROTOS = 30000
EMBED_DIM = 128
SMALL_CROPS = 6
ITERS = 3
NUM_ROWS = ROWS_DEV * NUM_GROUPS
EPS = 0.05
TAU = 0.1


def unit_rows(matrix):
    return matrix / jnp.sqrt(jnp.sum(matrix * matrix, axis=-1, keepdims=True))


def draw_mask(mask_key):
    k_count, k_full, k_one, k_perm = jax.random.split(mask_key, 4)
    counts = jax.random.randint(k_count, (NUM_GROUPS,), 1, ROWS_DEV + 1)
    full_grp = jax.random.randint(k_full, (), 0, NUM_GROUPS)
    one_grp = (full_grp + jax.random.randint(k_one, (), 1, NUM_GROUPS)) % NUM_GROUPS
    groups = jnp.arange(NUM_GROUPS)
    counts = jnp.where(groups == full_grp, ROWS_DEV, counts)
    counts = jnp.where(groups == one_grp, 1, counts)
    perm_keys = jax.random.split(k_perm, NUM_GROUPS)
    rank_vals = jax.vmap(lambda perm_key: jax.random.permutation(perm_key, ROWS_DEV))(perm_keys)
    return (rank_vals < counts[:, None]).astype(jnp.int32).reshape(NUM_ROWS)


def draw_views(view_key, protos_f):
    k_pick, k_noise = jax.random.split(view_key)
    win_width = max(NUM_PROTOS // 2, 1)
    offsets = jax.random.randint(k_pick, (NUM_ROWS,), 0, win_width)
    win_start = (jnp.arange(NUM_ROWS) // ROWS_DEV) * NUM_PROTOS // NUM_GROUPS
    pick_ids = (win_start + offsets) % NUM_PROTOS
    centers = protos_f[pick_ids]
    noise_vals = jax.random.normal(k_noise, (2 + SMALL_CROPS, NUM_ROWS, EMBED_DIM), jnp.float32)
    mixed = 0.6 * centers[None] + 0.8 * noise_vals * EMBED_DIM ** -0.5
    return unit_rows(mixed).astype(jnp.bfloat16)


def setup_inputs(seed: int = 0) -> dict:
    root_key = jax.random.key(seed)
    k_proto, k_views, k_mask = jax.random.split(root_key, 3)
    protos_f = unit_rows(jax.random.normal(k_proto, (NUM_PROTOS, EMBED_DIM), jnp.float32))
    crops_all = draw_views(k_views, protos_f)
    return {"z_one": crops_all[0], "z_two": crops_all[1], "z_small": crops_all[2:], "protos": protos_f.astype(jnp.bfloat16), "live_mask": draw_mask(k_mask)}


def sinkhorn(scores, live_f, live_total):
    live_col = live_f[:, None]

    def sk_step(weights, unused):
        col_sum = jnp.sum(weights, axis=0)
        weights = weights / (NUM_PROTOS * col_sum)
        row_sum = jnp.sum(weights, axis=1, keepdims=True)
        row_safe = jnp.where(live_col > 0, row_sum, 1.0)
        weights = weights * (live_col / (live_total * row_safe))
        return weights, None

    weights = lax.scan(sk_step, live_col * jnp.exp(scores / EPS), None, length=ITERS)[0]
    return live_total * weights


def reference(z_one, z_two, z_small, protos, live_mask):
    live_f = live_mask.astype(jnp.float32)
    live_col = live_f[:, None]
    live_total = jnp.sum(live_f)
    pair_count = 2 + 2 * SMALL_CROPS
    grad_scale = 1.0 / (TAU * live_total * pair_count)
    scores_one = jnp.dot(z_one, protos.T, preferred_element_type=jnp.float32)
    scores_two = jnp.dot(z_two, protos.T, preferred_element_type=jnp.float32)
    q_one = sinkhorn(scores_one, live_f, live_total)
    q_two = sinkhorn(scores_two, live_f, live_total)
    q_sum = q_one + q_two
    logp_one = jax.nn.log_softmax(scores_one / TAU, axis=-1)
    logp_two = jax.nn.log_softmax(scores_two / TAU, axis=-1)
    grad_one = ((live_col * jnp.exp(logp_one) - q_two) * grad_scale).astype(jnp.bfloat16)
    grad_two = ((live_col * jnp.exp(logp_two) - q_one) * grad_scale).astype(jnp.bfloat16)

    def small_view(z_crop):
        scores = jnp.dot(z_crop, protos.T, preferred_element_type=jnp.float32)
        logp_crop = jax.nn.log_softmax(scores / TAU, axis=-1)
        grad_crop = ((2.0 * live_col * jnp.exp(logp_crop) - q_sum) * grad_scale).astype(jnp.bfloat16)
        return (jnp.sum(q_sum * logp_crop), jnp.dot(grad_crop, protos, preferred_element_type=jnp.float32), jnp.dot(grad_crop.T, z_crop, preferred_element_type=jnp.float32))

    small_cross, dz_small, small_dc = lax.map(small_view, z_small)
    cross_sum = jnp.sum(q_two * logp_one) + jnp.sum(q_one * logp_two) + jnp.sum(small_cross)
    loss_total = -cross_sum / (live_total * pair_count)
    dz_one = jnp.dot(grad_one, protos, preferred_element_type=jnp.float32)
    dz_two = jnp.dot(grad_two, protos, preferred_element_type=jnp.float32)
    d_protos = jnp.dot(grad_one.T, z_one, preferred_element_type=jnp.float32) + jnp.dot(grad_two.T, z_two, preferred_element_type=jnp.float32) + jnp.sum(small_dc, axis=0)
    return (q_one, q_two, loss_total, dz_one, dz_two, dz_small, d_protos)
```

```python
import functools

import jax
import jax.numpy as jnp
import numpy as np
from jax import lax
from jax.experimental import pallas as pl
from jax.experimental.pallas import tpu as pltpu
from jax.sharding import PartitionSpec as P

TAU = 0.1
LOG2E = 1.4426950408889634
LN2 = 0.6931471805599453
SCALE = LOG2E / TAU
NDEV = 16
ROWS = 32
NS = 512
VIEWS = 8
D = 128
KP = 30000
SH = 1920
KPAD = SH * NDEV
LAST = KP - SH * (NDEV - 1)
CB = 384
NCH = SH // CB
PAIRS = 14.0
LOGICAL = pl.DeviceIdType.LOGICAL
VM = 60 * 1024 * 1024


def dot_nt(a, b):
    return lax.dot_general(a, b, (((1,), (1,)), ((), ())), preferred_element_type=jnp.float32)


def dot_nn(a, b):
    return lax.dot_general(a, b, (((1,), (0,)), ((), ())), preferred_element_type=jnp.float32)


def fold8(x):
    return jnp.sum(x.reshape(x.shape[0] // 8, 8, x.shape[1]), axis=0)


def flip(me, bit):
    return me + bit - 2 * bit * lax.rem(me // bit, 2)


def full_barrier(me):
    barrier = pltpu.get_barrier_semaphore()
    for d in range(1, NDEV):
        pl.semaphore_signal(barrier, inc=1, device_id=lax.rem(me + d, NDEV), device_id_type=LOGICAL)
    pl.semaphore_wait(barrier, NDEV - 1)


def send(src, dst, ssem, rsem, to):
    copy = pltpu.make_async_remote_copy(src_ref=src, dst_ref=dst, send_sem=ssem, recv_sem=rsem,
                                        device_id=to, device_id_type=LOGICAL)
    copy.start()


def drain(ref, sem):
    pltpu.make_async_copy(ref, ref, sem).wait()


def load_shard(me, protos, cs, sem, start):
    @pl.when(me < NDEV - 1)
    def _():
        c = pltpu.make_async_copy(protos.at[pl.ds(pl.multiple_of(me * SH, 8), SH)], cs, sem)
        c.start() if start else c.wait()

    @pl.when(me == NDEV - 1)
    def _():
        c = pltpu.make_async_copy(protos.at[pl.ds(SH * (NDEV - 1), LAST)], cs.at[pl.ds(0, LAST)], sem)
        if start:
            c.start()
            cs[pl.ds(LAST, SH - LAST), :] = jnp.zeros((SH - LAST, D), jnp.bfloat16)
        else:
            c.wait()


def sk_kernel(z1, z2, zs, m8, protos, zall, arow, brow, wall, lout,
              cs, ex, slots, lslots, csem, zsend, zlrecv, zs1recv, zs2send, zs2recv,
              arsend, arrecv, lsend, lrecv, wsend, wrecv):
    me = lax.axis_index("data")
    load_shard(me, protos, cs, csem, True)
    full_barrier(me)
    myrows = pl.ds(pl.multiple_of(me * ROWS, ROWS), ROWS)
    slots[0, me] = m8[...]
    for d in range(1, NDEV):
        to = lax.rem(me + d, NDEV)
        send(m8, slots.at[0, me], arsend.at[0], arrecv.at[0], to)
        send(z1, zall.at[0, myrows], zsend.at[0], zlrecv, to)
        send(z2, zall.at[1, myrows], zsend.at[0], zlrecv, to)
    for d in range(1, NDEV // 2):
        to = lax.rem(me + 2 * d, NDEV)
        send(zs, zall.at[pl.ds(2, 6), myrows], zsend.at[1], zs1recv, to)
    sib = flip(me, 1)
    zall[0, myrows] = z1[...]
    zall[1, myrows] = z2[...]
    zall[pl.ds(2, 6), myrows] = zs[...]
    send(zs, zall.at[pl.ds(2, 6), myrows], zs2send, zs2recv, sib)
    load_shard(me, protos, cs, csem, False)

    def ar_send(t):
        for d in range(1, NDEV):
            send(slots.at[t, me], slots.at[t, me], arsend.at[t], arrecv.at[t], lax.rem(me + d, NDEV))

    def ar_total(t):
        drain(slots.at[t, pl.ds(0, NDEV - 1)], arrecv.at[t])
        tot = slots[t, 0]
        for i in range(1, NDEV):
            tot = tot + slots[t, i]
        return tot

    mask8 = ar_total(0)
    live = jnp.sum(jnp.sum(mask8, axis=1, keepdims=True), axis=0, keepdims=True)
    mrow = jnp.concatenate([mask8[j:j + 1] for j in range(4)], axis=1)
    drain(zall.at[pl.ds(0, 2), pl.ds(0, NS - ROWS)], zlrecv)

    def col_scale(c, b):
        k = me * SH + b * CB + lax.broadcasted_iota(jnp.int32, (CB, 1), 0)
        return jnp.where(k < KP, 1.0 / (KP * c), 0.0)

    zero8 = jnp.zeros((8, NS), jnp.float32)

    def first(b, carry):
        rows = pl.ds(pl.multiple_of(b * CB, CB), CB)
        out = []
        for v in range(2):
            ps, r = carry[2 * v], carry[2 * v + 1]
            p = jnp.exp2(dot_nt(cs[rows], zall[v]) * SCALE)
            ps = ps + fold8(p)
            e = p * p * mrow
            ex[v, rows] = e
            w = col_scale(jnp.sum(e, axis=1, keepdims=True), b)
            r = r + fold8(e * w)
            out += [ps, r]
        return tuple(out)

    def put(t, r1, r2):
        for v, r in enumerate((r1, r2)):
            row = jnp.sum(r, axis=0, keepdims=True)
            for j in range(4):
                slots[t, me, pl.ds(4 * v + j, 1)] = row[:, 128 * j:128 * (j + 1)]

    def scale_rows(tot):
        us = []
        for v in range(2):
            r = jnp.concatenate([tot[4 * v + j:4 * v + j + 1] for j in range(4)], axis=1)
            us.append(mrow / (live * jnp.where(mrow > 0, r, 1.0)))
        return us

    pad = jnp.where(me == NDEV - 1, float(SH - LAST), 0.0)

    def put_lse(v, ps):
        row = jnp.sum(ps, axis=0, keepdims=True) - pad
        for j in range(4):
            lslots[me, pl.ds(4 * v + j, 1)] = row[:, 128 * j:128 * (j + 1)]

    ps1, r1, ps2, r2 = lax.fori_loop(0, NCH, first, (zero8, zero8, zero8, zero8))
    put(1, r1, r2)
    ar_send(1)
    put_lse(0, ps1)
    put_lse(1, ps2)
    drain(zall.at[pl.ds(2, 6), pl.ds(0, 7 * ROWS)], zs1recv)
    for d in range(1, NDEV // 2):
        rows = pl.ds(pl.multiple_of(lax.rem(me + 2 * d, NDEV) * ROWS, ROWS), ROWS)
        send(zall.at[pl.ds(2, 6), rows], zall.at[pl.ds(2, 6), rows], zs2send, zs2recv, sib)
    us = scale_rows(ar_total(1))

    def again(us, last):
        def step(b, carry):
            rows = pl.ds(pl.multiple_of(b * CB, CB), CB)
            out = []
            for v in range(2):
                e = ex[v, rows]
                w = col_scale(jnp.sum(e * us[v], axis=1, keepdims=True), b)
                out.append(carry[v] + fold8(e * w))
                if last:
                    for q in range(CB // 128):
                        wt = jnp.broadcast_to(w[128 * q:128 * (q + 1)], (128, 128)).T
                        wall[me, pl.ds(v, 1), pl.ds(pl.multiple_of(b * CB + 128 * q, 128), 128)] = wt[0:1]
            return tuple(out)
        return step

    r1, r2 = lax.fori_loop(0, NCH, again(us, False), (zero8, zero8))
    put(2, r1, r2)
    ar_send(2)
    drain(zall.at[pl.ds(2, 6), pl.ds(0, 8 * ROWS)], zs2recv)

    def small(i, carry):
        v = 2 + i

        def blk(b, ps):
            rows = pl.ds(pl.multiple_of(b * CB, CB), CB)
            return ps + fold8(jnp.exp2(dot_nt(cs[rows], zall[v]) * SCALE))

        ps = lax.fori_loop(0, NCH, blk, zero8)
        row = jnp.sum(ps, axis=0, keepdims=True) - pad
        for j in range(4):
            lslots[me, pl.ds(4 * v + j, 1)] = row[:, 128 * j:128 * (j + 1)]
        return carry

    lax.fori_loop(0, 6, small, 0)
    us = scale_rows(ar_total(2))
    r1, r2 = lax.fori_loop(0, NCH, again(us, True), (zero8, zero8))
    put(3, r1, r2)
    ar_send(3)
    for d in range(1, NDEV):
        to = lax.rem(me + d, NDEV)
        send(lslots.at[me], lslots.at[me], lsend, lrecv, to)
    for d in range(1, NDEV):
        to = lax.rem(me + d, NDEV)
        send(wall.at[me], wall.at[me], wsend, wrecv, to)
    us = scale_rows(ar_total(3))
    gs = 1.0 / (TAU * PAIRS * live)
    for v in range(2):
        brow[v:v + 1] = gs * live * us[v]
        brow[v + 2:v + 3] = live * us[v]
    brow[4:8] = jnp.zeros((4, NS), jnp.float32)
    drain(lslots.at[pl.ds(0, NDEV - 1)], lrecv)
    tot = lslots[0]
    for i in range(1, NDEV):
        tot = tot + lslots[i]
    inv = 1.0 / tot
    for v in range(VIEWS):
        for j in range(4):
            coef = 1.0 if v < 2 else 2.0
            arow[v:v + 1, 128 * j:128 * (j + 1)] = (coef * gs) * (mask8[j:j + 1] * inv[4 * v + j:4 * v + j + 1])
    weight = jnp.concatenate([mask8[0:4]] * 2 + [2.0 * mask8[0:4]] * 6, axis=0)
    lsum = jnp.sum(jnp.sum(weight * jnp.log(tot), axis=1, keepdims=True), axis=0, keepdims=True)
    lout[0:1] = jnp.broadcast_to(lsum, (1, 128))
    lout[1:2] = jnp.broadcast_to(live, (1, 128))
    lout[2:8] = jnp.zeros((6, 128), jnp.float32)
    drain(wall.at[pl.ds(0, NDEV - 1)], wrecv)
    drain(zall.at[pl.ds(0, 2), pl.ds(0, NS - ROWS)], zsend.at[0])
    drain(zall.at[pl.ds(2, 6), pl.ds(0, 7 * ROWS)], zsend.at[1])
    drain(zall.at[pl.ds(2, 6), pl.ds(0, 8 * ROWS)], zs2send)
    for t in range(4):
        drain(slots.at[t, pl.ds(0, NDEV - 1)], arsend.at[t])
    drain(lslots.at[pl.ds(0, NDEV - 1)], lsend)
    drain(wall.at[pl.ds(0, NDEV - 1)], wsend)


RB = 512
NIT = 15
RPI = KPAD // RB // NIT


def grad_kernel(zall, arow, brow, wall, lout, z1, z2, zs, protos, dc, dz1, dz2, dzs, loss,
                ca, gt, zl, cols, acc, lslots, csem, ssem, r1, r2, r3, rs, lsend, lrecv):
    me = lax.axis_index("data")
    cc = pltpu.make_async_copy(protos, ca.at[pl.ds(0, KP)], csem)
    cc.start()
    ca[pl.ds(KP, KPAD - KP), :] = jnp.zeros((KPAD - KP, D), jnp.bfloat16)
    full_barrier(me)
    dims = (flip(me, 2), flip(me, 4), flip(me, 8))
    sib = flip(me, 1)
    zl[pl.ds(0, ROWS)] = z1[...]
    zl[pl.ds(ROWS, ROWS)] = z2[...]
    zl[pl.ds(2 * ROWS, 6 * ROWS)] = zs[...].reshape(6 * ROWS, D)
    tile = pl.ds(pl.multiple_of((me // 4) * 128, 128), 128)
    cols[0] = jnp.broadcast_to(arow[:, tile].T, (128, 8))
    cols[1] = jnp.broadcast_to(brow[:, tile].T, (128, 8))
    acc[...] = jnp.zeros_like(acc)
    mine = pl.ds(pl.multiple_of(lax.rem(me, 4) * ROWS, ROWS), ROWS)
    ac = cols[0, mine]
    bc = cols[1, mine]
    cc.wait()

    def piece(owner, t, a):
        return dc.at[pl.ds(pl.multiple_of(owner * SH + t * CB + a * 128, 128), 128)]

    def push(owner, t, a, to, rsem):
        ref = piece(owner, t, a)
        send(ref, ref, ssem.at[t, a], rsem.at[t, a], to)

    def chunk(owner, t):
        base = pl.multiple_of(owner * SH + t * CB, 128)
        c = ca[pl.ds(base, CB)]
        wc = []
        for v in range(2):
            parts = []
            for q in range(CB // 128):
                off = pl.multiple_of(t * CB + q * 128, 128)
                row = wall[owner, pl.ds(v, 1), pl.ds(off, 128)]
                parts.append(jnp.broadcast_to(row, (128, 128)).T)
            wc.append(jnp.concatenate(parts, axis=0))

        def nblk(nb, carry):
            ln = pl.ds(pl.multiple_of(nb * 256, 256), 256)
            s = [dot_nt(c, zall[v, ln]) for v in range(VIEWS)]
            av = [arow[v:v + 1, ln] for v in range(VIEWS)]
            bv = [brow[v:v + 1, ln] for v in range(2)]
            for q in range(CB // 64):
                sl = slice(64 * q, 64 * (q + 1))
                w0 = jnp.concatenate([wc[0][sl], wc[0][sl]], axis=1)
                w1 = jnp.concatenate([wc[1][sl], wc[1][sl]], axis=1)
                p0 = jnp.exp2(s[0][sl] * SCALE)
                p1 = jnp.exp2(s[1][sl] * SCALE)
                x0 = (p0 * p0) * bv[0] * w0
                x1 = (p1 * p1) * bv[1] * w1
                xs = x0 + x1
                gs = [p0 * av[0] - x1, p1 * av[1] - x0]
                for v in range(2, VIEWS):
                    gs.append(jnp.exp2(s[v][sl] * SCALE) * av[v] - xs)
                for v in range(VIEWS):
                    gt[pl.ds(64 * q, 64), pl.ds(pl.multiple_of(v * NS + nb * 256, 256), 256)] = gs[v].astype(jnp.bfloat16)
            return carry

        lax.fori_loop(0, 2, nblk, 0)
        dc[pl.ds(base, CB)] = dot_nn(gt[...], zall[...].reshape(VIEWS * NS, D))

    def row_block(j, carry):
        base = pl.multiple_of(j * RB, RB)
        c = ca[pl.ds(base, RB)]
        s = dot_nt(zl[...], c) * SCALE
        sh = j // (SH // RB) if SH % RB == 0 else 0
        return carry, s, sh

    def rows_part(i):
        for h in range(RPI):
            base = pl.multiple_of(i * (RPI * RB) + h * RB, RB)
            c = ca[pl.ds(base, RB)]
            s = dot_nt(zl[...], c) * SCALE
            wr = []
            for v in range(2):
                parts = []
                for q in range(RB // 128):
                    b = i * (RPI * RB // 128) + h * (RB // 128) + q
                    parts.append(wall[b // (SH // 128), pl.ds(v, 1), pl.ds(pl.multiple_of(lax.rem(b, SH // 128) * 128, 128), 128)])
                wr.append(jnp.concatenate(parts, axis=1))
            sv = [s[ROWS * v:ROWS * (v + 1)] for v in range(VIEWS)]
            p0 = jnp.exp2(sv[0])
            p1 = jnp.exp2(sv[1])
            x0 = (p0 * p0) * bc[:, 0:1] * wr[0]
            x1 = (p1 * p1) * bc[:, 1:2] * wr[1]
            xs = x0 + x1
            gs = [p0 * ac[:, 0:1] - x1, p1 * ac[:, 1:2] - x0]
            ssum = sv[2]
            for v in range(3, VIEWS):
                ssum = ssum + sv[v]
            for v in range(2, VIEWS):
                gs.append(jnp.exp2(sv[v]) * ac[:, v:v + 1] - xs)
            g = jnp.concatenate([x.astype(jnp.bfloat16) for x in gs], axis=0)
            acc[pl.ds(0, VIEWS * ROWS)] += dot_nn(g, c)
            ls = x1 * sv[0] + x0 * sv[1] + xs * ssum
            part = ls[:, 0:128]
            for q in range(1, RB // 128):
                part = part + ls[:, 128 * q:128 * (q + 1)]
            acc[pl.ds(VIEWS * ROWS, ROWS)] += part

    def order(a):
        return dims[a], dims[(a + 1) % 3], dims[(a + 2) % 3]

    def own(t):
        for a in range(3):
            d0, d1, d2 = order(a)
            push(me, t, a, d0, r1)
            push(me, t, a, d1, r2)
            push(me, t, a, d2, r3)
            push(me, t, a, sib, rs)

    def serve1(t):
        for a in range(3):
            d0, d1, d2 = order(a)
            drain(piece(me, t, a), r1.at[t, a])
            push(d0, t, a, d1, r2)
            push(d0, t, a, d2, r3)
            push(d0, t, a, sib, rs)

    def serve2(t):
        for a in range(3):
            d0, d1, d2 = order(a)
            drain(dc.at[pl.ds(0, 256)], r2.at[t, a])
            d10 = d0 + d1 - me
            for o in (d1, d10):
                push(o, t, a, d2, r3)
                push(o, t, a, sib, rs)

    def serve3(t):
        for a in range(3):
            d0, d1, d2 = order(a)
            drain(dc.at[pl.ds(0, 512)], r3.at[t, a])
            for o in (d2, d2 + d0 - me, d2 + d1 - me, d2 + d1 + d0 - 2 * me):
                push(o, t, a, sib, rs)

    def main(it, carry):
        @pl.when(it < NCH)
        def _():
            chunk(me, it)
            own(it)

        rows_part(it)

        @pl.when(jnp.logical_and(it >= 2, it < 2 + NCH))
        def _():
            serve1(it - 2)

        @pl.when(jnp.logical_and(it >= 6, it < 6 + NCH))
        def _():
            serve2(it - 6)

        @pl.when(jnp.logical_and(it >= 9, it < 9 + NCH))
        def _():
            serve3(it - 9)

        return carry

    lax.fori_loop(0, NIT, main, 0)

    total = jnp.sum(jnp.sum(acc[pl.ds(VIEWS * ROWS, ROWS)], axis=1, keepdims=True), axis=0, keepdims=True)
    lslots[me] = jnp.broadcast_to(total, (8, 128))
    for d in range(1, NDEV):
        send(lslots.at[me], lslots.at[me], lsend, lrecv, lax.rem(me + d, NDEV))
    dz1[...] = acc[pl.ds(0, ROWS)]
    dz2[...] = acc[pl.ds(ROWS, ROWS)]
    dzs[...] = acc[pl.ds(2 * ROWS, 6 * ROWS)].reshape(6, ROWS, D)
    drain(lslots.at[pl.ds(0, NDEV - 1)], lrecv)
    tot = lslots[0]
    for i in range(1, NDEV):
        tot = tot + lslots[i]
    live = lout[1:2]
    cross = tot[0:1] * (LN2 * TAU * PAIRS) * live - lout[0:1]
    loss[...] = jnp.broadcast_to(-cross / (live * PAIRS), (8, 128))
    drain(lslots.at[pl.ds(0, NDEV - 1)], lsend)

    def finish(t, carry):
        for a in range(3):
            drain(dc.at[pl.ds(0, 8 * 128)], rs.at[t, a])
            drain(dc.at[pl.ds(0, 15 * 128)], ssem.at[t, a])
        return carry

    lax.fori_loop(0, NCH, finish, 0)


QB = 2048


def q_kernel(z1, z2, bcol, c, w, q1, q2):
    for v, (z, q) in enumerate(((z1, q1), (z2, q2))):
        p = jnp.exp2(dot_nt(z[...], c[...]) * SCALE)
        q[...] = (p * p) * bcol[:, v:v + 1] * w[v:v + 1]


def local_step(z_one, z_two, z_small, protos, live_mask):
    me = lax.axis_index("data")
    live_f = live_mask.astype(jnp.float32)
    pos = jnp.arange(1024, dtype=jnp.int32).reshape(8, 128) // ROWS
    m8 = jnp.where(pos == me, jnp.tile(live_f, 4)[None, :], 0.0)
    f32 = jnp.float32
    vmem = pl.BlockSpec(memory_space=pltpu.VMEM)
    anym = pl.BlockSpec(memory_space=pl.ANY)
    dma = pltpu.SemaphoreType.DMA
    zall, arow, brow, wall, lout = pl.pallas_call(
        sk_kernel,
        out_shape=[jax.ShapeDtypeStruct((VIEWS, NS, D), jnp.bfloat16), jax.ShapeDtypeStruct((8, NS), f32),
                   jax.ShapeDtypeStruct((8, NS), f32), jax.ShapeDtypeStruct((NDEV, 2, SH), f32),
                   jax.ShapeDtypeStruct((8, 128), f32)],
        in_specs=[vmem, vmem, vmem, vmem, anym],
        out_specs=[vmem] * 5,
        scratch_shapes=[pltpu.VMEM((SH, D), jnp.bfloat16), pltpu.VMEM((2, SH, NS), f32),
                        pltpu.VMEM((4, NDEV, 8, 128), f32), pltpu.VMEM((NDEV, 32, 128), f32),
                        dma, dma((2,)), dma, dma, dma, dma, dma((4,)), dma((4,)), dma, dma, dma, dma],
        compiler_params=pltpu.CompilerParams(collective_id=0, has_side_effects=True, vmem_limit_bytes=VM),
        name="sinkhorn",
    )(z_one, z_two, z_small, m8, protos)

    dcp, dz1, dz2, dzs, loss = pl.pallas_call(
        grad_kernel,
        out_shape=[jax.ShapeDtypeStruct((KPAD, D), f32), jax.ShapeDtypeStruct((ROWS, D), f32),
                   jax.ShapeDtypeStruct((ROWS, D), f32), jax.ShapeDtypeStruct((6, ROWS, D), f32),
                   jax.ShapeDtypeStruct((8, 128), f32)],
        in_specs=[vmem] * 8 + [anym],
        out_specs=[vmem] * 5,
        scratch_shapes=[pltpu.VMEM((KPAD, D), jnp.bfloat16), pltpu.VMEM((CB, VIEWS * NS), jnp.bfloat16),
                        pltpu.VMEM((VIEWS * ROWS, D), jnp.bfloat16), pltpu.VMEM((2, 128, 8), f32),
                        pltpu.VMEM((VIEWS * ROWS + ROWS, D), f32), pltpu.VMEM((NDEV, 8, 128), f32),
                        dma, dma((NCH, 3)), dma((NCH, 3)), dma((NCH, 3)), dma((NCH, 3)), dma((NCH, 3)), dma, dma],
        compiler_params=pltpu.CompilerParams(collective_id=1, has_side_effects=True, vmem_limit_bytes=VM),
        name="grads",
    )(zall, arow, brow, wall, lout, z_one, z_two, z_small, protos)

    bcol = lax.dynamic_slice(brow, (2, me * ROWS), (2, ROWS)).T
    w2 = jnp.swapaxes(wall, 0, 1).reshape(2, KPAD)
    q1, q2 = pl.pallas_call(
        q_kernel,
        grid=(pl.cdiv(KP, QB),),
        out_shape=[jax.ShapeDtypeStruct((ROWS, KP), f32)] * 2,
        in_specs=[pl.BlockSpec((ROWS, D), lambda j: (0, 0)), pl.BlockSpec((ROWS, D), lambda j: (0, 0)),
                  pl.BlockSpec((ROWS, 2), lambda j: (0, 0)), pl.BlockSpec((QB, D), lambda j: (j, 0)),
                  pl.BlockSpec((2, QB), lambda j: (0, j))],
        out_specs=[pl.BlockSpec((ROWS, QB), lambda j: (0, j))] * 2,
        compiler_params=pltpu.CompilerParams(dimension_semantics=("arbitrary",)),
        name="codes",
    )(z_one, z_two, bcol, protos, w2)
    return q1, q2, loss[0, 0], dz1, dz2, dzs, dcp[:KP]


def solution(mesh):
    row_spec = P("data", None)
    crop_spec = P(None, "data", None)
    return jax.shard_map(local_step, mesh=mesh,
                         in_specs=(row_spec, row_spec, crop_spec, P(None, None), P("data")),
                         out_specs=(row_spec, row_spec, P(), row_spec, row_spec, crop_spec, P(None, None)),
                         check_vma=False)
```

```python
import jax
import jax.numpy as jnp
from jax import lax
from jax.experimental import pallas as pl
from jax.experimental.pallas import tpu as pltpu
from jax.sharding import PartitionSpec as P

TAU = 0.1
LOG2E = 1.4426950408889634
LN2 = 0.6931471805599453
SCALE = LOG2E / TAU
NDEV = 16
ROWS = 32
NS = 512
VIEWS = 8
D = 128
KP = 30000
SH = 1920
KPAD = SH * NDEV
LAST = KP - SH * (NDEV - 1)
CB = 384
NCH = SH // CB
PAIRS = 14.0
LOGICAL = pl.DeviceIdType.LOGICAL
VM = 36 * 1024 * 1024
RB = 512
NROW = 15
RPI = KPAD // RB // NROW
LAG2, LAG3 = 3, 7
NIT = 2 * NCH + LAG3
STEPS = 2 * NCH


def dot_nt(a, b):
    return lax.dot_general(a, b, (((1,), (1,)), ((), ())), preferred_element_type=jnp.float32)


def dot_nn(a, b):
    return lax.dot_general(a, b, (((1,), (0,)), ((), ())), preferred_element_type=jnp.float32)


def fold8(x):
    return jnp.sum(x.reshape(x.shape[0] // 8, 8, x.shape[1]), axis=0)


def flip(me, bit):
    return me + bit - 2 * bit * lax.rem(me // bit, 2)


def full_barrier(me):
    barrier = pltpu.get_barrier_semaphore()
    for d in range(1, NDEV):
        pl.semaphore_signal(barrier, inc=1, device_id=lax.rem(me + d, NDEV), device_id_type=LOGICAL)
    pl.semaphore_wait(barrier, NDEV - 1)


def send(src, dst, ssem, rsem, to):
    copy = pltpu.make_async_remote_copy(src_ref=src, dst_ref=dst, send_sem=ssem, recv_sem=rsem,
                                        device_id=to, device_id_type=LOGICAL)
    copy.start()


def drain(ref, sem):
    pltpu.make_async_copy(ref, ref, sem).wait()


def kernel(z1, z2, zs, mpad, protos, dc, q1, q2, dz, loss,
           ca, ex, slots, lslots, wall, zall, arow, brow, gt, zl, cols, acc,
           csem, zsend, zlrecv, zs1recv, zs2send, zs2recv, arsend, arrecv, lsend, lrecv, wsend, wrecv,
           ssem, r2, r3, rs):
    me = lax.axis_index("data")
    cc = pltpu.make_async_copy(protos, ca.at[pl.ds(0, KP)], csem)
    cc.start()
    ca[pl.ds(KP, KPAD - KP), :] = jnp.zeros((KPAD - KP, D), jnp.bfloat16)
    dims = (flip(me, 2), flip(me, 4), flip(me, 8))
    sib = flip(me, 1)
    here = lax.broadcasted_iota(jnp.int32, (8, 128), 0) == me // 4
    slots[0, me] = jnp.where(here, pltpu.roll(mpad[...], ROWS * lax.rem(me, 4), 1), 0.0)
    with jax.named_scope("barrier"):
        full_barrier(me)
    myrows = pl.ds(pl.multiple_of(me * ROWS, ROWS), ROWS)

    def ar_send(t):
        for d in range(1, NDEV):
            send(slots.at[t, me], slots.at[t, me], arsend.at[t], arrecv.at[t], lax.rem(me + d, NDEV))

    def ar_total(t):
        drain(slots.at[t, pl.ds(0, NDEV - 1)], arrecv.at[t])
        tot = slots[t, 0]
        for i in range(1, NDEV):
            tot = tot + slots[t, i]
        return tot

    for d in range(1, NDEV):
        to = lax.rem(me + d, NDEV)
        send(z1, zall.at[0, myrows], zsend.at[0], zlrecv, to)
        send(z2, zall.at[1, myrows], zsend.at[0], zlrecv, to)
    ar_send(0)
    for d in range(1, NDEV // 2):
        send(zs, zall.at[pl.ds(2, 6), myrows], zsend.at[1], zs1recv, lax.rem(me + 2 * d, NDEV))
    zall[0, myrows] = z1[...]
    zall[1, myrows] = z2[...]
    zall[pl.ds(2, 6), myrows] = zs[...]
    send(zs, zall.at[pl.ds(2, 6), myrows], zs2send, zs2recv, sib)
    zl[pl.ds(0, ROWS)] = z1[...]
    zl[pl.ds(ROWS, ROWS)] = z2[...]
    zl[pl.ds(2 * ROWS, 6 * ROWS)] = zs[...].reshape(6 * ROWS, D)
    acc[...] = jnp.zeros_like(acc)
    cc.wait()
    with jax.named_scope("mask"):
        mask8 = ar_total(0)
    live = jnp.sum(jnp.sum(mask8, axis=1, keepdims=True), axis=0, keepdims=True)
    mrow = jnp.concatenate([mask8[j:j + 1] for j in range(4)], axis=1)
    with jax.named_scope("zlarge"):
        drain(zall.at[pl.ds(0, 2), pl.ds(0, NS - ROWS)], zlrecv)

    def shard(b):
        return ca[pl.ds(pl.multiple_of(me * SH + b * CB, 128), CB)]

    def col_scale(c, b):
        k = me * SH + b * CB + lax.broadcasted_iota(jnp.int32, (CB, 1), 0)
        return jnp.where(k < KP, 1.0 / (KP * c), 0.0)

    zero8 = jnp.zeros((8, NS), jnp.float32)

    def first(b, carry):
        rows = pl.ds(pl.multiple_of(b * CB, CB), CB)
        out = []
        for v in range(2):
            ps, r = carry[2 * v], carry[2 * v + 1]
            p = jnp.exp2(dot_nt(shard(b), zall[v]) * SCALE)
            ps = ps + fold8(p)
            e = p * p * mrow
            ex[v, rows] = e
            w = col_scale(jnp.sum(e, axis=1, keepdims=True), b)
            r = r + fold8(e * w)
            out += [ps, r]
        return tuple(out)

    def put(t, r1, r2):
        for v, r in enumerate((r1, r2)):
            row = jnp.sum(r, axis=0, keepdims=True)
            for j in range(4):
                slots[t, me, pl.ds(4 * v + j, 1)] = row[:, 128 * j:128 * (j + 1)]

    def scale_rows(tot):
        us = []
        for v in range(2):
            r = jnp.concatenate([tot[4 * v + j:4 * v + j + 1] for j in range(4)], axis=1)
            us.append(mrow / (live * jnp.where(mrow > 0, r, 1.0)))
        return us

    pad = jnp.where(me == NDEV - 1, float(SH - LAST), 0.0)

    def put_lse(v, ps):
        row = jnp.sum(ps, axis=0, keepdims=True) - pad
        for j in range(4):
            lslots[me, pl.ds(4 * v + j, 1)] = row[:, 128 * j:128 * (j + 1)]

    with jax.named_scope("first"):
        ps1, r1, ps2, rr2 = lax.fori_loop(0, NCH, first, (zero8, zero8, zero8, zero8))
        put(1, r1, rr2)
        ar_send(1)
    put_lse(0, ps1)
    put_lse(1, ps2)
    with jax.named_scope("zsmall1"):
        drain(zall.at[pl.ds(2, 6), pl.ds(0, 7 * ROWS)], zs1recv)
    for d in range(1, NDEV // 2):
        rows = pl.ds(pl.multiple_of(lax.rem(me + 2 * d, NDEV) * ROWS, ROWS), ROWS)
        send(zall.at[pl.ds(2, 6), rows], zall.at[pl.ds(2, 6), rows], zs2send, zs2recv, sib)
    with jax.named_scope("ar1"):
        us = scale_rows(ar_total(1))

    def again(us, last):
        def step(b, carry):
            rows = pl.ds(pl.multiple_of(b * CB, CB), CB)
            out = []
            for v in range(2):
                e = ex[v, rows]
                w = col_scale(jnp.sum(e * us[v], axis=1, keepdims=True), b)
                out.append(carry[v] + fold8(e * w))
                if last:
                    for q in range(CB // 128):
                        wt = jnp.broadcast_to(w[128 * q:128 * (q + 1)], (128, 128)).T
                        wall[me, pl.ds(v, 1), pl.ds(pl.multiple_of(b * CB + 128 * q, 128), 128)] = wt[0:1]
            return tuple(out)
        return step

    with jax.named_scope("again2"):
        r1, rr2 = lax.fori_loop(0, NCH, again(us, False), (zero8, zero8))
        put(2, r1, rr2)
        ar_send(2)
    with jax.named_scope("zsmall2"):
        drain(zall.at[pl.ds(2, 6), pl.ds(0, 8 * ROWS)], zs2recv)

    def small(i, carry):
        v = 2 + i

        def blk(b, ps):
            return ps + fold8(jnp.exp2(dot_nt(shard(b), zall[v]) * SCALE))

        put_lse(v, lax.fori_loop(0, NCH, blk, zero8))
        return carry

    with jax.named_scope("small"):
        lax.fori_loop(0, 6, small, 0)
        for d in range(1, NDEV):
            send(lslots.at[me], lslots.at[me], lsend, lrecv, lax.rem(me + d, NDEV))
    with jax.named_scope("ar2"):
        us = scale_rows(ar_total(2))
    with jax.named_scope("again3"):
        r1, rr2 = lax.fori_loop(0, NCH, again(us, True), (zero8, zero8))
        put(3, r1, rr2)
        ar_send(3)
        for d in range(1, NDEV):
            send(wall.at[me], wall.at[me], wsend, wrecv, lax.rem(me + d, NDEV))
    gsc = 1.0 / (TAU * PAIRS * live)
    with jax.named_scope("lse"):
        drain(lslots.at[pl.ds(0, NDEV - 1)], lrecv)
        tot = lslots[0]
        for i in range(1, NDEV):
            tot = tot + lslots[i]
        inv = 1.0 / tot
        for v in range(VIEWS):
            for j in range(4):
                coef = 1.0 if v < 2 else 2.0
                arow[v:v + 1, 128 * j:128 * (j + 1)] = (coef * gsc) * (mask8[j:j + 1] * inv[4 * v + j:4 * v + j + 1])
        weight = jnp.concatenate([mask8[0:4]] * 2 + [2.0 * mask8[0:4]] * 6, axis=0)
        lsum = jnp.sum(jnp.sum(weight * jnp.log(tot), axis=1, keepdims=True), axis=0, keepdims=True)
    with jax.named_scope("ar3"):
        us = scale_rows(ar_total(3))
    for v in range(2):
        brow[v:v + 1] = live * us[v]
    brow[2:8] = jnp.zeros((6, NS), jnp.float32)
    tile = pl.ds(pl.multiple_of((me // 4) * 128, 128), 128)
    cols[0] = arow[:, tile].T
    cols[1] = brow[:, tile].T
    mine = pl.ds(pl.multiple_of(lax.rem(me, 4) * ROWS, ROWS), ROWS)

    def piece_row(owner, t, a):
        return pl.multiple_of(owner * SH + t * CB + a * 128, 128)

    def push(owner, it, a, to, rsem):
        ref = dc.at[pl.ds(piece_row(owner, it // 2, a), 128)]
        send(ref, ref, ssem.at[it, a], rsem.at[it, a], to)

    def order(a):
        return dims[a], dims[(a + 1) % 3], dims[(a + 2) % 3]

    def owner_of(holder, d0, it):
        return holder + lax.rem(it, 2) * (d0 - me)

    def chunk(it):
        t = it // 2
        owners = [owner_of(me, dims[a], it) for a in range(3)]
        c = jnp.concatenate([ca[pl.ds(piece_row(owners[a], t, a), 128)] for a in range(3)], axis=0)
        wc = []
        for v in range(2):
            parts = []
            for a in range(3):
                off = pl.multiple_of(t * CB + a * 128, 128)
                row = wall[owners[a], pl.ds(v, 1), pl.ds(off, 128)] * gsc
                parts.append(jnp.broadcast_to(row, (128, 128)).T)
            wc.append(jnp.concatenate(parts, axis=0))

        def nblk(nb, carry):
            ln = pl.ds(pl.multiple_of(nb * 256, 256), 256)
            s = [dot_nt(c, zall[v, ln]) for v in range(VIEWS)]
            av = [arow[v:v + 1, ln] for v in range(VIEWS)]
            bv = [brow[v:v + 1, ln] for v in range(2)]
            for q in range(CB // 64):
                sl = slice(64 * q, 64 * (q + 1))
                w0 = jnp.concatenate([wc[0][sl], wc[0][sl]], axis=1)
                w1 = jnp.concatenate([wc[1][sl], wc[1][sl]], axis=1)
                p0 = jnp.exp2(s[0][sl] * SCALE)
                p1 = jnp.exp2(s[1][sl] * SCALE)
                x0 = (p0 * p0) * bv[0] * w0
                x1 = (p1 * p1) * bv[1] * w1
                xs = x0 + x1
                gs = [p0 * av[0] - x1, p1 * av[1] - x0]
                for v in range(2, VIEWS):
                    gs.append(jnp.exp2(s[v][sl] * SCALE) * av[v] - xs)
                for v in range(VIEWS):
                    gt[pl.ds(64 * q, 64), pl.ds(pl.multiple_of(v * NS + nb * 256, 256), 256)] = gs[v].astype(jnp.bfloat16)
            return carry

        lax.fori_loop(0, 2, nblk, 0)
        res = dot_nn(gt[...], zall[...].reshape(VIEWS * NS, D))
        for a in range(3):
            dc[pl.ds(piece_row(owners[a], t, a), 128)] = res[128 * a:128 * (a + 1)]

    def rows_part(i):
        ac = cols[0, mine]
        bc = cols[1, mine]
        for h in range(RPI):
            jb = i * RPI + h
            c = ca[pl.ds(pl.multiple_of(jb * RB, RB), RB)]
            s = dot_nt(zl[...], c) * SCALE
            wr = []
            for v in range(2):
                parts = []
                for q in range(RB // 128):
                    b = jb * (RB // 128) + q
                    parts.append(wall[b // (SH // 128), pl.ds(v, 1), pl.ds(pl.multiple_of(lax.rem(b, SH // 128) * 128, 128), 128)])
                wr.append(jnp.concatenate(parts, axis=1))
            sv = [s[ROWS * v:ROWS * (v + 1)] for v in range(VIEWS)]
            p0 = jnp.exp2(sv[0])
            p1 = jnp.exp2(sv[1])
            o0 = (p0 * p0) * bc[:, 0:1] * wr[0]
            o1 = (p1 * p1) * bc[:, 1:2] * wr[1]

            q1[:, pl.ds(pl.multiple_of(jb * RB, RB), RB)] = o0
            q2[:, pl.ds(pl.multiple_of(jb * RB, RB), RB)] = o1
            x0 = o0 * gsc
            x1 = o1 * gsc
            xs = x0 + x1
            gs = [p0 * ac[:, 0:1] - x1, p1 * ac[:, 1:2] - x0]
            ssum = sv[2]
            for v in range(3, VIEWS):
                ssum = ssum + sv[v]
            for v in range(2, VIEWS):
                gs.append(jnp.exp2(sv[v]) * ac[:, v:v + 1] - xs)
            g = jnp.concatenate([x.astype(jnp.bfloat16) for x in gs], axis=0)
            acc[pl.ds(0, VIEWS * ROWS)] += dot_nn(g, c)
            ls = x1 * sv[0] + x0 * sv[1] + xs * ssum
            part = ls[:, 0:128]
            for q in range(1, RB // 128):
                part = part + ls[:, 128 * q:128 * (q + 1)]
            acc[pl.ds(VIEWS * ROWS, ROWS)] += part

    def own(it):
        for a in range(3):
            d0, d1, d2 = order(a)
            o = owner_of(me, d0, it)
            push(o, it, a, d1, r2)
            push(o, it, a, d2, r3)
            push(o, it, a, sib, rs)

    def serve2(it):
        for a in range(3):
            d0, d1, d2 = order(a)
            drain(dc.at[pl.ds(0, 128)], r2.at[it, a])
            o = owner_of(d1, d0, it)
            push(o, it, a, d2, r3)
            push(o, it, a, sib, rs)

    def serve3(it):
        for a in range(3):
            d0, d1, d2 = order(a)
            drain(dc.at[pl.ds(0, 256)], r3.at[it, a])
            for holder in (d2, d2 + d1 - me):
                push(owner_of(holder, d0, it), it, a, sib, rs)

    def main(it, carry):
        @pl.when(it < STEPS)
        def _():
            with jax.named_scope("chunk"):
                chunk(it)
            own(it)

        @pl.when(it == 0)
        def _():
            with jax.named_scope("wait_w"):
                drain(wall.at[pl.ds(0, NDEV - 1)], wrecv)

        @pl.when(jnp.logical_and(it >= LAG2, it < LAG2 + STEPS))
        def _():
            with jax.named_scope("serve2"):
                serve2(it - LAG2)

        @pl.when(it < NROW)
        def _():
            with jax.named_scope("rows"):
                rows_part(it)

        @pl.when(it >= LAG3)
        def _():
            with jax.named_scope("serve3"):
                serve3(it - LAG3)

        return carry

    lax.fori_loop(0, NIT, main, 0)

    total = jnp.sum(jnp.sum(acc[pl.ds(VIEWS * ROWS, ROWS)], axis=1, keepdims=True), axis=0, keepdims=True)
    slots[4, me] = jnp.broadcast_to(total, (8, 128))
    ar_send(4)
    dz[...] = acc[pl.ds(0, VIEWS * ROWS)].reshape(VIEWS, ROWS, D)
    with jax.named_scope("loss"):
        tot = ar_total(4)
    cross = tot[0:1, 0:1] * (LN2 * TAU * PAIRS) * live - lsum
    loss[...] = jnp.broadcast_to(-cross / (live * PAIRS), (8, 128))

    def finish(it, carry):
        for a in range(3):
            drain(dc.at[pl.ds(0, 4 * 128)], rs.at[it, a])
            drain(dc.at[pl.ds(0, 7 * 128)], ssem.at[it, a])
        return carry

    with jax.named_scope("finish"):
        lax.fori_loop(0, STEPS, finish, 0)
    drain(zall.at[pl.ds(0, 2), pl.ds(0, NS - ROWS)], zsend.at[0])
    drain(zall.at[pl.ds(2, 6), pl.ds(0, 7 * ROWS)], zsend.at[1])
    drain(zall.at[pl.ds(2, 6), pl.ds(0, 8 * ROWS)], zs2send)
    for t in range(5):
        drain(slots.at[t, pl.ds(0, NDEV - 1)], arsend.at[t])
    drain(lslots.at[pl.ds(0, NDEV - 1)], lsend)
    drain(wall.at[pl.ds(0, NDEV - 1)], wsend)


def local_step(z_one, z_two, z_small, protos, live_mask):
    mpad = jnp.broadcast_to(jnp.pad(live_mask.astype(jnp.float32), (0, 128 - ROWS))[None, :], (8, 128))
    f32 = jnp.float32
    bf16 = jnp.bfloat16
    vmem = pl.BlockSpec(memory_space=pltpu.VMEM)
    anym = pl.BlockSpec(memory_space=pl.ANY)
    dma = pltpu.SemaphoreType.DMA
    vm = pltpu.VMEM
    dc, q1, q2, dz, loss = pl.pallas_call(
        kernel,
        out_shape=[vm((KPAD, D), f32), vm((ROWS, KPAD), f32), vm((ROWS, KPAD), f32),
                   vm((VIEWS, ROWS, D), f32), vm((8, 128), f32)],
        in_specs=[vmem] * 4 + [anym],
        out_specs=[vmem] * 5,
        scratch_shapes=[vm((KPAD, D), bf16), vm((2, SH, NS), f32), vm((5, NDEV, 8, 128), f32), vm((NDEV, 32, 128), f32),
                        vm((NDEV, 2, SH), f32), vm((VIEWS, NS, D), bf16), vm((8, NS), f32), vm((8, NS), f32),
                        vm((CB, VIEWS * NS), bf16), vm((VIEWS * ROWS, D), bf16), vm((2, 128, 8), f32),
                        vm((VIEWS * ROWS + ROWS, D), f32),
                        dma, dma((2,)), dma, dma, dma, dma, dma((5,)), dma((5,)), dma, dma, dma, dma,
                        dma((STEPS, 3)), dma((STEPS, 3)), dma((STEPS, 3)), dma((STEPS, 3))],
        compiler_params=pltpu.CompilerParams(collective_id=0, has_side_effects=True, vmem_limit_bytes=VM),
        name="step",
    )(z_one, z_two, z_small, mpad, protos)
    return q1[:, :KP], q2[:, :KP], loss[0, 0], dz[0], dz[1], dz[2:], dc[:KP]


def solution(mesh):
    row_spec = P("data", None)
    crop_spec = P(None, "data", None)
    return jax.shard_map(local_step, mesh=mesh,
                         in_specs=(row_spec, row_spec, crop_spec, P(None, None), P("data")),
                         out_specs=(row_spec, row_spec, P(), row_spec, row_spec, crop_spec, P(None, None)),
                         check_vma=False)
```

```python
import jax
import jax.numpy as jnp
from jax import lax
from jax.experimental import pallas as pl
from jax.experimental.pallas import tpu as pltpu
from jax.sharding import PartitionSpec as P

TAU = 0.1
LOG2E = 1.4426950408889634
LN2 = 0.6931471805599453
SCALE = LOG2E / TAU
NDEV = 16
ROWS = 32
NS = 512
VIEWS = 8
D = 128
KP = 30000
SH = 1920
KPAD = SH * NDEV
LAST = KP - SH * (NDEV - 1)
CB = 384
NCH = SH // CB
PAIRS = 14.0
LOGICAL = pl.DeviceIdType.LOGICAL
VM = 36 * 1024 * 1024
RB = 512
NROW = 15
RPI = KPAD // RB // NROW
LAG2, LAG3 = 3, 7
NIT = 2 * NCH + LAG3
STEPS = 2 * NCH


def dot_nt(a, b):
    return lax.dot_general(a, b, (((1,), (1,)), ((), ())), preferred_element_type=jnp.float32)


def dot_nn(a, b):
    return lax.dot_general(a, b, (((1,), (0,)), ((), ())), preferred_element_type=jnp.float32)


def fold8(x):
    return jnp.sum(x.reshape(x.shape[0] // 8, 8, x.shape[1]), axis=0)


def flip(me, bit):
    return me + bit - 2 * bit * lax.rem(me // bit, 2)


def full_barrier(me):
    barrier = pltpu.get_barrier_semaphore()
    for d in range(1, NDEV):
        pl.semaphore_signal(barrier, inc=1, device_id=lax.rem(me + d, NDEV), device_id_type=LOGICAL)
    pl.semaphore_wait(barrier, NDEV - 1)


def send(src, dst, ssem, rsem, to):
    copy = pltpu.make_async_remote_copy(src_ref=src, dst_ref=dst, send_sem=ssem, recv_sem=rsem,
                                        device_id=to, device_id_type=LOGICAL)
    copy.start()


def drain(ref, sem):
    pltpu.make_async_copy(ref, ref, sem).wait()


def kernel(z1, z2, zs, mask, protos, dc, q1, q2, dz, loss,
           ca, ex, slots, lslots, wall, zall, arow, brow, gt, zl, cols, acc,
           csem, zsend, zlrecv, zs1recv, zs2send, zs2recv, arsend, arrecv, lsend, lrecv, wsend, wrecv,
           ssem, r2, r3, rs):
    me = lax.axis_index("data")
    cc = pltpu.make_async_copy(protos, ca.at[pl.ds(0, KP)], csem)
    cc.start()
    ca[pl.ds(KP, KPAD - KP), :] = jnp.zeros((KPAD - KP, D), jnp.bfloat16)
    dims = (flip(me, 2), flip(me, 4), flip(me, 8))
    sib = flip(me, 1)
    here = lax.broadcasted_iota(jnp.int32, (8, 128), 0) == me // 4
    mpad = jnp.concatenate([mask[...].astype(jnp.float32), jnp.zeros((1, 128 - ROWS), jnp.float32)], axis=1)
    slots[0, me] = jnp.where(here, pltpu.roll(jnp.broadcast_to(mpad, (8, 128)), ROWS * lax.rem(me, 4), 1), 0.0)
    with jax.named_scope("barrier"):
        full_barrier(me)
    myrows = pl.ds(pl.multiple_of(me * ROWS, ROWS), ROWS)

    def ar_send(t):
        for d in range(1, NDEV):
            send(slots.at[t, me], slots.at[t, me], arsend.at[t], arrecv.at[t], lax.rem(me + d, NDEV))

    def ar_total(t):
        drain(slots.at[t, pl.ds(0, NDEV - 1)], arrecv.at[t])
        tot = slots[t, 0]
        for i in range(1, NDEV):
            tot = tot + slots[t, i]
        return tot

    for d in range(1, NDEV):
        to = lax.rem(me + d, NDEV)
        send(z1, zall.at[0, myrows], zsend.at[0], zlrecv, to)
        send(z2, zall.at[1, myrows], zsend.at[0], zlrecv, to)
    ar_send(0)
    for d in range(1, NDEV // 2):
        send(zs, zall.at[pl.ds(2, 6), myrows], zsend.at[1], zs1recv, lax.rem(me + 2 * d, NDEV))
    zall[0, myrows] = z1[...]
    zall[1, myrows] = z2[...]
    zall[pl.ds(2, 6), myrows] = zs[...]
    send(zs, zall.at[pl.ds(2, 6), myrows], zs2send, zs2recv, sib)
    zl[pl.ds(0, ROWS)] = z1[...]
    zl[pl.ds(ROWS, ROWS)] = z2[...]
    zl[pl.ds(2 * ROWS, 6 * ROWS)] = zs[...].reshape(6 * ROWS, D)
    acc[...] = jnp.zeros_like(acc)
    cc.wait()
    with jax.named_scope("mask"):
        mask8 = ar_total(0)
    live = jnp.sum(jnp.sum(mask8, axis=1, keepdims=True), axis=0, keepdims=True)
    mrow = jnp.concatenate([mask8[j:j + 1] for j in range(4)], axis=1)
    with jax.named_scope("zlarge"):
        drain(zall.at[pl.ds(0, 2), pl.ds(0, NS - ROWS)], zlrecv)

    def shard(b):
        return ca[pl.ds(pl.multiple_of(me * SH + b * CB, 128), CB)]

    def col_scale(c, b):
        k = me * SH + b * CB + lax.broadcasted_iota(jnp.int32, (CB, 1), 0)
        return jnp.where(k < KP, 1.0 / (KP * c), 0.0)

    zero8 = jnp.zeros((8, NS), jnp.float32)

    def first(b, carry):
        rows = pl.ds(b * CB, CB)
        out = []
        for v in range(2):
            ps, r = carry[2 * v], carry[2 * v + 1]
            p = jnp.exp2(dot_nt(shard(b), zall[v]) * SCALE)
            ps = ps + fold8(p)
            e = p * p * mrow
            ex[v, rows] = e
            w = col_scale(jnp.sum(e, axis=1, keepdims=True), b)
            r = r + fold8(e * w)
            out += [ps, r]
        return tuple(out)

    def put(t, r1, r2):
        for v, r in enumerate((r1, r2)):
            row = jnp.sum(r, axis=0, keepdims=True)
            for j in range(4):
                slots[t, me, pl.ds(4 * v + j, 1)] = row[:, 128 * j:128 * (j + 1)]

    def scale_rows(tot):
        us = []
        for v in range(2):
            r = jnp.concatenate([tot[4 * v + j:4 * v + j + 1] for j in range(4)], axis=1)
            us.append(mrow / (live * jnp.where(mrow > 0, r, 1.0)))
        return us

    pad = jnp.where(me == NDEV - 1, float(SH - LAST), 0.0)

    def put_lse(v, ps):
        row = jnp.sum(ps, axis=0, keepdims=True) - pad
        for j in range(4):
            lslots[me, pl.ds(4 * v + j, 1)] = row[:, 128 * j:128 * (j + 1)]

    with jax.named_scope("first"):
        carry = (zero8,) * 4
        for b in range(NCH):
            carry = first(b, carry)
        ps1, r1, ps2, rr2 = carry
        put(1, r1, rr2)
        ar_send(1)
    put_lse(0, ps1)
    put_lse(1, ps2)
    with jax.named_scope("zsmall1"):
        drain(zall.at[pl.ds(2, 6), pl.ds(0, 7 * ROWS)], zs1recv)
    for d in range(1, NDEV // 2):
        rows = pl.ds(pl.multiple_of(lax.rem(me + 2 * d, NDEV) * ROWS, ROWS), ROWS)
        send(zall.at[pl.ds(2, 6), rows], zall.at[pl.ds(2, 6), rows], zs2send, zs2recv, sib)
    def small(i, carry):
        v = 2 + i
        ps = zero8
        for b in range(NCH):
            ps = ps + fold8(jnp.exp2(dot_nt(shard(b), zall[v]) * SCALE))
        put_lse(v, ps)
        return carry

    with jax.named_scope("zsmall2"):
        drain(zall.at[pl.ds(2, 6), pl.ds(0, 8 * ROWS)], zs2recv)

    with jax.named_scope("small"):
        lax.fori_loop(0, 3, small, 0)
    with jax.named_scope("ar1"):
        us = scale_rows(ar_total(1))

    def again(us, last):
        def step(b, carry):
            rows = pl.ds(pl.multiple_of(b * CB, CB), CB)
            out = []
            for v in range(2):
                e = ex[v, rows]
                w = col_scale(jnp.sum(e * us[v], axis=1, keepdims=True), b)
                out.append(carry[v] + fold8(e * w))
                if last:
                    for q in range(CB // 128):
                        wt = jnp.broadcast_to(w[128 * q:128 * (q + 1)], (128, 128)).T
                        wall[me, pl.ds(v, 1), pl.ds(pl.multiple_of(b * CB + 128 * q, 128), 128)] = wt[0:1]
            return tuple(out)
        return step

    with jax.named_scope("again2"):
        r1, rr2 = lax.fori_loop(0, NCH, again(us, False), (zero8, zero8))
        put(2, r1, rr2)
        ar_send(2)
    with jax.named_scope("small"):
        lax.fori_loop(3, 6, small, 0)
        for d in range(1, NDEV):
            send(lslots.at[me], lslots.at[me], lsend, lrecv, lax.rem(me + d, NDEV))
    with jax.named_scope("ar2"):
        us = scale_rows(ar_total(2))
    with jax.named_scope("again3"):
        r1, rr2 = lax.fori_loop(0, NCH, again(us, True), (zero8, zero8))
        put(3, r1, rr2)
        ar_send(3)
        for d in range(1, NDEV):
            send(wall.at[me], wall.at[me], wsend, wrecv, lax.rem(me + d, NDEV))
    gsc = 1.0 / (TAU * PAIRS * live)
    with jax.named_scope("lse"):
        drain(lslots.at[pl.ds(0, NDEV - 1)], lrecv)
        tot = lslots[0]
        for i in range(1, NDEV):
            tot = tot + lslots[i]
        inv = 1.0 / tot
        for v in range(VIEWS):
            for j in range(4):
                coef = 1.0 if v < 2 else 2.0
                arow[v:v + 1, 128 * j:128 * (j + 1)] = (coef * gsc) * (mask8[j:j + 1] * inv[4 * v + j:4 * v + j + 1])
        weight = jnp.concatenate([mask8[0:4]] * 2 + [2.0 * mask8[0:4]] * 6, axis=0)
        lsum = jnp.sum(jnp.sum(weight * jnp.log(tot), axis=1, keepdims=True), axis=0, keepdims=True)
    with jax.named_scope("ar3"):
        us = scale_rows(ar_total(3))
    for v in range(2):
        brow[v:v + 1] = live * us[v]
    brow[2:8] = jnp.zeros((6, NS), jnp.float32)
    tile = pl.ds(pl.multiple_of((me // 4) * 128, 128), 128)
    cols[0] = arow[:, tile].T
    cols[1] = brow[:, tile].T
    mine = pl.ds(pl.multiple_of(lax.rem(me, 4) * ROWS, ROWS), ROWS)

    def piece_row(owner, t, a):
        return pl.multiple_of(owner * SH + t * CB + a * 128, 128)

    def push(owner, it, a, to, rsem):
        ref = dc.at[pl.ds(piece_row(owner, it // 2, a), 128)]
        send(ref, ref, ssem.at[it, a], rsem.at[it, a], to)

    def order(a):
        return dims[a], dims[(a + 1) % 3], dims[(a + 2) % 3]

    def owner_of(holder, d0, it):
        return holder + lax.rem(it, 2) * (d0 - me)

    def chunk(it):
        t = it // 2
        owners = [owner_of(me, dims[a], it) for a in range(3)]
        c = jnp.concatenate([ca[pl.ds(piece_row(owners[a], t, a), 128)] for a in range(3)], axis=0)
        wc = []
        for v in range(2):
            parts = []
            for a in range(3):
                off = pl.multiple_of(t * CB + a * 128, 128)
                row = wall[owners[a], pl.ds(v, 1), pl.ds(off, 128)] * gsc
                parts.append(jnp.broadcast_to(row, (128, 128)).T)
            wc.append(jnp.concatenate(parts, axis=0))

        def nblk(nb):
            ln = pl.ds(nb * 256, 256)
            s = [dot_nt(c, zall[v, ln]) for v in range(VIEWS)]
            av = [arow[v:v + 1, ln] for v in range(VIEWS)]
            bv = [brow[v:v + 1, ln] for v in range(2)]
            for q in range(CB // 64):
                sl = slice(64 * q, 64 * (q + 1))
                w0 = jnp.concatenate([wc[0][sl], wc[0][sl]], axis=1)
                w1 = jnp.concatenate([wc[1][sl], wc[1][sl]], axis=1)
                p0 = jnp.exp2(s[0][sl] * SCALE)
                p1 = jnp.exp2(s[1][sl] * SCALE)
                x0 = (p0 * p0) * bv[0] * w0
                x1 = (p1 * p1) * bv[1] * w1
                xs = x0 + x1
                gs = [p0 * av[0] - x1, p1 * av[1] - x0]
                for v in range(2, VIEWS):
                    gs.append(jnp.exp2(s[v][sl] * SCALE) * av[v] - xs)
                for v in range(VIEWS):
                    gt[nb, pl.ds(64 * q, 64), pl.ds(v * 256, 256)] = gs[v].astype(jnp.bfloat16)
            zz = jnp.concatenate([zall[v, ln] for v in range(VIEWS)], axis=0)
            return dot_nn(gt[nb], zz)

        res = nblk(0)
        res = res + nblk(1)
        for a in range(3):
            dc[pl.ds(piece_row(owners[a], t, a), 128)] = res[128 * a:128 * (a + 1)]

    def rows_part(i):
        ac = cols[0, mine]
        bc = cols[1, mine]
        outs = []
        for h in range(RPI):
            jb = i * RPI + h
            c = ca[pl.ds(pl.multiple_of(jb * RB, RB), RB)]
            s = dot_nt(zl[...], c) * SCALE
            wr = []
            for v in range(2):
                parts = []
                for q in range(RB // 128):
                    b = jb * (RB // 128) + q
                    parts.append(wall[b // (SH // 128), pl.ds(v, 1), pl.ds(pl.multiple_of(lax.rem(b, SH // 128) * 128, 128), 128)])
                wr.append(jnp.concatenate(parts, axis=1))
            sv = [s[ROWS * v:ROWS * (v + 1)] for v in range(VIEWS)]
            p0 = jnp.exp2(sv[0])
            p1 = jnp.exp2(sv[1])
            o0 = (p0 * p0) * bc[:, 0:1] * wr[0]
            o1 = (p1 * p1) * bc[:, 1:2] * wr[1]

            outs.append((o0, o1))
            x0 = o0 * gsc
            x1 = o1 * gsc
            xs = x0 + x1
            gs = [p0 * ac[:, 0:1] - x1, p1 * ac[:, 1:2] - x0]
            ssum = sv[2]
            for v in range(3, VIEWS):
                ssum = ssum + sv[v]
            for v in range(2, VIEWS):
                gs.append(jnp.exp2(sv[v]) * ac[:, v:v + 1] - xs)
            g = jnp.concatenate([x.astype(jnp.bfloat16) for x in gs], axis=0)
            acc[pl.ds(0, VIEWS * ROWS)] += dot_nn(g, c)
            ls = x1 * sv[0] + x0 * sv[1] + xs * ssum
            part = ls[:, 0:128]
            for q in range(1, RB // 128):
                part = part + ls[:, 128 * q:128 * (q + 1)]
            acc[pl.ds(VIEWS * ROWS, ROWS)] += part

        @pl.when(i < NROW - 1)
        def _():
            for h in range(RPI):
                ln = pl.ds(pl.multiple_of((i * RPI + h) * RB, RB), RB)
                q1[:, ln] = outs[h][0]
                q2[:, ln] = outs[h][1]

        @pl.when(i == NROW - 1)
        def _():
            for h in range(RPI):
                lo = ((NROW - 1) * RPI + h) * RB
                n = min(RB, KP - lo)
                if n > 0:
                    q1[:, pl.ds(lo, n)] = outs[h][0][:, :n]
                    q2[:, pl.ds(lo, n)] = outs[h][1][:, :n]

    def own(it):
        for a in range(3):
            d0, d1, d2 = order(a)
            o = owner_of(me, d0, it)
            push(o, it, a, d1, r2)
            push(o, it, a, d2, r3)
            push(o, it, a, sib, rs)

    def serve2(it):
        for a in range(3):
            d0, d1, d2 = order(a)
            drain(dc.at[pl.ds(0, 128)], r2.at[it, a])
            o = owner_of(d1, d0, it)
            push(o, it, a, d2, r3)
            push(o, it, a, sib, rs)

    def serve3(it):
        for a in range(3):
            d0, d1, d2 = order(a)
            drain(dc.at[pl.ds(0, 256)], r3.at[it, a])
            for holder in (d2, d2 + d1 - me):
                push(owner_of(holder, d0, it), it, a, sib, rs)

    def main(it, carry):
        @pl.when(it < STEPS)
        def _():
            with jax.named_scope("chunk"):
                chunk(it)
            own(it)

        @pl.when(it == 0)
        def _():
            with jax.named_scope("wait_w"):
                drain(wall.at[pl.ds(0, NDEV - 1)], wrecv)

        @pl.when(jnp.logical_and(it >= LAG2, it < LAG2 + STEPS))
        def _():
            with jax.named_scope("serve2"):
                serve2(it - LAG2)

        @pl.when(it < NROW)
        def _():
            with jax.named_scope("rows"):
                rows_part(it)

        @pl.when(it == NROW)
        def _():
            total = jnp.sum(jnp.sum(acc[pl.ds(VIEWS * ROWS, ROWS)], axis=1, keepdims=True), axis=0, keepdims=True)
            slots[4, me] = jnp.broadcast_to(total, (8, 128))
            ar_send(4)

        @pl.when(it >= LAG3)
        def _():
            with jax.named_scope("serve3"):
                serve3(it - LAG3)

        return carry

    lax.fori_loop(0, NIT, main, 0)

    dz[...] = acc[pl.ds(0, VIEWS * ROWS)].reshape(VIEWS, ROWS, D)
    with jax.named_scope("loss"):
        tot = ar_total(4)
    cross = tot[0:1, 0:1] * (LN2 * TAU * PAIRS) * live - lsum
    loss[...] = -cross / (live * PAIRS)

    def finish(it, carry):
        for a in range(3):
            drain(dc.at[pl.ds(0, 4 * 128)], rs.at[it, a])
            drain(dc.at[pl.ds(0, 7 * 128)], ssem.at[it, a])
        return carry

    with jax.named_scope("finish"):
        lax.fori_loop(0, STEPS, finish, 0)
    drain(zall.at[pl.ds(0, 2), pl.ds(0, NS - ROWS)], zsend.at[0])
    drain(zall.at[pl.ds(2, 6), pl.ds(0, 7 * ROWS)], zsend.at[1])
    drain(zall.at[pl.ds(2, 6), pl.ds(0, 8 * ROWS)], zs2send)
    for t in range(5):
        drain(slots.at[t, pl.ds(0, NDEV - 1)], arsend.at[t])
    drain(lslots.at[pl.ds(0, NDEV - 1)], lsend)
    drain(wall.at[pl.ds(0, NDEV - 1)], wsend)


def emit_kernel(dc, q1, q2, dz, loss, o_q1, o_q2, o_loss, o_z1, o_z2, o_zs, o_dc, sem):
    pairs = [(dc.at[pl.ds(0, KP)], o_dc), (q1, o_q1), (q2, o_q2), (loss, o_loss),
             (dz.at[0], o_z1), (dz.at[1], o_z2), (dz.at[pl.ds(2, 6)], o_zs)]
    copies = [pltpu.make_async_copy(a, b, sem.at[i]) for i, (a, b) in enumerate(pairs)]
    for c in copies:
        c.start()
    for c in copies:
        c.wait()


def local_step(z_one, z_two, z_small, protos, live_mask):
    f32 = jnp.float32
    bf16 = jnp.bfloat16
    vmem = pl.BlockSpec(memory_space=pltpu.VMEM)
    anym = pl.BlockSpec(memory_space=pl.ANY)
    dma = pltpu.SemaphoreType.DMA
    vm = pltpu.VMEM
    dc, q1, q2, dz, loss = pl.pallas_call(
        kernel,
        out_shape=[vm((KPAD, D), f32), vm((ROWS, KP), f32), vm((ROWS, KP), f32),
                   vm((VIEWS, ROWS, D), f32), vm((1, 1), f32)],
        in_specs=[vmem] * 4 + [anym],
        out_specs=[vmem] * 5,
        scratch_shapes=[vm((KPAD, D), bf16), vm((2, SH, NS), f32), vm((5, NDEV, 8, 128), f32), vm((NDEV, 32, 128), f32),
                        vm((NDEV, 2, SH), f32), vm((VIEWS, NS, D), bf16), vm((8, NS), f32), vm((8, NS), f32),
                        vm((2, CB, VIEWS * 256), bf16), vm((VIEWS * ROWS, D), bf16), vm((2, 128, 8), f32),
                        vm((VIEWS * ROWS + ROWS, D), f32),
                        dma, dma((2,)), dma, dma, dma, dma, dma((5,)), dma((5,)), dma, dma, dma, dma,
                        dma((STEPS, 3)), dma((STEPS, 3)), dma((STEPS, 3)), dma((STEPS, 3))],
        compiler_params=pltpu.CompilerParams(collective_id=0, has_side_effects=True, vmem_limit_bytes=VM),
        name="step",
    )(z_one, z_two, z_small, live_mask.reshape(1, ROWS), protos)
    q1, q2, loss, dz1, dz2, dzs, dc = pl.pallas_call(
        emit_kernel,
        out_shape=[jax.ShapeDtypeStruct((ROWS, KP), f32), jax.ShapeDtypeStruct((ROWS, KP), f32),
                   jax.ShapeDtypeStruct((1, 1), f32), jax.ShapeDtypeStruct((ROWS, D), f32),
                   jax.ShapeDtypeStruct((ROWS, D), f32), jax.ShapeDtypeStruct((6, ROWS, D), f32),
                   jax.ShapeDtypeStruct((KP, D), f32)],
        in_specs=[vmem] * 5,
        out_specs=[anym] * 7,
        scratch_shapes=[dma((7,))],
        compiler_params=pltpu.CompilerParams(vmem_limit_bytes=1024 * 1024),
        name="emit",
    )(dc, q1, q2, dz, loss)
    return q1, q2, loss.reshape(()), dz1, dz2, dzs, dc


def solution(mesh):
    row_spec = P("data", None)
    crop_spec = P(None, "data", None)
    return jax.shard_map(local_step, mesh=mesh,
                         in_specs=(row_spec, row_spec, crop_spec, P(None, None), P("data")),
                         out_specs=(row_spec, row_spec, P(), row_spec, row_spec, crop_spec, P(None, None)),
                         check_vma=False)
```

```python
import jax
import jax.numpy as jnp
from jax import lax
from jax.experimental import pallas as pl
from jax.experimental.pallas import tpu as pltpu
from jax.sharding import PartitionSpec as P

TAU = 0.1
LOG2E = 1.4426950408889634
LN2 = 0.6931471805599453
SCALE = LOG2E / TAU
NDEV = 16
ROWS = 32
NS = 512
VIEWS = 8
D = 128
KP = 30000
SH = 1920
KPAD = SH * NDEV
LAST = KP - SH * (NDEV - 1)
CB = 384
NCH = SH // CB
PAIRS = 14.0
LOGICAL = pl.DeviceIdType.LOGICAL
VM = 36 * 1024 * 1024
RB = 512
STEPS = 2 * NCH
RPI = KPAD // RB // STEPS
RW = RPI * RB
QT = KP - RW * (STEPS - 1)
LAG2, LAG3 = 2, 4


def dot_nt(a, b):
    return lax.dot_general(a, b, (((1,), (1,)), ((), ())), preferred_element_type=jnp.float32)


def dot_nn(a, b):
    return lax.dot_general(a, b, (((1,), (0,)), ((), ())), preferred_element_type=jnp.float32)


def fold8(x):
    return jnp.sum(x.reshape(x.shape[0] // 8, 8, x.shape[1]), axis=0)


def flip(me, bit):
    return me + bit - 2 * bit * lax.rem(me // bit, 2)


def full_barrier(me):
    barrier = pltpu.get_barrier_semaphore()
    for d in range(1, NDEV):
        pl.semaphore_signal(barrier, inc=1, device_id=lax.rem(me + d, NDEV), device_id_type=LOGICAL)
    pl.semaphore_wait(barrier, NDEV - 1)


def send(src, dst, ssem, rsem, to):
    copy = pltpu.make_async_remote_copy(src_ref=src, dst_ref=dst, send_sem=ssem, recv_sem=rsem,
                                        device_id=to, device_id_type=LOGICAL)
    copy.start()


def drain(ref, sem):
    pltpu.make_async_copy(ref, ref, sem).wait()


def kernel(z1, z2, zs, mask, protos, dc, qs, qt, dz, loss,
           ca, ex, slots, lslots, wall, zall, arow, brow, gt, xsc, gr, zl, cols, acc,
           csem, zsend, zlrecv, zs1recv, zs2send, zs2recv, arsend, arrecv, lsend, lrecv, wsend, wrecv,
           ssem, r2, r3, rs):
    me = lax.axis_index("data")
    cc = pltpu.make_async_copy(protos, ca.at[pl.ds(0, KP)], csem)
    cc.start()
    ca[pl.ds(KP, KPAD - KP), :] = jnp.zeros((KPAD - KP, D), jnp.bfloat16)
    dims = (flip(me, 2), flip(me, 4), flip(me, 8))
    sib = flip(me, 1)
    here = lax.broadcasted_iota(jnp.int32, (8, 128), 0) == me // 4
    mpad = jnp.concatenate([mask[...].astype(jnp.float32), jnp.zeros((1, 128 - ROWS), jnp.float32)], axis=1)
    slots[0, me] = jnp.where(here, pltpu.roll(jnp.broadcast_to(mpad, (8, 128)), ROWS * lax.rem(me, 4), 1), 0.0)
    with jax.named_scope("barrier"):
        full_barrier(me)
    myrows = pl.ds(pl.multiple_of(me * ROWS, ROWS), ROWS)

    def ar_send(t):
        for d in range(1, NDEV):
            send(slots.at[t, me], slots.at[t, me], arsend.at[t], arrecv.at[t], lax.rem(me + d, NDEV))

    def ar_total(t):
        drain(slots.at[t, pl.ds(0, NDEV - 1)], arrecv.at[t])
        tot = slots[t, 0]
        for i in range(1, NDEV):
            tot = tot + slots[t, i]
        return tot

    for d in range(1, NDEV):
        to = lax.rem(me + d, NDEV)
        send(z1, zall.at[0, myrows], zsend.at[0], zlrecv, to)
        send(z2, zall.at[1, myrows], zsend.at[0], zlrecv, to)
    ar_send(0)
    for d in range(1, NDEV // 2):
        send(zs, zall.at[pl.ds(2, 6), myrows], zsend.at[1], zs1recv, lax.rem(me + 2 * d, NDEV))
    zall[0, myrows] = z1[...]
    zall[1, myrows] = z2[...]
    zall[pl.ds(2, 6), myrows] = zs[...]
    send(zs, zall.at[pl.ds(2, 6), myrows], zs2send, zs2recv, sib)
    zl[pl.ds(0, ROWS)] = z1[...]
    zl[pl.ds(ROWS, ROWS)] = z2[...]
    zl[pl.ds(2 * ROWS, 6 * ROWS)] = zs[...].reshape(6 * ROWS, D)
    acc[...] = jnp.zeros_like(acc)
    cc.wait()
    with jax.named_scope("mask"):
        mask8 = ar_total(0)
    live = jnp.sum(jnp.sum(mask8, axis=1, keepdims=True), axis=0, keepdims=True)
    mrow = jnp.concatenate([mask8[j:j + 1] for j in range(4)], axis=1)
    with jax.named_scope("zlarge"):
        drain(zall.at[pl.ds(0, 2), pl.ds(0, NS - ROWS)], zlrecv)

    def shard(b):
        return ca[pl.ds(pl.multiple_of(me * SH + b * CB, 128), CB)]

    def col_scale(c, b):
        k = me * SH + b * CB + lax.broadcasted_iota(jnp.int32, (CB, 1), 0)
        return jnp.where(k < KP, 1.0 / (KP * c), 0.0)

    zero8 = jnp.zeros((8, NS), jnp.float32)

    def first(b, carry):
        rows = pl.ds(b * CB, CB)
        out = []
        for v in range(2):
            ps, r = carry[2 * v], carry[2 * v + 1]
            p = jnp.exp2(dot_nt(shard(b), zall[v]) * SCALE)
            ps = ps + fold8(p)
            e = p * p * mrow
            ex[v, rows] = e
            w = col_scale(jnp.sum(e, axis=1, keepdims=True), b)
            r = r + fold8(e * w)
            out += [ps, r]
        return tuple(out)

    def put(t, r1, r2):
        for v, r in enumerate((r1, r2)):
            row = jnp.sum(r, axis=0, keepdims=True)
            for j in range(4):
                slots[t, me, pl.ds(4 * v + j, 1)] = row[:, 128 * j:128 * (j + 1)]

    def scale_rows(tot):
        us = []
        for v in range(2):
            r = jnp.concatenate([tot[4 * v + j:4 * v + j + 1] for j in range(4)], axis=1)
            us.append(mrow / (live * jnp.where(mrow > 0, r, 1.0)))
        return us

    pad = jnp.where(me == NDEV - 1, float(SH - LAST), 0.0)

    def put_lse(v, ps):
        row = jnp.sum(ps, axis=0, keepdims=True) - pad
        for j in range(4):
            lslots[me, pl.ds(4 * v + j, 1)] = row[:, 128 * j:128 * (j + 1)]

    with jax.named_scope("first"):
        carry = (zero8,) * 4
        for b in range(NCH):
            carry = first(b, carry)
        ps1, r1, ps2, rr2 = carry
        put(1, r1, rr2)
        ar_send(1)
    put_lse(0, ps1)
    put_lse(1, ps2)
    with jax.named_scope("zsmall1"):
        drain(zall.at[pl.ds(2, 6), pl.ds(0, 7 * ROWS)], zs1recv)
    for d in range(1, NDEV // 2):
        rows = pl.ds(pl.multiple_of(lax.rem(me + 2 * d, NDEV) * ROWS, ROWS), ROWS)
        send(zall.at[pl.ds(2, 6), rows], zall.at[pl.ds(2, 6), rows], zs2send, zs2recv, sib)
    def small(i, carry):
        v = 2 + i
        ps = zero8
        for b in range(NCH):
            ps = ps + fold8(jnp.exp2(dot_nt(shard(b), zall[v]) * SCALE))
        put_lse(v, ps)
        return carry

    with jax.named_scope("zsmall2"):
        drain(zall.at[pl.ds(2, 6), pl.ds(0, 8 * ROWS)], zs2recv)

    with jax.named_scope("small"):
        lax.fori_loop(0, 3, small, 0)
    with jax.named_scope("ar1"):
        us = scale_rows(ar_total(1))

    def again(us, last):
        def step(b, carry):
            rows = pl.ds(pl.multiple_of(b * CB, CB), CB)
            out = []
            for v in range(2):
                e = ex[v, rows]
                w = col_scale(jnp.sum(e * us[v], axis=1, keepdims=True), b)
                out.append(carry[v] + fold8(e * w))
                if last:
                    for q in range(CB // 128):
                        wt = jnp.broadcast_to(w[128 * q:128 * (q + 1)], (128, 128)).T
                        wall[me, pl.ds(v, 1), pl.ds(pl.multiple_of(b * CB + 128 * q, 128), 128)] = wt[0:1]
            return tuple(out)
        return step

    with jax.named_scope("again2"):
        r1, rr2 = lax.fori_loop(0, NCH, again(us, False), (zero8, zero8))
        put(2, r1, rr2)
        ar_send(2)
    with jax.named_scope("small"):
        lax.fori_loop(3, 6, small, 0)
        for d in range(1, NDEV):
            send(lslots.at[me], lslots.at[me], lsend, lrecv, lax.rem(me + d, NDEV))
    with jax.named_scope("ar2"):
        us = scale_rows(ar_total(2))
    with jax.named_scope("again3"):
        r1, rr2 = lax.fori_loop(0, NCH, again(us, True), (zero8, zero8))
        put(3, r1, rr2)
        ar_send(3)
        for d in range(1, NDEV):
            send(wall.at[me], wall.at[me], wsend, wrecv, lax.rem(me + d, NDEV))
    gsc = 1.0 / (TAU * PAIRS * live)
    with jax.named_scope("lse"):
        drain(lslots.at[pl.ds(0, NDEV - 1)], lrecv)
        tot = lslots[0]
        for i in range(1, NDEV):
            tot = tot + lslots[i]
        inv = 1.0 / tot
        for v in range(VIEWS):
            for j in range(4):
                coef = 1.0 if v < 2 else 2.0
                arow[v:v + 1, 128 * j:128 * (j + 1)] = (coef * gsc) * (mask8[j:j + 1] * inv[4 * v + j:4 * v + j + 1])
        weight = jnp.concatenate([mask8[0:4]] * 2 + [2.0 * mask8[0:4]] * 6, axis=0)
        lsum = jnp.sum(jnp.sum(weight * jnp.log(tot), axis=1, keepdims=True), axis=0, keepdims=True)
    with jax.named_scope("ar3"):
        us = scale_rows(ar_total(3))
    for v in range(2):
        brow[v:v + 1] = live * us[v]
    brow[2:8] = jnp.zeros((6, NS), jnp.float32)
    tile = pl.ds(pl.multiple_of((me // 4) * 128, 128), 128)
    cols[0] = arow[:, tile].T
    cols[1] = brow[:, tile].T
    mine = pl.ds(pl.multiple_of(lax.rem(me, 4) * ROWS, ROWS), ROWS)

    def piece_row(owner, t, a):
        return pl.multiple_of(owner * SH + t * CB + a * 128, 128)

    def push(owner, it, a, to, rsem):
        ref = dc.at[pl.ds(piece_row(owner, it // 2, a), 128)]
        send(ref, ref, ssem.at[it, a], rsem.at[it, a], to)

    def order(a):
        return dims[a], dims[(a + 1) % 3], dims[(a + 2) % 3]

    def owner_of(holder, d0, it):
        return holder + lax.rem(it, 2) * (d0 - me)

    def chunk(it):
        t = it // 2
        owners = [owner_of(me, dims[a], it) for a in range(3)]
        c = jnp.concatenate([ca[pl.ds(piece_row(owners[a], t, a), 128)] for a in range(3)], axis=0)
        wc = []
        for v in range(2):
            parts = []
            for a in range(3):
                off = pl.multiple_of(t * CB + a * 128, 128)
                row = wall[owners[a], pl.ds(v, 1), pl.ds(off, 128)] * gsc
                parts.append(jnp.broadcast_to(row, (128, 128)).T)
            wc.append(jnp.concatenate(parts, axis=0))

        def nblk(nb):
            ln = pl.ds(nb * 256, 256)
            s0 = dot_nt(c, zall[0, ln])
            s1 = dot_nt(c, zall[1, ln])
            for q in range(CB // 64):
                sl = slice(64 * q, 64 * (q + 1))
                w0 = jnp.concatenate([wc[0][sl], wc[0][sl]], axis=1)
                w1 = jnp.concatenate([wc[1][sl], wc[1][sl]], axis=1)
                p0 = jnp.exp2(s0[sl] * SCALE)
                p1 = jnp.exp2(s1[sl] * SCALE)
                x0 = (p0 * p0) * brow[0:1, ln] * w0
                x1 = (p1 * p1) * brow[1:2, ln] * w1
                xsc[nb, pl.ds(64 * q, 64)] = x0 + x1
                gt[nb, pl.ds(64 * q, 64), pl.ds(0, 256)] = (p0 * arow[0:1, ln] - x1).astype(jnp.bfloat16)
                gt[nb, pl.ds(64 * q, 64), pl.ds(256, 256)] = (p1 * arow[1:2, ln] - x0).astype(jnp.bfloat16)
            for v in range(2, VIEWS):
                s = dot_nt(c, zall[v, ln])
                av = arow[v:v + 1, ln]
                for q in range(CB // 64):
                    sl = pl.ds(64 * q, 64)
                    g = jnp.exp2(s[64 * q:64 * (q + 1)] * SCALE) * av - xsc[nb, sl]
                    gt[nb, sl, pl.ds(v * 256, 256)] = g.astype(jnp.bfloat16)
            zz = jnp.concatenate([zall[v, ln] for v in range(VIEWS)], axis=0)
            return dot_nn(gt[nb], zz)

        res = nblk(0)
        res = res + nblk(1)
        for a in range(3):
            dc[pl.ds(piece_row(owners[a], t, a), 128)] = res[128 * a:128 * (a + 1)]

    def rows_part(i):
        ac = cols[0, mine]
        bc = cols[1, mine]
        for h in range(RPI):
            jb = i * RPI + h
            c = ca[pl.ds(pl.multiple_of(jb * RB, RB), RB)]
            s = dot_nt(zl[...], c) * SCALE
            wr = []
            for v in range(2):
                parts = []
                for q in range(RB // 128):
                    b = jb * (RB // 128) + q
                    parts.append(wall[b // (SH // 128), pl.ds(v, 1), pl.ds(pl.multiple_of(lax.rem(b, SH // 128) * 128, 128), 128)])
                wr.append(jnp.concatenate(parts, axis=1))
            sv = [s[ROWS * v:ROWS * (v + 1)] for v in range(VIEWS)]
            p0 = jnp.exp2(sv[0])
            p1 = jnp.exp2(sv[1])
            o0 = (p0 * p0) * bc[:, 0:1] * wr[0]
            o1 = (p1 * p1) * bc[:, 1:2] * wr[1]
            col = pl.ds(h * RB, RB)
            qs[i, 0, :, col] = o0
            qs[i, 1, :, col] = o1
            x0 = o0 * gsc
            x1 = o1 * gsc
            xs = x0 + x1
            gr[pl.ds(0, ROWS), col] = (p0 * ac[:, 0:1] - x1).astype(jnp.bfloat16)
            gr[pl.ds(ROWS, ROWS), col] = (p1 * ac[:, 1:2] - x0).astype(jnp.bfloat16)
            ssum = sv[2]
            for v in range(3, VIEWS):
                ssum = ssum + sv[v]
            for v in range(2, VIEWS):
                gr[pl.ds(v * ROWS, ROWS), col] = (jnp.exp2(sv[v]) * ac[:, v:v + 1] - xs).astype(jnp.bfloat16)
            ls = x1 * sv[0] + x0 * sv[1] + xs * ssum
            part = ls[:, 0:128]
            for q in range(1, RB // 128):
                part = part + ls[:, 128 * q:128 * (q + 1)]
            acc[pl.ds(VIEWS * ROWS, ROWS)] += part
        cs = ca[pl.ds(pl.multiple_of(i * RW, RW), RW)]
        acc[pl.ds(0, VIEWS * ROWS)] += dot_nn(gr[...], cs)

    def own(it):
        for a in range(3):
            d0, d1, d2 = order(a)
            o = owner_of(me, d0, it)
            push(o, it, a, d1, r2)
            push(o, it, a, d2, r3)
            push(o, it, a, sib, rs)

    def serve2(it):
        for a in range(3):
            d0, d1, d2 = order(a)
            drain(dc.at[pl.ds(0, 128)], r2.at[it, a])
            o = owner_of(d1, d0, it)
            push(o, it, a, d2, r3)
            push(o, it, a, sib, rs)

    def serve3(it):
        for a in range(3):
            d0, d1, d2 = order(a)
            drain(dc.at[pl.ds(0, 256)], r3.at[it, a])
            for holder in (d2, d2 + d1 - me):
                push(owner_of(holder, d0, it), it, a, sib, rs)

    def main(it, carry):
        @pl.when(it == 0)
        def _():
            with jax.named_scope("wait_w"):
                drain(wall.at[pl.ds(0, NDEV - 1)], wrecv)

        with jax.named_scope("compute"):
            chunk(it)
            rows_part(it)
        own(it)

        @pl.when(it >= LAG2)
        def _():
            with jax.named_scope("serve2"):
                serve2(it - LAG2)

        @pl.when(it >= LAG3)
        def _():
            with jax.named_scope("serve3"):
                serve3(it - LAG3)

        return carry

    lax.fori_loop(0, STEPS, main, 0)
    for v in range(2):
        qt[v] = qs[STEPS - 1, v, :, pl.ds(0, QT)]
    total = jnp.sum(jnp.sum(acc[pl.ds(VIEWS * ROWS, ROWS)], axis=1, keepdims=True), axis=0, keepdims=True)
    slots[4, me] = jnp.broadcast_to(total, (8, 128))
    ar_send(4)

    def rest(it, carry):
        @pl.when(it < STEPS + LAG2)
        def _():
            with jax.named_scope("serve2"):
                serve2(it - LAG2)

        with jax.named_scope("serve3"):
            serve3(it - LAG3)
        return carry

    lax.fori_loop(STEPS, STEPS + LAG3, rest, 0)
    dz[...] = acc[pl.ds(0, VIEWS * ROWS)].reshape(VIEWS, ROWS, D)
    with jax.named_scope("loss"):
        tot = ar_total(4)
    cross = tot[0:1, 0:1] * (LN2 * TAU * PAIRS) * live - lsum
    loss[...] = -cross / (live * PAIRS)

    def finish(it, carry):
        for a in range(3):
            drain(dc.at[pl.ds(0, 4 * 128)], rs.at[it, a])
            drain(dc.at[pl.ds(0, 7 * 128)], ssem.at[it, a])
        return carry

    with jax.named_scope("finish"):
        lax.fori_loop(0, STEPS, finish, 0)
    drain(zall.at[pl.ds(0, 2), pl.ds(0, NS - ROWS)], zsend.at[0])
    drain(zall.at[pl.ds(2, 6), pl.ds(0, 7 * ROWS)], zsend.at[1])
    drain(zall.at[pl.ds(2, 6), pl.ds(0, 8 * ROWS)], zs2send)
    for t in range(5):
        drain(slots.at[t, pl.ds(0, NDEV - 1)], arsend.at[t])
    drain(lslots.at[pl.ds(0, NDEV - 1)], lsend)
    drain(wall.at[pl.ds(0, NDEV - 1)], wsend)


def emit_kernel(dc, qs, qt, dz, loss, o_q1, o_q2, o_loss, o_z1, o_z2, o_zs, o_dc, sem):
    pairs = []
    for i in range(STEPS):
        for v, o in enumerate((o_q1, o_q2)):
            if i < STEPS - 1:
                pairs.append((qs.at[i, v], o.at[:, pl.ds(i * RW, RW)]))
            else:
                pairs.append((qt.at[v], o.at[:, pl.ds(i * RW, QT)]))
        rows = pl.ds(i * RW, RW if i < STEPS - 1 else QT)
        pairs.append((dc.at[rows], o_dc.at[rows]))
    pairs += [(loss, o_loss), (dz.at[0], o_z1), (dz.at[1], o_z2), (dz.at[pl.ds(2, 6)], o_zs)]
    copies = [pltpu.make_async_copy(a, b, sem.at[i]) for i, (a, b) in enumerate(pairs)]
    for c in copies:
        c.start()
    for c in copies:
        c.wait()


def local_step(z_one, z_two, z_small, protos, live_mask):
    f32 = jnp.float32
    bf16 = jnp.bfloat16
    vmem = pl.BlockSpec(memory_space=pltpu.VMEM)
    anym = pl.BlockSpec(memory_space=pl.ANY)
    dma = pltpu.SemaphoreType.DMA
    vm = pltpu.VMEM
    dc, qs, qt, dz, loss = pl.pallas_call(
        kernel,
        out_shape=[vm((KPAD, D), f32), vm((STEPS, 2, ROWS, RW), f32), vm((2, ROWS, QT), f32),
                   vm((VIEWS, ROWS, D), f32), vm((1, 1), f32)],
        in_specs=[vmem] * 4 + [anym],
        out_specs=[vmem] * 5,
        scratch_shapes=[vm((KPAD, D), bf16), vm((2, SH, NS), f32), vm((5, NDEV, 8, 128), f32), vm((NDEV, 32, 128), f32),
                        vm((NDEV, 2, SH), f32), vm((VIEWS, NS, D), bf16), vm((8, NS), f32), vm((8, NS), f32),
                        vm((2, CB, VIEWS * 256), bf16), vm((2, CB, 256), f32),
                        vm((VIEWS * ROWS, RW), bf16), vm((VIEWS * ROWS, D), bf16), vm((2, 128, 8), f32),
                        vm((VIEWS * ROWS + ROWS, D), f32),
                        dma, dma((2,)), dma, dma, dma, dma, dma((5,)), dma((5,)), dma, dma, dma, dma,
                        dma((STEPS, 3)), dma((STEPS, 3)), dma((STEPS, 3)), dma((STEPS, 3))],
        compiler_params=pltpu.CompilerParams(collective_id=0, has_side_effects=True, vmem_limit_bytes=VM),
        name="step",
    )(z_one, z_two, z_small, live_mask.reshape(1, ROWS), protos)
    q1, q2, loss, dz1, dz2, dzs, dc = pl.pallas_call(
        emit_kernel,
        out_shape=[jax.ShapeDtypeStruct((ROWS, KP), f32), jax.ShapeDtypeStruct((ROWS, KP), f32),
                   jax.ShapeDtypeStruct((1, 1), f32), jax.ShapeDtypeStruct((ROWS, D), f32),
                   jax.ShapeDtypeStruct((ROWS, D), f32), jax.ShapeDtypeStruct((6, ROWS, D), f32),
                   jax.ShapeDtypeStruct((KP, D), f32)],
        in_specs=[vmem] * 5,
        out_specs=[anym] * 7,
        scratch_shapes=[dma((3 * STEPS + 4,))],
        compiler_params=pltpu.CompilerParams(vmem_limit_bytes=1024 * 1024),
        name="emit",
    )(dc, qs, qt, dz, loss)
    return q1, q2, loss.reshape(()), dz1, dz2, dzs, dc


def solution(mesh):
    row_spec = P("data", None)
    crop_spec = P(None, "data", None)
    return jax.shard_map(local_step, mesh=mesh,
                         in_specs=(row_spec, row_spec, crop_spec, P(None, None), P("data")),
                         out_specs=(row_spec, row_spec, P(), row_spec, row_spec, crop_spec, P(None, None)),
                         check_vma=False)
```

```python
import jax
import jax.numpy as jnp
from jax import lax
from jax.experimental import pallas as pl
from jax.experimental.pallas import tpu as pltpu
from jax.sharding import PartitionSpec as P

TAU = 0.1
LOG2E = 1.4426950408889634
LN2 = 0.6931471805599453
SCALE = LOG2E / TAU
NDEV = 16
ROWS = 32
NS = 512
VIEWS = 8
D = 128
KP = 30000
SH = 1920
KPAD = SH * NDEV
LAST = KP - SH * (NDEV - 1)
CB = 384
NCH = SH // CB
PAIRS = 14.0
LOGICAL = pl.DeviceIdType.LOGICAL
VM = 36 * 1024 * 1024
RB = 512
NQ = 1
N2 = 2 * (NCH - NQ)
STEPS = N2 + 4 * NQ
PARTS = 15
RPI = KPAD // RB // PARTS
RW = RPI * RB
QT = KP - RW * (PARTS - 1)
LAG2, LAG3 = 3, 7


def dot_nt(a, b):
    return lax.dot_general(a, b, (((1,), (1,)), ((), ())), preferred_element_type=jnp.float32)


def dot_nn(a, b):
    return lax.dot_general(a, b, (((1,), (0,)), ((), ())), preferred_element_type=jnp.float32)


def fold8(x):
    return jnp.sum(x.reshape(x.shape[0] // 8, 8, x.shape[1]), axis=0)


def flip(me, bit):
    return me + bit - 2 * bit * lax.rem(me // bit, 2)


def full_barrier(me):
    barrier = pltpu.get_barrier_semaphore()
    for d in range(1, NDEV):
        pl.semaphore_signal(barrier, inc=1, device_id=lax.rem(me + d, NDEV), device_id_type=LOGICAL)
    pl.semaphore_wait(barrier, NDEV - 1)


def send(src, dst, ssem, rsem, to):
    copy = pltpu.make_async_remote_copy(src_ref=src, dst_ref=dst, send_sem=ssem, recv_sem=rsem,
                                        device_id=to, device_id_type=LOGICAL)
    copy.start()


def drain(ref, sem):
    pltpu.make_async_copy(ref, ref, sem).wait()


def kernel(z1, z2, zs, mask, protos, dc, qs, qt, dz, loss,
           ca, ex, mrows, slots, lslots, wall, zall, arow, brow, gt, xsc, gr, zt, px, zl, cols, acc,
           csem, zsend, zlrecv, zs1recv, zs2send, zs2recv, arsend, arrecv, lsend, lrecv, wsend, wrecv,
           ssem, r2, r3, rs):
    me = lax.axis_index("data")
    cc = pltpu.make_async_copy(protos, ca.at[pl.ds(0, KP)], csem)
    cc.start()
    ca[pl.ds(KP, KPAD - KP), :] = jnp.zeros((KPAD - KP, D), jnp.bfloat16)
    dims = (flip(me, 2), flip(me, 4), flip(me, 8))
    sib = flip(me, 1)
    mpad = jnp.concatenate([mask[...].astype(jnp.float32), jnp.zeros((1, 128 - ROWS), jnp.float32)], axis=1)
    mrows[me] = pltpu.roll(jnp.broadcast_to(mpad, (8, 128)), ROWS * lax.rem(me, 4), 1)[0:1]
    with jax.named_scope("barrier"):
        full_barrier(me)
    myrows = pl.ds(pl.multiple_of(me * ROWS, ROWS), ROWS)

    def ar_send(t):
        for d in range(1, NDEV):
            send(slots.at[t, me], slots.at[t, me], arsend.at[t], arrecv.at[t], lax.rem(me + d, NDEV))

    def ar_total(t):
        drain(slots.at[t, pl.ds(0, NDEV - 1)], arrecv.at[t])
        tot = slots[t, 0]
        for i in range(1, NDEV):
            tot = tot + slots[t, i]
        return tot

    for d in range(1, NDEV):
        to = lax.rem(me + d, NDEV)
        send(z1, zall.at[0, myrows], zsend.at[0], zlrecv, to)
        send(z2, zall.at[1, myrows], zsend.at[0], zlrecv, to)
    for d in range(1, NDEV):
        send(mrows.at[me], mrows.at[me], arsend.at[0], arrecv.at[0], lax.rem(me + d, NDEV))
    for d in range(1, NDEV // 2):
        send(zs, zall.at[pl.ds(2, 6), myrows], zsend.at[1], zs1recv, lax.rem(me + 2 * d, NDEV))
    zall[0, myrows] = z1[...]
    zall[1, myrows] = z2[...]
    zall[pl.ds(2, 6), myrows] = zs[...]
    send(zs, zall.at[pl.ds(2, 6), myrows], zs2send, zs2recv, sib)
    zl[pl.ds(0, ROWS), pl.ds(0, D)] = z1[...]
    zl[pl.ds(ROWS, ROWS), pl.ds(0, D)] = z2[...]
    zl[pl.ds(2 * ROWS, 6 * ROWS), pl.ds(0, D)] = zs[...].reshape(6 * ROWS, D)
    zl[pl.ds(0, 2 * ROWS), pl.ds(D, 128)] = jnp.zeros((2 * ROWS, 128), jnp.bfloat16)
    acc[...] = jnp.zeros_like(acc)
    cc.wait()
    with jax.named_scope("mask"):
        drain(mrows.at[pl.ds(0, NDEV - 1)], arrecv.at[0])
        mask8 = [mrows[4 * j] + mrows[4 * j + 1] + mrows[4 * j + 2] + mrows[4 * j + 3] for j in range(4)]
    mask4 = jnp.concatenate(mask8, axis=0)
    mrow = jnp.concatenate(mask8, axis=1)
    live = jnp.sum(jnp.sum(mask4, axis=1, keepdims=True), axis=0, keepdims=True)
    with jax.named_scope("zlarge"):
        drain(zall.at[pl.ds(0, 2), pl.ds(0, NS - ROWS)], zlrecv)

    def shard(b):
        return ca[pl.ds(pl.multiple_of(me * SH + b * CB, 128), CB)]

    def col_scale(c, b):
        k = me * SH + b * CB + lax.broadcasted_iota(jnp.int32, (CB, 1), 0)
        return jnp.where(k < KP, 1.0 / (KP * c), 0.0)

    zero8 = jnp.zeros((8, NS), jnp.float32)

    def first(b, carry):
        rows = pl.ds(b * CB, CB)
        out = []
        for v in range(2):
            ps, r = carry[2 * v], carry[2 * v + 1]
            p = jnp.exp2(dot_nt(shard(b), zall[v]) * SCALE)
            ps = ps + fold8(p)
            e = p * p * mrow
            ex[v, rows] = e
            w = col_scale(jnp.sum(e, axis=1, keepdims=True), b)
            r = r + fold8(e * w)
            out += [ps, r]
        return tuple(out)

    def put(t, r1, r2):
        for v, r in enumerate((r1, r2)):
            row = jnp.sum(r, axis=0, keepdims=True)
            for j in range(4):
                slots[t, me, pl.ds(4 * v + j, 1)] = row[:, 128 * j:128 * (j + 1)]

    def scale_rows(tot):
        us = []
        for v in range(2):
            r = jnp.concatenate([tot[4 * v + j:4 * v + j + 1] for j in range(4)], axis=1)
            us.append(mrow / (live * jnp.where(mrow > 0, r, 1.0)))
        return us

    pad = jnp.where(me == NDEV - 1, float(SH - LAST), 0.0)

    def put_lse(v, ps):
        row = jnp.sum(ps, axis=0, keepdims=True) - pad
        for j in range(4):
            lslots[me, pl.ds(4 * v + j, 1)] = row[:, 128 * j:128 * (j + 1)]

    with jax.named_scope("first"):
        carry = (zero8,) * 4
        for b in range(NCH):
            carry = first(b, carry)
        ps1, r1, ps2, rr2 = carry
        put(1, r1, rr2)
        ar_send(1)
    put_lse(0, ps1)
    put_lse(1, ps2)
    with jax.named_scope("zsmall1"):
        drain(zall.at[pl.ds(2, 6), pl.ds(0, 7 * ROWS)], zs1recv)
    for d in range(1, NDEV // 2):
        rows = pl.ds(pl.multiple_of(lax.rem(me + 2 * d, NDEV) * ROWS, ROWS), ROWS)
        send(zall.at[pl.ds(2, 6), rows], zall.at[pl.ds(2, 6), rows], zs2send, zs2recv, sib)
    def small(i, carry):
        v = 2 + i
        ps = zero8
        for b in range(NCH):
            ps = ps + fold8(jnp.exp2(dot_nt(shard(b), zall[v]) * SCALE))
        put_lse(v, ps)
        return carry

    with jax.named_scope("zsmall2"):
        drain(zall.at[pl.ds(2, 6), pl.ds(0, 8 * ROWS)], zs2recv)

    with jax.named_scope("small"):
        lax.fori_loop(0, 3, small, 0)
    with jax.named_scope("ar1"):
        us = scale_rows(ar_total(1))

    def again(us, last):
        def step(b, carry):
            rows = pl.ds(pl.multiple_of(b * CB, CB), CB)
            out = []
            for v in range(2):
                e = ex[v, rows]
                w = col_scale(jnp.sum(e * us[v], axis=1, keepdims=True), b)
                out.append(carry[v] + fold8(e * w))
                if last:
                    for q in range(CB // 128):
                        wt = jnp.broadcast_to(w[128 * q:128 * (q + 1)], (128, 128)).T
                        wall[me, pl.ds(v, 1), pl.ds(pl.multiple_of(b * CB + 128 * q, 128), 128)] = wt[0:1]
            return tuple(out)
        return step

    with jax.named_scope("again2"):
        r1, rr2 = lax.fori_loop(0, NCH, again(us, False), (zero8, zero8))
        put(2, r1, rr2)
        ar_send(2)
    with jax.named_scope("small"):
        lax.fori_loop(3, 6, small, 0)
        for d in range(1, NDEV):
            send(lslots.at[me], lslots.at[me], lsend, lrecv, lax.rem(me + d, NDEV))
    with jax.named_scope("ar2"):
        us = scale_rows(ar_total(2))
    with jax.named_scope("again3"):
        r1, rr2 = lax.fori_loop(0, NCH, again(us, True), (zero8, zero8))
        put(3, r1, rr2)
        ar_send(3)
        for d in range(1, NDEV):
            send(wall.at[me], wall.at[me], wsend, wrecv, lax.rem(me + d, NDEV))
    gsc = 1.0 / (TAU * PAIRS * live)
    with jax.named_scope("lse"):
        drain(lslots.at[pl.ds(0, NDEV - 1)], lrecv)
        tot = lslots[0]
        for i in range(1, NDEV):
            tot = tot + lslots[i]
        logs = jnp.log(tot)
        inv = 1.0 / tot[0:8]
        for v in range(2):
            for j in range(4):
                arow[v:v + 1, 128 * j:128 * (j + 1)] = gsc * (mask8[j] * inv[4 * v + j:4 * v + j + 1])
        lg2 = jnp.log(2.0 * gsc)
        lsum = jnp.sum(jnp.sum(jnp.concatenate([mask4] * 2, axis=0) * logs[0:8], axis=1, keepdims=True), axis=0, keepdims=True)
        lsum = lsum + (12.0 * live) * lg2
        rest_ = jnp.where(jnp.concatenate([mask4] * 8, axis=0) > 0, TAU * (lg2 - logs), -100.0)
        for k in range(3):
            piece_ = rest_.astype(jnp.bfloat16).astype(jnp.float32)
            px[k] = piece_
            rest_ = rest_ - piece_
        for j in range(4):
            block = jnp.concatenate([px[k, pl.ds(8 + j, 6, 4)] for k in range(3)] + [jnp.zeros((110, 128), jnp.float32)], axis=0)
            zt[pl.ds(128 * j, 128)] = block.T.astype(jnp.bfloat16)
        lane = lax.broadcasted_iota(jnp.int32, (ROWS, 128), 1)
        own_rows = zt[myrows].astype(jnp.float32)
        for v in range(2, VIEWS):
            pick = jnp.where(jnp.logical_and(lax.rem(lane, 6) == v - 2, lane < 18), own_rows, 0.0)
            zl[pl.ds(v * ROWS, ROWS), pl.ds(D, 128)] = pick.astype(jnp.bfloat16)
    with jax.named_scope("ar3"):
        us = scale_rows(ar_total(3))
    for v in range(2):
        brow[v:v + 1] = live * us[v]
    brow[2:8] = jnp.zeros((6, NS), jnp.float32)
    arow[2:8] = jnp.zeros((6, NS), jnp.float32)
    tile = pl.ds(pl.multiple_of((me // 4) * 128, 128), 128)
    cols[0] = arow[:, tile].T
    cols[1] = brow[:, tile].T
    mine = pl.ds(pl.multiple_of(lax.rem(me, 4) * ROWS, ROWS), ROWS)

    def piece_row(owner, t, a):
        return pl.multiple_of(owner * SH + t * CB + a * 128, 128)

    def parts_of(it):
        quad = (it + 8 - N2) // 8
        t = (1 - quad) * (it // 2) + quad * (NCH - NQ + (it - N2) // 4)
        par = (1 - quad) * lax.rem(it, 2) + quad * lax.rem(it + 4 - N2 % 4, 4)
        return t, par

    def push(owner, it, a, to, rsem):
        ref = dc.at[pl.ds(piece_row(owner, parts_of(it)[0], a), 128)]
        send(ref, ref, ssem.at[it, a], rsem.at[it, a], to)

    def order(a):
        return dims[a], dims[(a + 1) % 3], dims[(a + 2) % 3]

    def owner_of(holder, a, it):
        d0, d1, _ = order(a)
        par = parts_of(it)[1]
        return holder + lax.rem(par, 2) * (d0 - me) + (par // 2) * (d1 - me)

    def chunk(it):
        t = parts_of(it)[0]
        owners = [owner_of(me, a, it) for a in range(3)]
        c = jnp.concatenate([ca[pl.ds(piece_row(owners[a], t, a), 128)] for a in range(3)], axis=0)
        wc = []
        for v in range(2):
            parts = []
            for a in range(3):
                off = pl.multiple_of(t * CB + a * 128, 128)
                row = wall[owners[a], pl.ds(v, 1), pl.ds(off, 128)] * gsc
                parts.append(jnp.broadcast_to(row, (128, 128)).T)
            wc.append(jnp.concatenate(parts, axis=0))
        QR = 32
        lanes = lax.broadcasted_iota(jnp.int32, (CB, 128), 1)
        HALF = CB // 2
        LW = 256

        def put_g(v, q, l, g):
            gt[v // 4, pl.ds(QR * q, QR), pl.ds((v % 4) * NS + LW * l, LW)] = g.astype(jnp.bfloat16)

        def dc_part(h):
            zz = zall[pl.ds(4 * h, 4)].reshape(4 * NS, D)
            return [dot_nn(gt[h, pl.ds(HALF * m, HALF)], zz) for m in range(2)]

        def rows_of(ref, v, l):
            return ref[v:v + 1, LW * l:LW * (l + 1)]

        s0 = dot_nt(c, zall[0])
        s1 = dot_nt(c, zall[1])
        for l in range(NS // LW):
            b0, b1, a0, a1 = rows_of(brow, 0, l), rows_of(brow, 1, l), rows_of(arow, 0, l), rows_of(arow, 1, l)
            ln = slice(LW * l, LW * (l + 1))
            for q in range(CB // QR):
                sl = slice(QR * q, QR * (q + 1))
                p0 = jnp.exp2(s0[sl, ln] * SCALE)
                p1 = jnp.exp2(s1[sl, ln] * SCALE)
                x0 = (p0 * p0) * b0 * jnp.concatenate([wc[0][sl]] * 2, axis=1)
                x1 = (p1 * p1) * b1 * jnp.concatenate([wc[1][sl]] * 2, axis=1)
                xsc[pl.ds(QR * q, QR), pl.ds(LW * l, LW)] = x0 + x1
                put_g(0, q, l, p0 * a0 - x1)
                put_g(1, q, l, p1 * a1 - x0)
        res = None
        for v in range(2, VIEWS):
            sel = jnp.where(jnp.logical_and(lax.rem(lanes, 6) == v - 2, lanes < 18), 1.0, 0.0).astype(jnp.bfloat16)
            s = dot_nt(jnp.concatenate([c, sel], axis=1), jnp.concatenate([zall[v], zt[...]], axis=1))
            for l in range(NS // LW):
                ln = slice(LW * l, LW * (l + 1))
                for q in range(CB // QR):
                    sl = slice(QR * q, QR * (q + 1))
                    put_g(v, q, l, jnp.exp2(s[sl, ln] * SCALE) - xsc[pl.ds(QR * q, QR), pl.ds(LW * l, LW)])
            if v == 3:
                res = dc_part(0)
        more = dc_part(1)
        out = jnp.concatenate([res[0] + more[0], res[1] + more[1]], axis=0)
        for a in range(3):
            dc[pl.ds(piece_row(owners[a], t, a), 128)] = out[128 * a:128 * (a + 1)]

    def rows_part(i):
        ac = cols[0, mine]
        bc = cols[1, mine]
        lanes = lax.broadcasted_iota(jnp.int32, (RB, 128), 1)
        ones = jnp.where(lanes < 18, 1.0, 0.0).astype(jnp.bfloat16)
        for h in range(RPI):
            jb = i * RPI + h
            c = ca[pl.ds(pl.multiple_of(jb * RB, RB), RB)]
            s = dot_nt(zl[...], jnp.concatenate([c, ones], axis=1)) * SCALE
            wr = []
            for v in range(2):
                parts = []
                for q in range(RB // 128):
                    b = jb * (RB // 128) + q
                    parts.append(wall[b // (SH // 128), pl.ds(v, 1), pl.ds(pl.multiple_of(lax.rem(b, SH // 128) * 128, 128), 128)])
                wr.append(jnp.concatenate(parts, axis=1))
            sv = [s[ROWS * v:ROWS * (v + 1)] for v in range(VIEWS)]
            p0 = jnp.exp2(sv[0])
            p1 = jnp.exp2(sv[1])
            o0 = (p0 * p0) * bc[:, 0:1] * wr[0]
            o1 = (p1 * p1) * bc[:, 1:2] * wr[1]
            col = pl.ds(h * RB, RB)
            qs[i, 0, :, col] = o0
            qs[i, 1, :, col] = o1
            x0 = o0 * gsc
            x1 = o1 * gsc
            xs = x0 + x1
            gr[pl.ds(0, ROWS), col] = (p0 * ac[:, 0:1] - x1).astype(jnp.bfloat16)
            gr[pl.ds(ROWS, ROWS), col] = (p1 * ac[:, 1:2] - x0).astype(jnp.bfloat16)
            ssum = sv[2]
            for v in range(3, VIEWS):
                ssum = ssum + sv[v]
            for v in range(2, VIEWS):
                gr[pl.ds(v * ROWS, ROWS), col] = (jnp.exp2(sv[v]) - xs).astype(jnp.bfloat16)
            ls = x1 * sv[0] + x0 * sv[1] + xs * ssum
            part = ls[:, 0:128]
            for q in range(1, RB // 128):
                part = part + ls[:, 128 * q:128 * (q + 1)]
            acc[pl.ds(VIEWS * ROWS, ROWS)] += part
        cs = ca[pl.ds(pl.multiple_of(i * RW, RW), RW)]
        acc[pl.ds(0, VIEWS * ROWS)] += dot_nn(gr[...], cs)

    def own(it):
        for a in range(3):
            o = owner_of(me, a, it)
            push(o, it, a, order(a)[2], r3)
            push(o, it, a, sib, rs)

    def own1(it):
        for a in range(3):
            push(owner_of(me, a, it), it, a, order(a)[1], r2)

    def serve2(it):
        for a in range(3):
            d0, d1, d2 = order(a)
            drain(dc.at[pl.ds(0, 128)], r2.at[it, a])
            o = owner_of(d1, a, it)
            push(o, it, a, d2, r3)
            push(o, it, a, sib, rs)

    def serve3(it):
        @pl.when(it < N2)
        def _():
            for a in range(3):
                d0, d1, d2 = order(a)
                drain(dc.at[pl.ds(0, 256)], r3.at[it, a])
                for holder in (d2, d2 + d1 - me):
                    push(owner_of(holder, a, it), it, a, sib, rs)

        @pl.when(it >= N2)
        def _():
            for a in range(3):
                drain(dc.at[pl.ds(0, 128)], r3.at[it, a])
                push(owner_of(order(a)[2], a, it), it, a, sib, rs)

    with jax.named_scope("chunk0"):
        chunk(0)
    own1(0)
    own(0)
    with jax.named_scope("wait_w"):
        drain(wall.at[pl.ds(0, NDEV - 1)], wrecv)

    def main(it, carry):
        with jax.named_scope("compute"):
            chunk(it)
            rows_part(it - 1)

        @pl.when(it < N2)
        def _():
            own1(it)

        own(it)

        @pl.when(jnp.logical_and(it >= LAG2, it < LAG2 + N2))
        def _():
            with jax.named_scope("serve2"):
                serve2(it - LAG2)

        @pl.when(it >= LAG3)
        def _():
            with jax.named_scope("serve3"):
                serve3(it - LAG3)

        return carry

    lax.fori_loop(1, STEPS, main, 0)

    def rest(i, carry):
        with jax.named_scope("rows"):
            rows_part(i)
        return carry

    lax.fori_loop(STEPS - 1, PARTS, rest, 0)
    for v in range(2):
        qt[v] = qs[PARTS - 1, v, :, pl.ds(0, QT)]
    total = jnp.sum(jnp.sum(acc[pl.ds(VIEWS * ROWS, ROWS)], axis=1, keepdims=True), axis=0, keepdims=True)
    slots[4, me] = jnp.broadcast_to(total, (8, 128))
    ar_send(4)

    def last(it, carry):
        with jax.named_scope("serve3"):
            serve3(it)
        return carry

    lax.fori_loop(STEPS - LAG3, STEPS, last, 0)
    dz[...] = acc[pl.ds(0, VIEWS * ROWS)].reshape(VIEWS, ROWS, D)
    with jax.named_scope("loss"):
        tot = ar_total(4)
    cross = tot[0:1, 0:1] * (LN2 * TAU * PAIRS) * live - lsum
    loss[...] = -cross / (live * PAIRS)

    def finish(it, carry):
        @pl.when(it < N2)
        def _():
            for a in range(3):
                drain(dc.at[pl.ds(0, 4 * 128)], rs.at[it, a])
                drain(dc.at[pl.ds(0, 7 * 128)], ssem.at[it, a])

        @pl.when(it >= N2)
        def _():
            for a in range(3):
                drain(dc.at[pl.ds(0, 2 * 128)], rs.at[it, a])
                drain(dc.at[pl.ds(0, 3 * 128)], ssem.at[it, a])
        return carry

    with jax.named_scope("finish"):
        lax.fori_loop(0, STEPS, finish, 0)
    drain(zall.at[pl.ds(0, 2), pl.ds(0, NS - ROWS)], zsend.at[0])
    drain(zall.at[pl.ds(2, 6), pl.ds(0, 7 * ROWS)], zsend.at[1])
    drain(zall.at[pl.ds(2, 6), pl.ds(0, 8 * ROWS)], zs2send)
    drain(mrows.at[pl.ds(0, NDEV - 1)], arsend.at[0])
    for t in range(1, 5):
        drain(slots.at[t, pl.ds(0, NDEV - 1)], arsend.at[t])
    drain(lslots.at[pl.ds(0, NDEV - 1)], lsend)
    drain(wall.at[pl.ds(0, NDEV - 1)], wsend)


def emit_kernel(dc, qs, qt, dz, loss, o_q1, o_q2, o_loss, o_z1, o_z2, o_zs, o_dc, sem):
    pairs = []
    for i in range(PARTS):
        for v, o in enumerate((o_q1, o_q2)):
            if i < PARTS - 1:
                pairs.append((qs.at[i, v], o.at[:, pl.ds(i * RW, RW)]))
            else:
                pairs.append((qt.at[v], o.at[:, pl.ds(i * RW, QT)]))
        rows = pl.ds(i * RW, RW if i < PARTS - 1 else QT)
        pairs.append((dc.at[rows], o_dc.at[rows]))
    pairs += [(loss, o_loss), (dz.at[0], o_z1), (dz.at[1], o_z2), (dz.at[pl.ds(2, 6)], o_zs)]
    copies = [pltpu.make_async_copy(a, b, sem.at[i]) for i, (a, b) in enumerate(pairs)]
    for c in copies:
        c.start()
    for c in copies:
        c.wait()


def local_step(z_one, z_two, z_small, protos, live_mask):
    f32 = jnp.float32
    bf16 = jnp.bfloat16
    vmem = pl.BlockSpec(memory_space=pltpu.VMEM)
    anym = pl.BlockSpec(memory_space=pl.ANY)
    dma = pltpu.SemaphoreType.DMA
    vm = pltpu.VMEM
    dc, qs, qt, dz, loss = pl.pallas_call(
        kernel,
        out_shape=[vm((KPAD, D), f32), vm((PARTS, 2, ROWS, RW), f32), vm((2, ROWS, QT), f32),
                   vm((VIEWS, ROWS, D), f32), vm((1, 1), f32)],
        in_specs=[vmem] * 4 + [anym],
        out_specs=[vmem] * 5,
        scratch_shapes=[vm((KPAD, D), bf16), vm((2, SH, NS), f32), vm((NDEV, 1, 128), f32), vm((5, NDEV, 8, 128), f32), vm((NDEV, 32, 128), f32),
                        vm((NDEV, 2, SH), f32), vm((VIEWS, NS, D), bf16), vm((8, NS), f32), vm((8, NS), f32),
                        vm((2, CB, 4 * NS), bf16), vm((CB, NS), f32),
                        vm((VIEWS * ROWS, RW), bf16), vm((NS, 128), bf16), vm((3, 32, 128), f32), vm((VIEWS * ROWS, 2 * D), bf16),
                        vm((2, 128, 8), f32),
                        vm((VIEWS * ROWS + ROWS, D), f32),
                        dma, dma((2,)), dma, dma, dma, dma, dma((5,)), dma((5,)), dma, dma, dma, dma,
                        dma((STEPS, 3)), dma((STEPS, 3)), dma((STEPS, 3)), dma((STEPS, 3))],
        compiler_params=pltpu.CompilerParams(collective_id=0, has_side_effects=True, vmem_limit_bytes=VM),
        name="step",
    )(z_one, z_two, z_small, live_mask.reshape(1, ROWS), protos)
    q1, q2, loss, dz1, dz2, dzs, dc = pl.pallas_call(
        emit_kernel,
        out_shape=[jax.ShapeDtypeStruct((ROWS, KP), f32), jax.ShapeDtypeStruct((ROWS, KP), f32),
                   jax.ShapeDtypeStruct((1, 1), f32), jax.ShapeDtypeStruct((ROWS, D), f32),
                   jax.ShapeDtypeStruct((ROWS, D), f32), jax.ShapeDtypeStruct((6, ROWS, D), f32),
                   jax.ShapeDtypeStruct((KP, D), f32)],
        in_specs=[vmem] * 5,
        out_specs=[anym] * 7,
        scratch_shapes=[dma((3 * PARTS + 4,))],
        compiler_params=pltpu.CompilerParams(vmem_limit_bytes=1024 * 1024),
        name="emit",
    )(dc, qs, qt, dz, loss)
    return q1, q2, loss.reshape(()), dz1, dz2, dzs, dc


def solution(mesh):
    row_spec = P("data", None)
    crop_spec = P(None, "data", None)
    return jax.shard_map(local_step, mesh=mesh,
                         in_specs=(row_spec, row_spec, crop_spec, P(None, None), P("data")),
                         out_specs=(row_spec, row_spec, P(), row_spec, row_spec, crop_spec, P(None, None)),
                         check_vma=False)
```

```python
import jax
import jax.numpy as jnp
from jax import lax
from jax.experimental import pallas as pl
from jax.experimental.pallas import tpu as pltpu
from jax.sharding import PartitionSpec as P

TAU = 0.1
LOG2E = 1.4426950408889634
LN2 = 0.6931471805599453
SCALE = LOG2E / TAU
NDEV = 16
ROWS = 32
NS = 512
VIEWS = 8
D = 128
KP = 30000
SH = 1920
KPAD = SH * NDEV
LAST = KP - SH * (NDEV - 1)
CB = 384
NCH = SH // CB
PAIRS = 14.0
LOGICAL = pl.DeviceIdType.LOGICAL
VM = 36 * 1024 * 1024
RB = 512
NQ = 1
N2 = 2 * (NCH - NQ)
STEPS = N2 + 4 * NQ
PARTS = 15
RPI = KPAD // RB // PARTS
RW = RPI * RB
QT = KP - RW * (PARTS - 1)
LAG2, LAG3 = 3, 7
LANE = 128
OTHERS = NDEV - 1
CROPS = pl.ds(2, 6)
SMALL = range(2, VIEWS)
PEERS = range(1, NDEV)
PEERS_HALF = range(1, NDEV // 2)
QR, LW = 32, 256


def dot_nt(a, b):
    return lax.dot_general(a, b, (((1,), (1,)), ((), ())), preferred_element_type=jnp.float32)


def dot_nn(a, b):
    return lax.dot_general(a, b, (((1,), (0,)), ((), ())), preferred_element_type=jnp.float32)


def fold8(x):
    return jnp.sum(x.reshape(x.shape[0] // 8, 8, x.shape[1]), axis=0)


def flip(me, bit):
    return me + bit - 2 * bit * lax.rem(me // bit, 2)


def full_barrier(me):
    barrier = pltpu.get_barrier_semaphore()
    for d in PEERS:
        pl.semaphore_signal(barrier, inc=1, device_id=lax.rem(me + d, NDEV), device_id_type=LOGICAL)
    pl.semaphore_wait(barrier, OTHERS)


def send(src, dst, ssem, rsem, to):
    copy = pltpu.make_async_remote_copy(src_ref=src, dst_ref=dst, send_sem=ssem, recv_sem=rsem,
                                        device_id=to, device_id_type=LOGICAL)
    copy.start()


def drain(ref, sem):
    pltpu.make_async_copy(ref, ref, sem).wait()


def kernel(z1, z2, zs, mask, protos, dc, qs, qt, dz, loss,
           ca, ex, mrows, slots, lslots, wall, zall, arow, brow, gt, xsc, gr, zt, px, zl, cols, acc,
           csem, zsend, zlrecv, zs1recv, zs2send, zs2recv, arsend, arrecv, lsend, lrecv, wsend, wrecv,
           ssem, r2, r3, rs):
    me = lax.axis_index("data")
    cc = pltpu.make_async_copy(protos, ca.at[pl.ds(0, KP)], csem)
    cc.start()
    ca[pl.ds(KP, KPAD - KP), :] = jnp.zeros((KPAD - KP, D), jnp.bfloat16)
    dims = (flip(me, 2), flip(me, 4), flip(me, 8))
    sib = flip(me, 1)
    mpad = jnp.concatenate([mask[...].astype(jnp.float32), jnp.zeros((1, LANE - ROWS), jnp.float32)], axis=1)
    mrows[me] = pltpu.roll(jnp.broadcast_to(mpad, (8, LANE)), ROWS * lax.rem(me, 4), 1)[0:1]
    with jax.named_scope("barrier"):
        full_barrier(me)
    myrows = pl.ds(pl.multiple_of(me * ROWS, ROWS), ROWS)

    def ar_send(t):
        for d in PEERS:
            send(slots.at[t, me], slots.at[t, me], arsend.at[t], arrecv.at[t], lax.rem(me + d, NDEV))

    def ar_total(t):
        drain(slots.at[t, pl.ds(0, OTHERS)], arrecv.at[t])
        tot = slots[t, 0]
        for i in PEERS:
            tot = tot + slots[t, i]
        return tot

    for d in PEERS:
        to = lax.rem(me + d, NDEV)
        send(z1, zall.at[0, myrows], zsend.at[0], zlrecv, to)
        send(z2, zall.at[1, myrows], zsend.at[0], zlrecv, to)
    for d in PEERS:
        send(mrows.at[me], mrows.at[me], arsend.at[0], arrecv.at[0], lax.rem(me + d, NDEV))
    for d in PEERS_HALF:
        send(zs, zall.at[CROPS, myrows], zsend.at[1], zs1recv, lax.rem(me + 2 * d, NDEV))
    zall[0, myrows] = z1[...]
    zall[1, myrows] = z2[...]
    zall[CROPS, myrows] = zs[...]
    send(zs, zall.at[CROPS, myrows], zs2send, zs2recv, sib)
    zl[pl.ds(0, ROWS), pl.ds(0, D)] = z1[...]
    zl[pl.ds(ROWS, ROWS), pl.ds(0, D)] = z2[...]
    zl[pl.ds(2 * ROWS, 6 * ROWS), pl.ds(0, D)] = zs[...].reshape(6 * ROWS, D)
    zl[pl.ds(0, 2 * ROWS), pl.ds(D, LANE)] = jnp.zeros((2 * ROWS, LANE), jnp.bfloat16)
    acc[...] = jnp.zeros_like(acc)
    cc.wait()
    with jax.named_scope("mask"):
        drain(mrows.at[pl.ds(0, OTHERS)], arrecv.at[0])
        mask8 = [mrows[4 * j] + mrows[4 * j + 1] + mrows[4 * j + 2] + mrows[4 * j + 3] for j in range(4)]
    mask4 = jnp.concatenate(mask8, axis=0)
    mrow = jnp.concatenate(mask8, axis=1)
    live = jnp.sum(jnp.sum(mask4, axis=1, keepdims=True), axis=0, keepdims=True)
    with jax.named_scope("zlarge"):
        drain(zall.at[pl.ds(0, 2), pl.ds(0, NS - ROWS)], zlrecv)

    def shard(b):
        return ca[pl.ds(pl.multiple_of(me * SH + b * CB, LANE), CB)]

    def col_scale(c, b):
        k = me * SH + b * CB + lax.broadcasted_iota(jnp.int32, (CB, 1), 0)
        return jnp.where(k < KP, 1.0 / (KP * c), 0.0)

    zero8 = jnp.zeros((8, NS), jnp.float32)

    def first(b, carry):
        rows = pl.ds(b * CB, CB)
        out = []
        for v in range(2):
            ps, r = carry[2 * v], carry[2 * v + 1]
            p = jnp.exp2(dot_nt(shard(b), zall[v]) * SCALE)
            ps = ps + fold8(p)
            e = p * p * mrow
            ex[v, rows] = e
            w = col_scale(jnp.sum(e, axis=1, keepdims=True), b)
            r = r + fold8(e * w)
            out += [ps, r]
        return tuple(out)

    def put(t, r1, r2):
        for v, r in enumerate((r1, r2)):
            row = jnp.sum(r, axis=0, keepdims=True)
            for j in range(4):
                slots[t, me, pl.ds(4 * v + j, 1)] = row[:, LANE * j:LANE * (j + 1)]

    def scale_rows(tot):
        us = []
        for v in range(2):
            r = jnp.concatenate([tot[4 * v + j:4 * v + j + 1] for j in range(4)], axis=1)
            us.append(mrow / (live * jnp.where(mrow > 0, r, 1.0)))
        return us

    pad = jnp.where(me == OTHERS, float(SH - LAST), 0.0)

    def put_lse(v, ps):
        row = jnp.sum(ps, axis=0, keepdims=True) - pad
        for j in range(4):
            lslots[me, pl.ds(4 * v + j, 1)] = row[:, LANE * j:LANE * (j + 1)]

    with jax.named_scope("first"):
        carry = (zero8,) * 4
        for b in range(NCH):
            carry = first(b, carry)
        ps1, r1, ps2, rr2 = carry
        put(1, r1, rr2)
        ar_send(1)
    put_lse(0, ps1)
    put_lse(1, ps2)
    with jax.named_scope("zsmall1"):
        drain(zall.at[CROPS, pl.ds(0, 7 * ROWS)], zs1recv)
    for d in PEERS_HALF:
        rows = pl.ds(pl.multiple_of(lax.rem(me + 2 * d, NDEV) * ROWS, ROWS), ROWS)
        send(zall.at[CROPS, rows], zall.at[CROPS, rows], zs2send, zs2recv, sib)

    def small(i, carry):
        v = 2 + i
        ps = zero8
        for b in range(NCH):
            ps = ps + fold8(jnp.exp2(dot_nt(shard(b), zall[v]) * SCALE))
        put_lse(v, ps)
        return carry

    with jax.named_scope("zsmall2"):
        drain(zall.at[CROPS, pl.ds(0, 8 * ROWS)], zs2recv)

    with jax.named_scope("small"):
        lax.fori_loop(0, 3, small, 0)
    with jax.named_scope("ar1"):
        us = scale_rows(ar_total(1))

    def again(us, last):
        def step(b, carry):
            rows = pl.ds(pl.multiple_of(b * CB, CB), CB)
            out = []
            for v in range(2):
                e = ex[v, rows]
                w = col_scale(jnp.sum(e * us[v], axis=1, keepdims=True), b)
                out.append(carry[v] + fold8(e * w))
                if last:
                    for q in range(CB // LANE):
                        wt = jnp.broadcast_to(w[LANE * q:LANE * (q + 1)], (LANE, LANE)).T
                        wall[me, pl.ds(v, 1), pl.ds(pl.multiple_of(b * CB + LANE * q, LANE), LANE)] = wt[0:1]
            return tuple(out)
        return step

    with jax.named_scope("again2"):
        r1, rr2 = lax.fori_loop(0, NCH, again(us, False), (zero8, zero8))
        put(2, r1, rr2)
        ar_send(2)
    with jax.named_scope("small"):
        lax.fori_loop(3, 6, small, 0)
        for d in PEERS:
            send(lslots.at[me], lslots.at[me], lsend, lrecv, lax.rem(me + d, NDEV))
    with jax.named_scope("ar2"):
        us = scale_rows(ar_total(2))
    with jax.named_scope("again3"):
        r1, rr2 = lax.fori_loop(0, NCH, again(us, True), (zero8, zero8))
        put(3, r1, rr2)
        ar_send(3)
        for d in PEERS:
            send(wall.at[me], wall.at[me], wsend, wrecv, lax.rem(me + d, NDEV))
    gsc = 1.0 / (TAU * PAIRS * live)
    with jax.named_scope("lse"):
        drain(lslots.at[pl.ds(0, OTHERS)], lrecv)
        tot = lslots[0]
        for i in PEERS:
            tot = tot + lslots[i]
        logs = jnp.log(tot)
        inv = 1.0 / tot[0:8]
        for v in range(2):
            for j in range(4):
                arow[v:v + 1, LANE * j:LANE * (j + 1)] = gsc * (mask8[j] * inv[4 * v + j:4 * v + j + 1])
        lg2 = jnp.log(2.0 * gsc)
        lsum = jnp.sum(jnp.sum(jnp.concatenate([mask4] * 2, axis=0) * logs[0:8], axis=1, keepdims=True), axis=0, keepdims=True)
        lsum = lsum + (12.0 * live) * lg2
        rest_ = jnp.where(jnp.concatenate([mask4] * 8, axis=0) > 0, TAU * (lg2 - logs), -100.0)
        for k in range(3):
            piece_ = rest_.astype(jnp.bfloat16).astype(jnp.float32)
            px[k] = piece_
            rest_ = rest_ - piece_
        for j in range(4):
            block = jnp.concatenate([px[k, pl.ds(8 + j, 6, 4)] for k in range(3)] + [jnp.zeros((110, LANE), jnp.float32)], axis=0)
            zt[pl.ds(LANE * j, LANE)] = block.T.astype(jnp.bfloat16)
        lane = lax.broadcasted_iota(jnp.int32, (ROWS, LANE), 1)
        own_rows = zt[myrows].astype(jnp.float32)
        for v in SMALL:
            pick = jnp.where(jnp.logical_and(lax.rem(lane, 6) == v - 2, lane < 18), own_rows, 0.0)
            zl[pl.ds(v * ROWS, ROWS), pl.ds(D, LANE)] = pick.astype(jnp.bfloat16)
    def probs(c, v):
        if v < 2:
            return dot_nt(c, zall[v])
        lanes = lax.broadcasted_iota(jnp.int32, (CB, LANE), 1)
        sel = jnp.where(jnp.logical_and(lax.rem(lanes, 6) == v - 2, lanes < 18), 1.0, 0.0).astype(jnp.bfloat16)
        return dot_nt(jnp.concatenate([c, sel], axis=1), jnp.concatenate([zall[v], zt[...]], axis=1))

    with jax.named_scope("ahead"):
        for v in range(VIEWS):
            ex[v % 2, pl.ds(v // 2 * CB, CB)] = jnp.exp2(probs(shard(0), v) * SCALE)
    with jax.named_scope("ar3"):
        us = scale_rows(ar_total(3))
    for v in range(2):
        brow[v:v + 1] = live * us[v]
    brow[2:8] = jnp.zeros((6, NS), jnp.float32)
    arow[2:8] = jnp.zeros((6, NS), jnp.float32)
    tile = pl.ds(pl.multiple_of((me // 4) * LANE, LANE), LANE)
    cols[0] = arow[:, tile].T
    cols[1] = brow[:, tile].T
    mine = pl.ds(pl.multiple_of(lax.rem(me, 4) * ROWS, ROWS), ROWS)

    def piece_row(owner, t, a):
        return pl.multiple_of(owner * SH + t * CB + a * LANE, LANE)

    def parts_of(it):
        quad = (it + 8 - N2) // 8
        t = (1 - quad) * (it // 2) + quad * (NCH - NQ + (it - N2) // 4)
        par = (1 - quad) * lax.rem(it, 2) + quad * lax.rem(it + 4 - N2 % 4, 4)
        return t, par

    def push(owner, it, a, to, rsem):
        ref = dc.at[pl.ds(piece_row(owner, parts_of(it)[0], a), LANE)]
        send(ref, ref, ssem.at[it, a], rsem.at[it, a], to)

    def order(a):
        return dims[a], dims[(a + 1) % 3], dims[(a + 2) % 3]

    def owner_of(holder, a, it):
        d0, d1, _ = order(a)
        par = parts_of(it)[1]
        return holder + lax.rem(par, 2) * (d0 - me) + (par // 2) * (d1 - me)

    def chunk(it, ready=False):
        t = parts_of(it)[0]
        owners = [owner_of(me, a, it) for a in range(3)]
        c = jnp.concatenate([ca[pl.ds(piece_row(owners[a], t, a), LANE)] for a in range(3)], axis=0)
        wc = []
        for v in range(2):
            parts = []
            for a in range(3):
                off = pl.multiple_of(t * CB + a * LANE, LANE)
                row = wall[owners[a], pl.ds(v, 1), pl.ds(off, LANE)] * gsc
                parts.append(jnp.broadcast_to(row, (LANE, LANE)).T)
            wc.append(jnp.concatenate(parts, axis=0))
        HALF = CB // 2

        def prob_at(s, v, q, l):
            if ready:
                return ex[v % 2, pl.ds(v // 2 * CB + QR * q, QR), pl.ds(LW * l, LW)]
            return jnp.exp2(s[QR * q:QR * (q + 1), LW * l:LW * (l + 1)] * SCALE)

        def put_g(v, q, l, g):
            gt[v // 4, pl.ds(QR * q, QR), pl.ds((v % 4) * NS + LW * l, LW)] = g.astype(jnp.bfloat16)

        def dc_part(h):
            zz = zall[pl.ds(4 * h, 4)].reshape(4 * NS, D)
            return [dot_nn(gt[h, pl.ds(HALF * m, HALF)], zz) for m in range(2)]

        def rows_of(ref, v, l):
            return ref[v:v + 1, LW * l:LW * (l + 1)]

        e0 = probs(c, 0) if not ready else None
        e1 = probs(c, 1) if not ready else None
        for l in range(NS // LW):
            b0, b1, a0, a1 = rows_of(brow, 0, l), rows_of(brow, 1, l), rows_of(arow, 0, l), rows_of(arow, 1, l)
            for q in range(CB // QR):
                sl = slice(QR * q, QR * (q + 1))
                p0 = prob_at(e0, 0, q, l)
                p1 = prob_at(e1, 1, q, l)
                x0 = (p0 * p0) * b0 * jnp.concatenate([wc[0][sl]] * 2, axis=1)
                x1 = (p1 * p1) * b1 * jnp.concatenate([wc[1][sl]] * 2, axis=1)
                xsc[pl.ds(QR * q, QR), pl.ds(LW * l, LW)] = x0 + x1
                put_g(0, q, l, p0 * a0 - x1)
                put_g(1, q, l, p1 * a1 - x0)
        res = None
        for v in SMALL:
            e = probs(c, v) if not ready else None
            for l in range(NS // LW):
                for q in range(CB // QR):
                    put_g(v, q, l, prob_at(e, v, q, l) - xsc[pl.ds(QR * q, QR), pl.ds(LW * l, LW)])
            if v == 3:
                res = dc_part(0)
        more = dc_part(1)
        out = jnp.concatenate([res[0] + more[0], res[1] + more[1]], axis=0)
        for a in range(3):
            dc[pl.ds(piece_row(owners[a], t, a), LANE)] = out[LANE * a:LANE * (a + 1)]

    def rows_part(i):
        ac = cols[0, mine]
        bc = cols[1, mine]
        lanes = lax.broadcasted_iota(jnp.int32, (RB, LANE), 1)
        ones = jnp.where(lanes < 18, 1.0, 0.0).astype(jnp.bfloat16)
        for h in range(RPI):
            jb = i * RPI + h
            c = ca[pl.ds(pl.multiple_of(jb * RB, RB), RB)]
            s = dot_nt(zl[...], jnp.concatenate([c, ones], axis=1)) * SCALE
            wr = []
            for v in range(2):
                parts = []
                for q in range(RB // LANE):
                    b = jb * (RB // LANE) + q
                    parts.append(wall[b // (SH // LANE), pl.ds(v, 1), pl.ds(pl.multiple_of(lax.rem(b, SH // LANE) * LANE, LANE), LANE)])
                wr.append(jnp.concatenate(parts, axis=1))
            sv = [s[ROWS * v:ROWS * (v + 1)] for v in range(VIEWS)]
            p0 = jnp.exp2(sv[0])
            p1 = jnp.exp2(sv[1])
            o0 = (p0 * p0) * bc[:, 0:1] * wr[0]
            o1 = (p1 * p1) * bc[:, 1:2] * wr[1]
            col = pl.ds(h * RB, RB)
            qs[i, 0, :, col] = o0
            qs[i, 1, :, col] = o1
            x0 = o0 * gsc
            x1 = o1 * gsc
            xs = x0 + x1
            gr[pl.ds(0, ROWS), col] = (p0 * ac[:, 0:1] - x1).astype(jnp.bfloat16)
            gr[pl.ds(ROWS, ROWS), col] = (p1 * ac[:, 1:2] - x0).astype(jnp.bfloat16)
            ssum = sv[2]
            for v in range(3, VIEWS):
                ssum = ssum + sv[v]
            for v in SMALL:
                gr[pl.ds(v * ROWS, ROWS), col] = (jnp.exp2(sv[v]) - xs).astype(jnp.bfloat16)
            ls = x1 * sv[0] + x0 * sv[1] + xs * ssum
            part = ls[:, 0:LANE]
            for q in range(1, RB // LANE):
                part = part + ls[:, LANE * q:LANE * (q + 1)]
            acc[pl.ds(VIEWS * ROWS, ROWS)] += part
        cs = ca[pl.ds(pl.multiple_of(i * RW, RW), RW)]
        acc[pl.ds(0, VIEWS * ROWS)] += dot_nn(gr[...], cs)

    def own(it):
        for a in range(3):
            o = owner_of(me, a, it)
            push(o, it, a, order(a)[2], r3)
            push(o, it, a, sib, rs)

    def own1(it):
        for a in range(3):
            push(owner_of(me, a, it), it, a, order(a)[1], r2)

    def serve2(it):
        for a in range(3):
            d0, d1, d2 = order(a)
            drain(dc.at[pl.ds(0, LANE)], r2.at[it, a])
            o = owner_of(d1, a, it)
            push(o, it, a, d2, r3)
            push(o, it, a, sib, rs)

    def serve3(it):
        @pl.when(it < N2)
        def _():
            for a in range(3):
                d0, d1, d2 = order(a)
                drain(dc.at[pl.ds(0, 256)], r3.at[it, a])
                for holder in (d2, d2 + d1 - me):
                    push(owner_of(holder, a, it), it, a, sib, rs)

        @pl.when(it >= N2)
        def _():
            for a in range(3):
                drain(dc.at[pl.ds(0, LANE)], r3.at[it, a])
                push(owner_of(order(a)[2], a, it), it, a, sib, rs)

    with jax.named_scope("chunk0"):
        chunk(0, ready=True)
    own1(0)
    own(0)
    with jax.named_scope("wait_w"):
        drain(wall.at[pl.ds(0, OTHERS)], wrecv)

    def main(it, carry):
        with jax.named_scope("compute"):
            chunk(it)
            rows_part(it - 1)

        @pl.when(it < N2)
        def _():
            own1(it)

        own(it)

        @pl.when(jnp.logical_and(it >= LAG2, it < LAG2 + N2))
        def _():
            with jax.named_scope("serve2"):
                serve2(it - LAG2)

        @pl.when(it >= LAG3)
        def _():
            with jax.named_scope("serve3"):
                serve3(it - LAG3)

        return carry

    lax.fori_loop(1, STEPS, main, 0)

    def rest(i, carry):
        with jax.named_scope("rows"):
            rows_part(i)
        return carry

    lax.fori_loop(STEPS - 1, PARTS, rest, 0)
    for v in range(2):
        qt[v] = qs[PARTS - 1, v, :, pl.ds(0, QT)]
    total = jnp.sum(jnp.sum(acc[pl.ds(VIEWS * ROWS, ROWS)], axis=1, keepdims=True), axis=0, keepdims=True)
    slots[4, me] = jnp.broadcast_to(total, (8, LANE))
    ar_send(4)

    def last(it, carry):
        with jax.named_scope("serve3"):
            serve3(it)
        return carry

    lax.fori_loop(STEPS - LAG3, STEPS, last, 0)
    dz[...] = acc[pl.ds(0, VIEWS * ROWS)].reshape(VIEWS, ROWS, D)
    with jax.named_scope("loss"):
        tot = ar_total(4)
    cross = tot[0:1, 0:1] * (LN2 * TAU * PAIRS) * live - lsum
    loss[...] = -cross / (live * PAIRS)

    def finish(it, carry):
        @pl.when(it < N2)
        def _():
            for a in range(3):
                drain(dc.at[pl.ds(0, 4 * LANE)], rs.at[it, a])
                drain(dc.at[pl.ds(0, 7 * LANE)], ssem.at[it, a])

        @pl.when(it >= N2)
        def _():
            for a in range(3):
                drain(dc.at[pl.ds(0, 2 * LANE)], rs.at[it, a])
                drain(dc.at[pl.ds(0, 3 * LANE)], ssem.at[it, a])
        return carry

    with jax.named_scope("finish"):
        lax.fori_loop(0, STEPS, finish, 0)
    drain(zall.at[pl.ds(0, 2), pl.ds(0, NS - ROWS)], zsend.at[0])
    drain(zall.at[CROPS, pl.ds(0, 7 * ROWS)], zsend.at[1])
    drain(zall.at[CROPS, pl.ds(0, 8 * ROWS)], zs2send)
    drain(mrows.at[pl.ds(0, OTHERS)], arsend.at[0])
    for t in range(1, 5):
        drain(slots.at[t, pl.ds(0, OTHERS)], arsend.at[t])
    drain(lslots.at[pl.ds(0, OTHERS)], lsend)
    drain(wall.at[pl.ds(0, OTHERS)], wsend)


def emit_kernel(dc, qs, qt, dz, loss, o_q1, o_q2, o_loss, o_z1, o_z2, o_zs, o_dc, sem):
    pairs = []
    for i in range(PARTS):
        for v, o in enumerate((o_q1, o_q2)):
            if i < PARTS - 1:
                pairs.append((qs.at[i, v], o.at[:, pl.ds(i * RW, RW)]))
            else:
                pairs.append((qt.at[v], o.at[:, pl.ds(i * RW, QT)]))
        rows = pl.ds(i * RW, RW if i < PARTS - 1 else QT)
        pairs.append((dc.at[rows], o_dc.at[rows]))
    pairs += [(loss, o_loss), (dz.at[0], o_z1), (dz.at[1], o_z2), (dz.at[CROPS], o_zs)]
    copies = [pltpu.make_async_copy(a, b, sem.at[i]) for i, (a, b) in enumerate(pairs)]
    for c in copies:
        c.start()
    for c in copies:
        c.wait()


def local_step(z_one, z_two, z_small, protos, live_mask):
    f32 = jnp.float32
    bf16 = jnp.bfloat16
    vmem = pl.BlockSpec(memory_space=pltpu.VMEM)
    anym = pl.BlockSpec(memory_space=pl.ANY)
    dma = pltpu.SemaphoreType.DMA
    vm = pltpu.VMEM
    dc, qs, qt, dz, loss = pl.pallas_call(
        kernel,
        out_shape=[vm((KPAD, D), f32), vm((PARTS, 2, ROWS, RW), f32), vm((2, ROWS, QT), f32),
                   vm((VIEWS, ROWS, D), f32), vm((1, 1), f32)],
        in_specs=[vmem] * 4 + [anym],
        out_specs=[vmem] * 5,
        scratch_shapes=[vm((KPAD, D), bf16), vm((2, SH, NS), f32), vm((NDEV, 1, LANE), f32), vm((5, NDEV, 8, LANE), f32), vm((NDEV, 32, LANE), f32),
                        vm((NDEV, 2, SH), f32), vm((VIEWS, NS, D), bf16), vm((8, NS), f32), vm((8, NS), f32),
                        vm((2, CB, 4 * NS), bf16), vm((CB, NS), f32),
                        vm((VIEWS * ROWS, RW), bf16), vm((NS, LANE), bf16), vm((3, 32, LANE), f32), vm((VIEWS * ROWS, 2 * D), bf16),
                        vm((2, LANE, 8), f32),
                        vm((VIEWS * ROWS + ROWS, D), f32),
                        dma, dma((2,)), dma, dma, dma, dma, dma((5,)), dma((5,)), dma, dma, dma, dma,
                        dma((STEPS, 3)), dma((STEPS, 3)), dma((STEPS, 3)), dma((STEPS, 3))],
        compiler_params=pltpu.CompilerParams(collective_id=0, has_side_effects=True, vmem_limit_bytes=VM),
        name="step",
    )(z_one, z_two, z_small, live_mask.reshape(1, ROWS), protos)
    q1, q2, loss, dz1, dz2, dzs, dc = pl.pallas_call(
        emit_kernel,
        out_shape=[jax.ShapeDtypeStruct((ROWS, KP), f32), jax.ShapeDtypeStruct((ROWS, KP), f32),
                   jax.ShapeDtypeStruct((1, 1), f32), jax.ShapeDtypeStruct((ROWS, D), f32),
                   jax.ShapeDtypeStruct((ROWS, D), f32), jax.ShapeDtypeStruct((6, ROWS, D), f32),
                   jax.ShapeDtypeStruct((KP, D), f32)],
        in_specs=[vmem] * 5,
        out_specs=[anym] * 7,
        scratch_shapes=[dma((3 * PARTS + 4,))],
        compiler_params=pltpu.CompilerParams(vmem_limit_bytes=1024 * 1024),
        name="emit",
    )(dc, qs, qt, dz, loss)
    return q1, q2, loss.reshape(()), dz1, dz2, dzs, dc


def solution(mesh):
    row_spec = P("data", None)
    crop_spec = P(None, "data", None)
    return jax.shard_map(local_step, mesh=mesh,
                         in_specs=(row_spec, row_spec, crop_spec, P(None, None), P("data")),
                         out_specs=(row_spec, row_spec, P(), row_spec, row_spec, crop_spec, P(None, None)),
                         check_vma=False)
```

```python
import jax
import jax.numpy as jnp
from jax import lax
from jax.experimental import pallas as pl
from jax.experimental.pallas import tpu as pltpu
from jax.sharding import PartitionSpec as P

TAU = 0.1
LOG2E = 1.4426950408889634
LN2 = 0.6931471805599453
SCALE = LOG2E / TAU
NDEV = 16
ROWS = 32
NS = 512
VIEWS = 8
D = 128
KP = 30000
SH = 1920
KPAD = SH * NDEV
LAST = KP - SH * (NDEV - 1)
CB = 384
NCH = SH // CB
PAIRS = 14.0
LOGICAL = pl.DeviceIdType.LOGICAL
VM = 36 * 1024 * 1024
RB = 512
NQ = 1
N2 = 2 * (NCH - NQ)
STEPS = N2 + 4 * NQ
PARTS = 15
RPI = KPAD // RB // PARTS
RW = RPI * RB
QT = KP - RW * (PARTS - 1)
LAG2, LAG3 = 3, 7
LANE = 128
OTHERS = NDEV - 1
CROPS = pl.ds(2, 6)
SMALL = range(2, VIEWS)
PEERS = range(1, NDEV)
PEERS_HALF = range(1, NDEV // 2)
QR, LW = 32, 256


def dot_nt(a, b):
    return lax.dot_general(a, b, (((1,), (1,)), ((), ())), preferred_element_type=jnp.float32)


def dot_nn(a, b):
    return lax.dot_general(a, b, (((1,), (0,)), ((), ())), preferred_element_type=jnp.float32)


def fold8(x):
    return jnp.sum(x.reshape(x.shape[0] // 8, 8, x.shape[1]), axis=0)


def flip(me, bit):
    return me + bit - 2 * bit * lax.rem(me // bit, 2)


def send(src, dst, ssem, rsem, to):
    copy = pltpu.make_async_remote_copy(src_ref=src, dst_ref=dst, send_sem=ssem, recv_sem=rsem,
                                        device_id=to, device_id_type=LOGICAL)
    copy.start()


def drain(ref, sem):
    pltpu.make_async_copy(ref, ref, sem).wait()


def kernel(z1, z2, zs, mask, protos, dc, qs, qt, dz, loss,
           ca, ex, mrows, slots, lslots, wall, zall, arow, brow, gt, xsc, gr, zt, px, zl, cols, acc, mv,
           insem, msem, csem, zsend, zlrecv, zs1recv, zs2send, zs2recv, arsend, arrecv, lsend, lrecv, wsend, wrecv,
           ssem, r2, r3, rs):
    me = lax.axis_index("data")
    barrier = pltpu.get_barrier_semaphore()
    for d in PEERS:
        pl.semaphore_signal(barrier, inc=1, device_id=lax.rem(me + d, NDEV), device_id_type=LOGICAL)
    myrows = pl.ds(pl.multiple_of(me * ROWS, ROWS), ROWS)
    ins = [pltpu.make_async_copy(src, dst, insem.at[i]) for i, (src, dst) in enumerate((
        (mask, mv), (z1, zall.at[0, myrows]), (z2, zall.at[1, myrows]), (zs, zall.at[CROPS, myrows])))]
    for c in ins:
        c.start()
    cc = pltpu.make_async_copy(protos, ca.at[pl.ds(0, KP)], csem)
    cc.start()
    dims = (flip(me, 2), flip(me, 4), flip(me, 8))
    sib = flip(me, 1)
    ins[0].wait()
    mpad = jnp.concatenate([mv[...].astype(jnp.float32), jnp.zeros((1, LANE - ROWS), jnp.float32)], axis=1)
    mrows[me] = pltpu.roll(jnp.broadcast_to(mpad, (8, LANE)), ROWS * lax.rem(me, 4), 1)[0:1]
    for c in ins[1:]:
        c.wait()
    with jax.named_scope("barrier"):
        pl.semaphore_wait(barrier, OTHERS)

    def ar_send(t):
        for d in PEERS:
            send(slots.at[t, me], slots.at[t, me], arsend.at[t], arrecv.at[t], lax.rem(me + d, NDEV))

    def ar_total(t):
        drain(slots.at[t, pl.ds(0, OTHERS)], arrecv.at[t])
        tot = slots[t, 0]
        for i in PEERS:
            tot = tot + slots[t, i]
        return tot

    for d in PEERS:
        send(zall.at[0, myrows], zall.at[0, myrows], zsend.at[0], zlrecv.at[0], lax.rem(me + d, NDEV))
    for d in PEERS:
        send(mrows.at[me], mrows.at[me], msem.at[0], msem.at[1], lax.rem(me + d, NDEV))
    for d in PEERS:
        send(zall.at[1, myrows], zall.at[1, myrows], zsend.at[1], zlrecv.at[1], lax.rem(me + d, NDEV))
    for d in PEERS_HALF:
        send(zall.at[CROPS, myrows], zall.at[CROPS, myrows], zsend.at[2], zs1recv, lax.rem(me + 2 * d, NDEV))
    send(zall.at[CROPS, myrows], zall.at[CROPS, myrows], zs2send, zs2recv, sib)
    zl[pl.ds(0, ROWS), pl.ds(0, D)] = zall[0, myrows]
    zl[pl.ds(ROWS, ROWS), pl.ds(0, D)] = zall[1, myrows]
    zl[pl.ds(2 * ROWS, 6 * ROWS), pl.ds(0, D)] = zall[CROPS, myrows].reshape(6 * ROWS, D)
    zl[pl.ds(0, 2 * ROWS), pl.ds(D, LANE)] = jnp.zeros((2 * ROWS, LANE), jnp.bfloat16)
    ca[pl.ds(KP, KPAD - KP), :] = jnp.zeros((KPAD - KP, D), jnp.bfloat16)
    acc[...] = jnp.zeros_like(acc)
    cc.wait()
    with jax.named_scope("mask"):
        drain(mrows.at[pl.ds(0, OTHERS)], msem.at[1])
        mask8 = [mrows[4 * j] + mrows[4 * j + 1] + mrows[4 * j + 2] + mrows[4 * j + 3] for j in range(4)]
    mask4 = jnp.concatenate(mask8, axis=0)
    mrow = jnp.concatenate(mask8, axis=1)
    live = jnp.sum(jnp.sum(mask4, axis=1, keepdims=True), axis=0, keepdims=True)

    def zwait(v):
        with jax.named_scope("zlarge"):
            drain(zall.at[0, pl.ds(0, NS - ROWS)], zlrecv.at[v])

    def shard(b):
        return ca[pl.ds(pl.multiple_of(me * SH + b * CB, LANE), CB)]

    def col_scale(c, b):
        k = me * SH + b * CB + lax.broadcasted_iota(jnp.int32, (CB, 1), 0)
        return jnp.where(k < KP, 1.0 / (KP * c), 0.0)

    zero8 = jnp.zeros((8, NS), jnp.float32)

    def first(v):
        ps, r = zero8, zero8
        for b in range(NCH):
            p = jnp.exp2(dot_nt(shard(b), zall[v]) * SCALE)
            ps = ps + fold8(p)
            e = p * p * mrow
            ex[v, pl.ds(b * CB, CB)] = e
            w = col_scale(jnp.sum(e, axis=1, keepdims=True), b)
            r = r + fold8(e * w)
        return ps, r

    def put(t, r):
        row = jnp.sum(r, axis=0, keepdims=True)
        for j in range(4):
            slots[t, me, pl.ds(j, 1)] = row[:, LANE * j:LANE * (j + 1)]

    def scale_row(tot):
        r = jnp.concatenate([tot[j:j + 1] for j in range(4)], axis=1)
        return mrow / (live * jnp.where(mrow > 0, r, 1.0))

    pad = jnp.where(me == OTHERS, float(SH - LAST), 0.0)

    def put_lse(v, ps):
        row = jnp.sum(ps, axis=0, keepdims=True) - pad
        for j in range(4):
            lslots[me, pl.ds(4 * v + j, 1)] = row[:, LANE * j:LANE * (j + 1)]

    def lse_send(k):
        ref = lslots.at[me, pl.ds(8 * k, 8)]
        for d in PEERS:
            send(ref, ref, lsend.at[k], lrecv.at[k], lax.rem(me + d, NDEV))

    for v in range(2):
        zwait(v)
        with jax.named_scope("first"):
            ps, r = first(v)
            put(v, r)
            ar_send(v)
        put_lse(v, ps)
    lse_send(0)
    with jax.named_scope("zsmall1"):
        drain(zall.at[CROPS, pl.ds(0, 7 * ROWS)], zs1recv)
    for d in PEERS_HALF:
        rows = pl.ds(pl.multiple_of(lax.rem(me + 2 * d, NDEV) * ROWS, ROWS), ROWS)
        send(zall.at[CROPS, rows], zall.at[CROPS, rows], zs2send, zs2recv, sib)

    def small(i, carry):
        v = 2 + i
        ps = zero8
        for b in range(NCH):
            ps = ps + fold8(jnp.exp2(dot_nt(shard(b), zall[v]) * SCALE))
        put_lse(v, ps)
        return carry

    def again(v, t):
        with jax.named_scope("ar%d" % t):
            u = scale_row(ar_total(t - 2))
        last = t > 3

        def step(b, r):
            rows = pl.ds(pl.multiple_of(b * CB, CB), CB)
            e = ex[v, rows]
            w = col_scale(jnp.sum(e * u, axis=1, keepdims=True), b)
            if last:
                for q in range(CB // LANE):
                    wt = jnp.broadcast_to(w[LANE * q:LANE * (q + 1)], (LANE, LANE)).T
                    wall[me, pl.ds(v, 1), pl.ds(pl.multiple_of(b * CB + LANE * q, LANE), LANE)] = wt[0:1]
            return r + fold8(e * w)

        with jax.named_scope("again%d" % t):
            put(t, lax.fori_loop(0, NCH, step, zero8))
            ar_send(t)

    again(0, 2)
    again(1, 3)
    with jax.named_scope("zsmall2"):
        drain(zall.at[CROPS, pl.ds(0, 8 * ROWS)], zs2recv)
    with jax.named_scope("small"):
        for k in range(1, 4):
            lax.fori_loop(2 * k - 2, 2 * k, small, 0)
            lse_send(k)
    again(0, 4)
    again(1, 5)
    for d in PEERS:
        send(wall.at[me], wall.at[me], wsend, wrecv, lax.rem(me + d, NDEV))
    gsc = 1.0 / (TAU * PAIRS * live)
    with jax.named_scope("lse"):
        for k in range(4):
            drain(lslots.at[pl.ds(0, OTHERS), pl.ds(0, 8)], lrecv.at[k])
        tot = lslots[0]
        for i in PEERS:
            tot = tot + lslots[i]
        logs = jnp.log(tot)
        inv = 1.0 / tot[0:8]
        for v in range(2):
            for j in range(4):
                arow[v:v + 1, LANE * j:LANE * (j + 1)] = gsc * (mask8[j] * inv[4 * v + j:4 * v + j + 1])
        lg2 = jnp.log(2.0 * gsc)
        lsum = jnp.sum(jnp.sum(jnp.concatenate([mask4] * 2, axis=0) * logs[0:8], axis=1, keepdims=True), axis=0, keepdims=True)
        lsum = lsum + (12.0 * live) * lg2
        rest_ = jnp.where(jnp.concatenate([mask4] * 8, axis=0) > 0, TAU * (lg2 - logs), -100.0)
        for k in range(3):
            piece_ = rest_.astype(jnp.bfloat16).astype(jnp.float32)
            px[k] = piece_
            rest_ = rest_ - piece_
        for j in range(4):
            block = jnp.concatenate([px[k, pl.ds(8 + j, 6, 4)] for k in range(3)] + [jnp.zeros((110, LANE), jnp.float32)], axis=0)
            zt[pl.ds(LANE * j, LANE)] = block.T.astype(jnp.bfloat16)
        lane = lax.broadcasted_iota(jnp.int32, (ROWS, LANE), 1)
        own_rows = zt[myrows].astype(jnp.float32)
        for v in SMALL:
            pick = jnp.where(jnp.logical_and(lax.rem(lane, 6) == v - 2, lane < 18), own_rows, 0.0)
            zl[pl.ds(v * ROWS, ROWS), pl.ds(D, LANE)] = pick.astype(jnp.bfloat16)
    def probs(c, v):
        if v < 2:
            return dot_nt(c, zall[v])
        lanes = lax.broadcasted_iota(jnp.int32, (CB, LANE), 1)
        sel = jnp.where(jnp.logical_and(lax.rem(lanes, 6) == v - 2, lanes < 18), 1.0, 0.0).astype(jnp.bfloat16)
        return dot_nt(jnp.concatenate([c, sel], axis=1), jnp.concatenate([zall[v], zt[...]], axis=1))

    with jax.named_scope("ahead"):
        for v in range(VIEWS):
            ex[v % 2, pl.ds(v // 2 * CB, CB)] = jnp.exp2(probs(shard(0), v) * SCALE)
    with jax.named_scope("ar3"):
        us = [scale_row(ar_total(4)), scale_row(ar_total(5))]
    for v in range(2):
        brow[v:v + 1] = live * us[v]
    brow[2:8] = jnp.zeros((6, NS), jnp.float32)
    arow[2:8] = jnp.zeros((6, NS), jnp.float32)
    tile = pl.ds(pl.multiple_of((me // 4) * LANE, LANE), LANE)
    cols[0] = arow[:, tile].T
    cols[1] = brow[:, tile].T
    mine = pl.ds(pl.multiple_of(lax.rem(me, 4) * ROWS, ROWS), ROWS)

    def piece_row(owner, t, a):
        return pl.multiple_of(owner * SH + t * CB + a * LANE, LANE)

    def parts_of(it):
        quad = (it + 8 - N2) // 8
        t = (1 - quad) * (it // 2) + quad * (NCH - NQ + (it - N2) // 4)
        par = (1 - quad) * lax.rem(it, 2) + quad * lax.rem(it + 4 - N2 % 4, 4)
        return t, par

    def push(owner, it, a, to, rsem):
        ref = dc.at[pl.ds(piece_row(owner, parts_of(it)[0], a), LANE)]
        send(ref, ref, ssem.at[it, a], rsem.at[it, a], to)

    def order(a):
        return dims[a], dims[(a + 1) % 3], dims[(a + 2) % 3]

    def owner_of(holder, a, it):
        d0, d1, _ = order(a)
        par = parts_of(it)[1]
        return holder + lax.rem(par, 2) * (d0 - me) + (par // 2) * (d1 - me)

    def chunk(it, ready=False):
        t = parts_of(it)[0]
        owners = [owner_of(me, a, it) for a in range(3)]
        c = jnp.concatenate([ca[pl.ds(piece_row(owners[a], t, a), LANE)] for a in range(3)], axis=0)
        wc = []
        for v in range(2):
            parts = []
            for a in range(3):
                off = pl.multiple_of(t * CB + a * LANE, LANE)
                row = wall[owners[a], pl.ds(v, 1), pl.ds(off, LANE)] * gsc
                parts.append(jnp.broadcast_to(row, (LANE, LANE)).T)
            wc.append(jnp.concatenate(parts, axis=0))
        HALF = CB // 2

        def prob_at(s, v, q, l):
            if ready:
                return ex[v % 2, pl.ds(v // 2 * CB + QR * q, QR), pl.ds(LW * l, LW)]
            return jnp.exp2(s[QR * q:QR * (q + 1), LW * l:LW * (l + 1)] * SCALE)

        def put_g(v, q, l, g):
            gt[v // 4, pl.ds(QR * q, QR), pl.ds((v % 4) * NS + LW * l, LW)] = g.astype(jnp.bfloat16)

        def dc_part(h):
            zz = zall[pl.ds(4 * h, 4)].reshape(4 * NS, D)
            return [dot_nn(gt[h, pl.ds(HALF * m, HALF)], zz) for m in range(2)]

        def rows_of(ref, v, l):
            return ref[v:v + 1, LW * l:LW * (l + 1)]

        e0 = probs(c, 0) if not ready else None
        e1 = probs(c, 1) if not ready else None
        for l in range(NS // LW):
            b0, b1, a0, a1 = rows_of(brow, 0, l), rows_of(brow, 1, l), rows_of(arow, 0, l), rows_of(arow, 1, l)
            for q in range(CB // QR):
                sl = slice(QR * q, QR * (q + 1))
                p0 = prob_at(e0, 0, q, l)
                p1 = prob_at(e1, 1, q, l)
                x0 = (p0 * p0) * b0 * jnp.concatenate([wc[0][sl]] * 2, axis=1)
                x1 = (p1 * p1) * b1 * jnp.concatenate([wc[1][sl]] * 2, axis=1)
                xsc[pl.ds(QR * q, QR), pl.ds(LW * l, LW)] = x0 + x1
                put_g(0, q, l, p0 * a0 - x1)
                put_g(1, q, l, p1 * a1 - x0)
        res = None
        for v in SMALL:
            e = probs(c, v) if not ready else None
            for l in range(NS // LW):
                for q in range(CB // QR):
                    put_g(v, q, l, prob_at(e, v, q, l) - xsc[pl.ds(QR * q, QR), pl.ds(LW * l, LW)])
            if v == 3:
                res = dc_part(0)
        more = dc_part(1)
        out = jnp.concatenate([res[0] + more[0], res[1] + more[1]], axis=0)
        for a in range(3):
            dc[pl.ds(piece_row(owners[a], t, a), LANE)] = out[LANE * a:LANE * (a + 1)]

    def rows_part(i):
        ac = cols[0, mine]
        bc = cols[1, mine]
        lanes = lax.broadcasted_iota(jnp.int32, (RB, LANE), 1)
        ones = jnp.where(lanes < 18, 1.0, 0.0).astype(jnp.bfloat16)
        for h in range(RPI):
            jb = i * RPI + h
            c = ca[pl.ds(pl.multiple_of(jb * RB, RB), RB)]
            s = dot_nt(zl[...], jnp.concatenate([c, ones], axis=1)) * SCALE
            wr = []
            for v in range(2):
                parts = []
                for q in range(RB // LANE):
                    b = jb * (RB // LANE) + q
                    parts.append(wall[b // (SH // LANE), pl.ds(v, 1), pl.ds(pl.multiple_of(lax.rem(b, SH // LANE) * LANE, LANE), LANE)])
                wr.append(jnp.concatenate(parts, axis=1))
            sv = [s[ROWS * v:ROWS * (v + 1)] for v in range(VIEWS)]
            p0 = jnp.exp2(sv[0])
            p1 = jnp.exp2(sv[1])
            o0 = (p0 * p0) * bc[:, 0:1] * wr[0]
            o1 = (p1 * p1) * bc[:, 1:2] * wr[1]
            col = pl.ds(h * RB, RB)
            qs[i, 0, :, col] = o0
            qs[i, 1, :, col] = o1
            x0 = o0 * gsc
            x1 = o1 * gsc
            xs = x0 + x1
            gr[pl.ds(0, ROWS), col] = (p0 * ac[:, 0:1] - x1).astype(jnp.bfloat16)
            gr[pl.ds(ROWS, ROWS), col] = (p1 * ac[:, 1:2] - x0).astype(jnp.bfloat16)
            ssum = sv[2]
            for v in range(3, VIEWS):
                ssum = ssum + sv[v]
            for v in SMALL:
                gr[pl.ds(v * ROWS, ROWS), col] = (jnp.exp2(sv[v]) - xs).astype(jnp.bfloat16)
            ls = x1 * sv[0] + x0 * sv[1] + xs * ssum
            part = ls[:, 0:LANE]
            for q in range(1, RB // LANE):
                part = part + ls[:, LANE * q:LANE * (q + 1)]
            acc[pl.ds(VIEWS * ROWS, ROWS)] += part
        cs = ca[pl.ds(pl.multiple_of(i * RW, RW), RW)]
        acc[pl.ds(0, VIEWS * ROWS)] += dot_nn(gr[...], cs)

    def own(it):
        for a in range(3):
            o = owner_of(me, a, it)
            push(o, it, a, order(a)[2], r3)
            push(o, it, a, sib, rs)

    def own1(it):
        for a in range(3):
            push(owner_of(me, a, it), it, a, order(a)[1], r2)

    def serve2(it):
        for a in range(3):
            d0, d1, d2 = order(a)
            drain(dc.at[pl.ds(0, LANE)], r2.at[it, a])
            o = owner_of(d1, a, it)
            push(o, it, a, d2, r3)
            push(o, it, a, sib, rs)

    def serve3(it):
        @pl.when(it < N2)
        def _():
            for a in range(3):
                d0, d1, d2 = order(a)
                drain(dc.at[pl.ds(0, 256)], r3.at[it, a])
                for holder in (d2, d2 + d1 - me):
                    push(owner_of(holder, a, it), it, a, sib, rs)

        @pl.when(it >= N2)
        def _():
            for a in range(3):
                drain(dc.at[pl.ds(0, LANE)], r3.at[it, a])
                push(owner_of(order(a)[2], a, it), it, a, sib, rs)

    with jax.named_scope("chunk0"):
        chunk(0, ready=True)
    own1(0)
    own(0)
    with jax.named_scope("wait_w"):
        drain(wall.at[pl.ds(0, OTHERS)], wrecv)

    def main(it, carry):
        with jax.named_scope("compute"):
            chunk(it)
            rows_part(it - 1)

        @pl.when(it < N2)
        def _():
            own1(it)

        own(it)

        @pl.when(jnp.logical_and(it >= LAG2, it < LAG2 + N2))
        def _():
            with jax.named_scope("serve2"):
                serve2(it - LAG2)

        @pl.when(it >= LAG3)
        def _():
            with jax.named_scope("serve3"):
                serve3(it - LAG3)

        return carry

    lax.fori_loop(1, STEPS, main, 0)

    def rest(i, carry):
        with jax.named_scope("rows"):
            rows_part(i)
        return carry

    lax.fori_loop(STEPS - 1, PARTS, rest, 0)
    for v in range(2):
        qt[v] = qs[PARTS - 1, v, :, pl.ds(0, QT)]
    total = jnp.sum(jnp.sum(acc[pl.ds(VIEWS * ROWS, ROWS)], axis=1, keepdims=True), axis=0, keepdims=True)
    slots[6, me] = jnp.broadcast_to(total, (4, LANE))
    ar_send(6)

    def last(it, carry):
        with jax.named_scope("serve3"):
            serve3(it)
        return carry

    lax.fori_loop(STEPS - LAG3, STEPS, last, 0)
    dz[...] = acc[pl.ds(0, VIEWS * ROWS)].reshape(VIEWS, ROWS, D)
    with jax.named_scope("loss"):
        tot = ar_total(6)
    cross = tot[0:1, 0:1] * (LN2 * TAU * PAIRS) * live - lsum
    loss[...] = -cross / (live * PAIRS)

    def finish(it, carry):
        @pl.when(it < N2)
        def _():
            for a in range(3):
                drain(dc.at[pl.ds(0, 4 * LANE)], rs.at[it, a])
                drain(dc.at[pl.ds(0, 7 * LANE)], ssem.at[it, a])

        @pl.when(it >= N2)
        def _():
            for a in range(3):
                drain(dc.at[pl.ds(0, 2 * LANE)], rs.at[it, a])
                drain(dc.at[pl.ds(0, 3 * LANE)], ssem.at[it, a])
        return carry

    with jax.named_scope("finish"):
        lax.fori_loop(0, STEPS, finish, 0)
    for v in range(2):
        drain(zall.at[0, pl.ds(0, NS - ROWS)], zsend.at[v])
    drain(zall.at[CROPS, pl.ds(0, 7 * ROWS)], zsend.at[2])
    drain(zall.at[CROPS, pl.ds(0, 8 * ROWS)], zs2send)
    drain(mrows.at[pl.ds(0, OTHERS)], msem.at[0])
    for t in range(7):
        drain(slots.at[t, pl.ds(0, OTHERS)], arsend.at[t])
    for k in range(4):
        drain(lslots.at[pl.ds(0, OTHERS), pl.ds(0, 8)], lsend.at[k])
    drain(wall.at[pl.ds(0, OTHERS)], wsend)


def emit_kernel(dc, qs, qt, dz, loss, o_q1, o_q2, o_loss, o_z1, o_z2, o_zs, o_dc, sem):
    pairs = []
    for i in range(PARTS):
        for v, o in enumerate((o_q1, o_q2)):
            if i < PARTS - 1:
                pairs.append((qs.at[i, v], o.at[:, pl.ds(i * RW, RW)]))
            else:
                pairs.append((qt.at[v], o.at[:, pl.ds(i * RW, QT)]))
        rows = pl.ds(i * RW, RW if i < PARTS - 1 else QT)
        pairs.append((dc.at[rows], o_dc.at[rows]))
    pairs += [(loss, o_loss), (dz.at[0], o_z1), (dz.at[1], o_z2), (dz.at[CROPS], o_zs)]
    copies = [pltpu.make_async_copy(a, b, sem.at[i]) for i, (a, b) in enumerate(pairs)]
    for c in copies:
        c.start()
    for c in copies:
        c.wait()


def local_step(z_one, z_two, z_small, protos, live_mask):
    f32 = jnp.float32
    bf16 = jnp.bfloat16
    vmem = pl.BlockSpec(memory_space=pltpu.VMEM)
    anym = pl.BlockSpec(memory_space=pl.ANY)
    dma = pltpu.SemaphoreType.DMA
    vm = pltpu.VMEM
    dc, qs, qt, dz, loss = pl.pallas_call(
        kernel,
        out_shape=[vm((KPAD, D), f32), vm((PARTS, 2, ROWS, RW), f32), vm((2, ROWS, QT), f32),
                   vm((VIEWS, ROWS, D), f32), vm((1, 1), f32)],
        in_specs=[anym] * 5,
        out_specs=[vmem] * 5,
        scratch_shapes=[vm((KPAD, D), bf16), vm((2, SH, NS), f32), vm((NDEV, 1, LANE), f32), vm((7, NDEV, 4, LANE), f32), vm((NDEV, 32, LANE), f32),
                        vm((NDEV, 2, SH), f32), vm((VIEWS, NS, D), bf16), vm((8, NS), f32), vm((8, NS), f32),
                        vm((2, CB, 4 * NS), bf16), vm((CB, NS), f32),
                        vm((VIEWS * ROWS, RW), bf16), vm((NS, LANE), bf16), vm((3, 32, LANE), f32), vm((VIEWS * ROWS, 2 * D), bf16),
                        vm((2, LANE, 8), f32),
                        vm((VIEWS * ROWS + ROWS, D), f32),
                        vm((1, ROWS), jnp.int32),
                        dma((4,)), dma((2,)), dma, dma((3,)), dma((2,)), dma, dma, dma, dma((7,)), dma((7,)), dma((4,)), dma((4,)), dma, dma,
                        dma((STEPS, 3)), dma((STEPS, 3)), dma((STEPS, 3)), dma((STEPS, 3))],
        compiler_params=pltpu.CompilerParams(collective_id=0, has_side_effects=True, vmem_limit_bytes=VM),
        name="step",
    )(z_one, z_two, z_small, live_mask.reshape(1, ROWS), protos)
    q1, q2, loss, dz1, dz2, dzs, dc = pl.pallas_call(
        emit_kernel,
        out_shape=[jax.ShapeDtypeStruct((ROWS, KP), f32), jax.ShapeDtypeStruct((ROWS, KP), f32),
                   jax.ShapeDtypeStruct((1, 1), f32), jax.ShapeDtypeStruct((ROWS, D), f32),
                   jax.ShapeDtypeStruct((ROWS, D), f32), jax.ShapeDtypeStruct((6, ROWS, D), f32),
                   jax.ShapeDtypeStruct((KP, D), f32)],
        in_specs=[vmem] * 5,
        out_specs=[anym] * 7,
        scratch_shapes=[dma((3 * PARTS + 4,))],
        compiler_params=pltpu.CompilerParams(vmem_limit_bytes=1024 * 1024),
        name="emit",
    )(dc, qs, qt, dz, loss)
    return q1, q2, loss.reshape(()), dz1, dz2, dzs, dc


def solution(mesh):
    row_spec = P("data", None)
    crop_spec = P(None, "data", None)
    return jax.shard_map(local_step, mesh=mesh,
                         in_specs=(row_spec, row_spec, crop_spec, P(None, None), P("data")),
                         out_specs=(row_spec, row_spec, P(), row_spec, row_spec, crop_spec, P(None, None)),
                         check_vma=False)
```

```python
import jax
import jax.numpy as jnp
from jax import lax
from jax.experimental import pallas as pl
from jax.experimental.pallas import tpu as pltpu
from jax.sharding import PartitionSpec as P

TAU = 0.1
LOG2E = 1.4426950408889634
LN2 = 0.6931471805599453
SCALE = LOG2E / TAU
NDEV = 16
ROWS = 32
NS = 512
VIEWS = 8
D = 128
KP = 30000
SH = 1920
KPAD = SH * NDEV
LAST = KP - SH * (NDEV - 1)
CB = 384
NCH = SH // CB
PAIRS = 14.0
LOGICAL = pl.DeviceIdType.LOGICAL
VM = 36 * 1024 * 1024
RB = 512
NQ = 1
N2 = 2 * (NCH - NQ)
STEPS = N2 + 4 * NQ
PARTS = 15
ALONE = 3
RPI = KPAD // RB // PARTS
RW = RPI * RB
QT = KP - RW * (PARTS - 1)
LAG2, LAG3 = 3, 7
LANE = 128
OTHERS = NDEV - 1
CROPS = pl.ds(2, 6)
SMALL = range(2, VIEWS)
PEERS = range(1, NDEV)
PEERS_HALF = range(1, NDEV // 2)
QR, LW = 32, 256


def dot_nt(a, b):
    return lax.dot_general(a, b, (((1,), (1,)), ((), ())), preferred_element_type=jnp.float32)


def dot_nn(a, b):
    return lax.dot_general(a, b, (((1,), (0,)), ((), ())), preferred_element_type=jnp.float32)


def fold8(x):
    return jnp.sum(x.reshape(x.shape[0] // 8, 8, x.shape[1]), axis=0)


def flip(me, bit):
    return me + bit - 2 * bit * lax.rem(me // bit, 2)


def send(src, dst, ssem, rsem, to):
    copy = pltpu.make_async_remote_copy(src_ref=src, dst_ref=dst, send_sem=ssem, recv_sem=rsem,
                                        device_id=to, device_id_type=LOGICAL)
    copy.start()


def drain(ref, sem):
    pltpu.make_async_copy(ref, ref, sem).wait()


def kernel(z1, z2, zs, mask, protos, dc, qs, qt, dz, loss,
           ca, ex, mrows, slots, lslots, wall, zall, arow, brow, gt, xsc, gr, zt, px, zl, cols, acc, mv,
           insem, msem, csem, zsend, zlrecv, zs1recv, zs2send, zs2recv, arsend, arrecv, lsend, lrecv, wsend, wrecv,
           ssem, r2, r3, rs):
    me = lax.axis_index("data")
    barrier = pltpu.get_barrier_semaphore()
    for d in PEERS:
        pl.semaphore_signal(barrier, inc=1, device_id=lax.rem(me + d, NDEV), device_id_type=LOGICAL)
    myrows = pl.ds(pl.multiple_of(me * ROWS, ROWS), ROWS)
    ins = [pltpu.make_async_copy(src, dst, insem.at[i]) for i, (src, dst) in enumerate((
        (mask, mv), (z1, zall.at[0, myrows]), (z2, zall.at[1, myrows]), (zs, zall.at[CROPS, myrows])))]
    for c in ins:
        c.start()
    cc = pltpu.make_async_copy(protos, ca.at[pl.ds(0, KP)], csem)
    cc.start()
    dims = (flip(me, 2), flip(me, 4), flip(me, 8))
    sib = flip(me, 1)
    ins[0].wait()
    mpad = jnp.concatenate([mv[...].astype(jnp.float32), jnp.zeros((1, LANE - ROWS), jnp.float32)], axis=1)
    mrows[me] = pltpu.roll(jnp.broadcast_to(mpad, (8, LANE)), ROWS * lax.rem(me, 4), 1)[0:1]
    for c in ins[1:]:
        c.wait()
    with jax.named_scope("barrier"):
        pl.semaphore_wait(barrier, OTHERS)

    def ar_send(t):
        for d in PEERS:
            send(slots.at[t, me], slots.at[t, me], arsend.at[t], arrecv.at[t], lax.rem(me + d, NDEV))

    def ar_total(t):
        drain(slots.at[t, pl.ds(0, OTHERS)], arrecv.at[t])
        tot = slots[t, 0]
        for i in PEERS:
            tot = tot + slots[t, i]
        return tot

    for d in PEERS:
        send(zall.at[0, myrows], zall.at[0, myrows], zsend.at[0], zlrecv.at[0], lax.rem(me + d, NDEV))
    for d in PEERS:
        send(mrows.at[me], mrows.at[me], msem.at[0], msem.at[1], lax.rem(me + d, NDEV))
    for d in PEERS:
        send(zall.at[1, myrows], zall.at[1, myrows], zsend.at[1], zlrecv.at[1], lax.rem(me + d, NDEV))
    for d in PEERS_HALF:
        send(zall.at[CROPS, myrows], zall.at[CROPS, myrows], zsend.at[2], zs1recv, lax.rem(me + 2 * d, NDEV))
    send(zall.at[CROPS, myrows], zall.at[CROPS, myrows], zs2send, zs2recv, sib)
    zl[pl.ds(0, ROWS), pl.ds(0, D)] = zall[0, myrows]
    zl[pl.ds(ROWS, ROWS), pl.ds(0, D)] = zall[1, myrows]
    zl[pl.ds(2 * ROWS, 6 * ROWS), pl.ds(0, D)] = zall[CROPS, myrows].reshape(6 * ROWS, D)
    zl[pl.ds(0, 2 * ROWS), pl.ds(D, LANE)] = jnp.zeros((2 * ROWS, LANE), jnp.bfloat16)
    ca[pl.ds(KP, KPAD - KP), :] = jnp.zeros((KPAD - KP, D), jnp.bfloat16)
    acc[...] = jnp.zeros_like(acc)
    cc.wait()
    with jax.named_scope("mask"):
        drain(mrows.at[pl.ds(0, OTHERS)], msem.at[1])
        mask8 = [mrows[4 * j] + mrows[4 * j + 1] + mrows[4 * j + 2] + mrows[4 * j + 3] for j in range(4)]
    mask4 = jnp.concatenate(mask8, axis=0)
    mrow = jnp.concatenate(mask8, axis=1)
    live = jnp.sum(jnp.sum(mask4, axis=1, keepdims=True), axis=0, keepdims=True)

    def zwait(v):
        with jax.named_scope("zlarge"):
            drain(zall.at[0, pl.ds(0, NS - ROWS)], zlrecv.at[v])

    def shard(b):
        return ca[pl.ds(pl.multiple_of(me * SH + b * CB, LANE), CB)]

    def col_scale(c, b):
        k = me * SH + b * CB + lax.broadcasted_iota(jnp.int32, (CB, 1), 0)
        return jnp.where(k < KP, 1.0 / (KP * c), 0.0)

    zero8 = jnp.zeros((8, NS), jnp.float32)

    def first(v):
        ps, r = zero8, zero8
        for b in range(NCH):
            p = jnp.exp2(dot_nt(shard(b), zall[v]) * SCALE)
            ps = ps + fold8(p)
            e = p * p * mrow
            ex[v, pl.ds(b * CB, CB)] = e
            w = col_scale(jnp.sum(e, axis=1, keepdims=True), b)
            r = r + fold8(e * w)
        return ps, r

    def put(t, r):
        row = jnp.sum(r, axis=0, keepdims=True)
        for j in range(4):
            slots[t, me, pl.ds(j, 1)] = row[:, LANE * j:LANE * (j + 1)]

    def scale_row(tot):
        r = jnp.concatenate([tot[j:j + 1] for j in range(4)], axis=1)
        return mrow / (live * jnp.where(mrow > 0, r, 1.0))

    pad = jnp.where(me == OTHERS, float(SH - LAST), 0.0)

    def put_lse(v, ps):
        row = jnp.sum(ps, axis=0, keepdims=True) - pad
        for j in range(4):
            lslots[me, pl.ds(4 * v + j, 1)] = row[:, LANE * j:LANE * (j + 1)]

    def lse_send(k):
        ref = lslots.at[me, pl.ds(8 * k, 8)]
        for d in PEERS:
            send(ref, ref, lsend.at[k], lrecv.at[k], lax.rem(me + d, NDEV))

    for v in range(2):
        zwait(v)
        with jax.named_scope("first"):
            ps, r = first(v)
            put(v, r)
            ar_send(v)
        put_lse(v, ps)
    lse_send(0)
    with jax.named_scope("zsmall1"):
        drain(zall.at[CROPS, pl.ds(0, 7 * ROWS)], zs1recv)
    for d in PEERS_HALF:
        rows = pl.ds(pl.multiple_of(lax.rem(me + 2 * d, NDEV) * ROWS, ROWS), ROWS)
        send(zall.at[CROPS, rows], zall.at[CROPS, rows], zs2send, zs2recv, sib)

    def small(i, carry):
        v = 2 + i
        ps = zero8
        for b in range(NCH):
            ps = ps + fold8(jnp.exp2(dot_nt(shard(b), zall[v]) * SCALE))
        put_lse(v, ps)
        return carry

    def again(v, t):
        with jax.named_scope("ar%d" % t):
            u = scale_row(ar_total(t - 2))
        last = t > 3

        def step(b, r):
            rows = pl.ds(pl.multiple_of(b * CB, CB), CB)
            e = ex[v, rows]
            w = col_scale(jnp.sum(e * u, axis=1, keepdims=True), b)
            if last:
                for q in range(CB // LANE):
                    wt = jnp.broadcast_to(w[LANE * q:LANE * (q + 1)], (LANE, LANE)).T
                    wall[me, pl.ds(v, 1), pl.ds(pl.multiple_of(b * CB + LANE * q, LANE), LANE)] = wt[0:1]
            return r + fold8(e * w)

        with jax.named_scope("again%d" % t):
            put(t, lax.fori_loop(0, NCH, step, zero8))
            ar_send(t)

    again(0, 2)
    again(1, 3)
    with jax.named_scope("zsmall2"):
        drain(zall.at[CROPS, pl.ds(0, 8 * ROWS)], zs2recv)
    with jax.named_scope("small"):
        for k in range(1, 4):
            lax.fori_loop(2 * k - 2, 2 * k, small, 0)
            lse_send(k)
    again(0, 4)
    again(1, 5)
    for d in PEERS:
        send(wall.at[me], wall.at[me], wsend, wrecv, lax.rem(me + d, NDEV))
    gsc = 1.0 / (TAU * PAIRS * live)
    with jax.named_scope("lse"):
        for k in range(4):
            drain(lslots.at[pl.ds(0, OTHERS), pl.ds(0, 8)], lrecv.at[k])
        tot = lslots[0]
        for i in PEERS:
            tot = tot + lslots[i]
        logs = jnp.log(tot)
        inv = 1.0 / tot[0:8]
        for v in range(2):
            for j in range(4):
                arow[v:v + 1, LANE * j:LANE * (j + 1)] = gsc * (mask8[j] * inv[4 * v + j:4 * v + j + 1])
        lg2 = jnp.log(2.0 * gsc)
        lsum = jnp.sum(jnp.sum(jnp.concatenate([mask4] * 2, axis=0) * logs[0:8], axis=1, keepdims=True), axis=0, keepdims=True)
        lsum = lsum + (12.0 * live) * lg2
        rest_ = jnp.where(jnp.concatenate([mask4] * 8, axis=0) > 0, TAU * (lg2 - logs), -100.0)
        for k in range(3):
            piece_ = rest_.astype(jnp.bfloat16).astype(jnp.float32)
            px[k] = piece_
            rest_ = rest_ - piece_
        for j in range(4):
            block = jnp.concatenate([px[k, pl.ds(8 + j, 6, 4)] for k in range(3)] + [jnp.zeros((110, LANE), jnp.float32)], axis=0)
            zt[pl.ds(LANE * j, LANE)] = block.T.astype(jnp.bfloat16)
        lane = lax.broadcasted_iota(jnp.int32, (ROWS, LANE), 1)
        own_rows = zt[myrows].astype(jnp.float32)
        for v in SMALL:
            pick = jnp.where(jnp.logical_and(lax.rem(lane, 6) == v - 2, lane < 18), own_rows, 0.0)
            zl[pl.ds(v * ROWS, ROWS), pl.ds(D, LANE)] = pick.astype(jnp.bfloat16)
    def probs(c, v):
        if v < 2:
            return dot_nt(c, zall[v])
        lanes = lax.broadcasted_iota(jnp.int32, (CB, LANE), 1)
        sel = jnp.where(jnp.logical_and(lax.rem(lanes, 6) == v - 2, lanes < 18), 1.0, 0.0).astype(jnp.bfloat16)
        return dot_nt(jnp.concatenate([c, sel], axis=1), jnp.concatenate([zall[v], zt[...]], axis=1))

    with jax.named_scope("ahead"):
        for v in range(VIEWS):
            ex[v % 2, pl.ds(v // 2 * CB, CB)] = jnp.exp2(probs(shard(0), v) * SCALE)
    with jax.named_scope("ar3"):
        us = [scale_row(ar_total(4)), scale_row(ar_total(5))]
    for v in range(2):
        brow[v:v + 1] = live * us[v]
    brow[2:8] = jnp.zeros((6, NS), jnp.float32)
    arow[2:8] = jnp.zeros((6, NS), jnp.float32)
    tile = pl.ds(pl.multiple_of((me // 4) * LANE, LANE), LANE)
    cols[0] = arow[:, tile].T
    cols[1] = brow[:, tile].T
    mine = pl.ds(pl.multiple_of(lax.rem(me, 4) * ROWS, ROWS), ROWS)

    def piece_row(owner, t, a):
        return pl.multiple_of(owner * SH + t * CB + a * LANE, LANE)

    def parts_of(it):
        quad = (it + 8 - N2) // 8
        t = (1 - quad) * (it // 2) + quad * (NCH - NQ + (it - N2) // 4)
        par = (1 - quad) * lax.rem(it, 2) + quad * lax.rem(it + 4 - N2 % 4, 4)
        return t, par

    def push(owner, it, a, to, rsem):
        ref = dc.at[pl.ds(piece_row(owner, parts_of(it)[0], a), LANE)]
        send(ref, ref, ssem.at[it, a], rsem.at[it, a], to)

    def order(a):
        return dims[a], dims[(a + 1) % 3], dims[(a + 2) % 3]

    def owner_of(holder, a, it):
        d0, d1, _ = order(a)
        par = parts_of(it)[1]
        return holder + lax.rem(par, 2) * (d0 - me) + (par // 2) * (d1 - me)

    def chunk(it, ready=False):
        t = parts_of(it)[0]
        owners = [owner_of(me, a, it) for a in range(3)]
        c = jnp.concatenate([ca[pl.ds(piece_row(owners[a], t, a), LANE)] for a in range(3)], axis=0)
        wc = []
        for v in range(2):
            parts = []
            for a in range(3):
                off = pl.multiple_of(t * CB + a * LANE, LANE)
                row = wall[owners[a], pl.ds(v, 1), pl.ds(off, LANE)] * gsc
                parts.append(jnp.broadcast_to(row, (LANE, LANE)).T)
            wc.append(jnp.concatenate(parts, axis=0))
        HALF = CB // 2

        def prob_at(s, v, q, l):
            if ready:
                return ex[v % 2, pl.ds(v // 2 * CB + QR * q, QR), pl.ds(LW * l, LW)]
            return jnp.exp2(s[QR * q:QR * (q + 1), LW * l:LW * (l + 1)] * SCALE)

        def put_g(v, q, l, g):
            gt[v // 4, pl.ds(QR * q, QR), pl.ds((v % 4) * NS + LW * l, LW)] = g.astype(jnp.bfloat16)

        def dc_part(h):
            zz = zall[pl.ds(4 * h, 4)].reshape(4 * NS, D)
            return [dot_nn(gt[h, pl.ds(HALF * m, HALF)], zz) for m in range(2)]

        def rows_of(ref, v, l):
            return ref[v:v + 1, LW * l:LW * (l + 1)]

        e0 = probs(c, 0) if not ready else None
        e1 = probs(c, 1) if not ready else None
        for l in range(NS // LW):
            b0, b1, a0, a1 = rows_of(brow, 0, l), rows_of(brow, 1, l), rows_of(arow, 0, l), rows_of(arow, 1, l)
            for q in range(CB // QR):
                sl = slice(QR * q, QR * (q + 1))
                p0 = prob_at(e0, 0, q, l)
                p1 = prob_at(e1, 1, q, l)
                x0 = (p0 * p0) * b0 * jnp.concatenate([wc[0][sl]] * 2, axis=1)
                x1 = (p1 * p1) * b1 * jnp.concatenate([wc[1][sl]] * 2, axis=1)
                xsc[pl.ds(QR * q, QR), pl.ds(LW * l, LW)] = x0 + x1
                put_g(0, q, l, p0 * a0 - x1)
                put_g(1, q, l, p1 * a1 - x0)
        res = None
        for v in SMALL:
            e = probs(c, v) if not ready else None
            for l in range(NS // LW):
                for q in range(CB // QR):
                    put_g(v, q, l, prob_at(e, v, q, l) - xsc[pl.ds(QR * q, QR), pl.ds(LW * l, LW)])
            if v == 3:
                res = dc_part(0)
        more = dc_part(1)
        out = jnp.concatenate([res[0] + more[0], res[1] + more[1]], axis=0)
        for a in range(3):
            dc[pl.ds(piece_row(owners[a], t, a), LANE)] = out[LANE * a:LANE * (a + 1)]

    def rows_part(i):
        ac = cols[0, mine]
        bc = cols[1, mine]
        lanes = lax.broadcasted_iota(jnp.int32, (RB, LANE), 1)
        ones = jnp.where(lanes < 18, 1.0, 0.0).astype(jnp.bfloat16)
        for h in range(RPI):
            jb = i * RPI + h
            c = ca[pl.ds(pl.multiple_of(jb * RB, RB), RB)]
            s = dot_nt(zl[...], jnp.concatenate([c, ones], axis=1)) * SCALE
            wr = []
            for v in range(2):
                parts = []
                for q in range(RB // LANE):
                    b = jb * (RB // LANE) + q
                    parts.append(wall[b // (SH // LANE), pl.ds(v, 1), pl.ds(pl.multiple_of(lax.rem(b, SH // LANE) * LANE, LANE), LANE)])
                wr.append(jnp.concatenate(parts, axis=1))
            sv = [s[ROWS * v:ROWS * (v + 1)] for v in range(VIEWS)]
            p0 = jnp.exp2(sv[0])
            p1 = jnp.exp2(sv[1])
            o0 = (p0 * p0) * bc[:, 0:1] * wr[0]
            o1 = (p1 * p1) * bc[:, 1:2] * wr[1]
            col = pl.ds(h * RB, RB)
            qs[i, 0, :, col] = o0
            qs[i, 1, :, col] = o1
            x0 = o0 * gsc
            x1 = o1 * gsc
            xs = x0 + x1
            gr[pl.ds(0, ROWS), col] = (p0 * ac[:, 0:1] - x1).astype(jnp.bfloat16)
            gr[pl.ds(ROWS, ROWS), col] = (p1 * ac[:, 1:2] - x0).astype(jnp.bfloat16)
            ssum = sv[2]
            for v in range(3, VIEWS):
                ssum = ssum + sv[v]
            for v in SMALL:
                gr[pl.ds(v * ROWS, ROWS), col] = (jnp.exp2(sv[v]) - xs).astype(jnp.bfloat16)
            ls = x1 * sv[0] + x0 * sv[1] + xs * ssum
            part = ls[:, 0:LANE]
            for q in range(1, RB // LANE):
                part = part + ls[:, LANE * q:LANE * (q + 1)]
            acc[pl.ds(VIEWS * ROWS, ROWS)] += part
        cs = ca[pl.ds(pl.multiple_of(i * RW, RW), RW)]
        acc[pl.ds(0, VIEWS * ROWS)] += dot_nn(gr[...], cs)

    def own(it):
        for a in range(3):
            o = owner_of(me, a, it)
            push(o, it, a, order(a)[2], r3)
            push(o, it, a, sib, rs)

    def own1(it):
        for a in range(3):
            push(owner_of(me, a, it), it, a, order(a)[1], r2)

    def serve2(it):
        for a in range(3):
            d0, d1, d2 = order(a)
            drain(dc.at[pl.ds(0, LANE)], r2.at[it, a])
            o = owner_of(d1, a, it)
            push(o, it, a, d2, r3)
            push(o, it, a, sib, rs)

    def serve3(it):
        @pl.when(it < N2)
        def _():
            for a in range(3):
                d0, d1, d2 = order(a)
                drain(dc.at[pl.ds(0, 256)], r3.at[it, a])
                for holder in (d2, d2 + d1 - me):
                    push(owner_of(holder, a, it), it, a, sib, rs)

        @pl.when(it >= N2)
        def _():
            for a in range(3):
                drain(dc.at[pl.ds(0, LANE)], r3.at[it, a])
                push(owner_of(order(a)[2], a, it), it, a, sib, rs)

    with jax.named_scope("chunk0"):
        chunk(0, ready=True)
    own1(0)
    own(0)
    with jax.named_scope("wait_w"):
        drain(wall.at[pl.ds(0, OTHERS)], wrecv)

    def main(it, with_rows):
        with jax.named_scope("compute"):
            chunk(it)
            if with_rows:
                rows_part(it - ALONE)

        @pl.when(it < N2)
        def _():
            own1(it)

        own(it)

        @pl.when(jnp.logical_and(it >= LAG2, it < LAG2 + N2))
        def _():
            with jax.named_scope("serve2"):
                serve2(it - LAG2)

        @pl.when(it >= LAG3)
        def _():
            with jax.named_scope("serve3"):
                serve3(it - LAG3)

    def main_alone(it, carry):
        main(it, False)
        return carry

    def main_rows(it, carry):
        main(it, True)
        return carry

    lax.fori_loop(1, ALONE, main_alone, 0)
    lax.fori_loop(ALONE, STEPS, main_rows, 0)

    def rest(i, carry):
        with jax.named_scope("rows"):
            rows_part(i)
        return carry

    lax.fori_loop(STEPS - ALONE, PARTS, rest, 0)
    for v in range(2):
        qt[v] = qs[PARTS - 1, v, :, pl.ds(0, QT)]
    total = jnp.sum(jnp.sum(acc[pl.ds(VIEWS * ROWS, ROWS)], axis=1, keepdims=True), axis=0, keepdims=True)
    slots[6, me] = jnp.broadcast_to(total, (4, LANE))
    ar_send(6)

    def last(it, carry):
        with jax.named_scope("serve3"):
            serve3(it)
        return carry

    lax.fori_loop(STEPS - LAG3, STEPS, last, 0)
    dz[...] = acc[pl.ds(0, VIEWS * ROWS)].reshape(VIEWS, ROWS, D)
    with jax.named_scope("loss"):
        tot = ar_total(6)
    cross = tot[0:1, 0:1] * (LN2 * TAU * PAIRS) * live - lsum
    loss[...] = -cross / (live * PAIRS)

    def finish(it, carry):
        @pl.when(it < N2)
        def _():
            for a in range(3):
                drain(dc.at[pl.ds(0, 4 * LANE)], rs.at[it, a])
                drain(dc.at[pl.ds(0, 7 * LANE)], ssem.at[it, a])

        @pl.when(it >= N2)
        def _():
            for a in range(3):
                drain(dc.at[pl.ds(0, 2 * LANE)], rs.at[it, a])
                drain(dc.at[pl.ds(0, 3 * LANE)], ssem.at[it, a])
        return carry

    with jax.named_scope("finish"):
        lax.fori_loop(0, STEPS, finish, 0)
    for v in range(2):
        drain(zall.at[0, pl.ds(0, NS - ROWS)], zsend.at[v])
    drain(zall.at[CROPS, pl.ds(0, 7 * ROWS)], zsend.at[2])
    drain(zall.at[CROPS, pl.ds(0, 8 * ROWS)], zs2send)
    drain(mrows.at[pl.ds(0, OTHERS)], msem.at[0])
    for t in range(7):
        drain(slots.at[t, pl.ds(0, OTHERS)], arsend.at[t])
    for k in range(4):
        drain(lslots.at[pl.ds(0, OTHERS), pl.ds(0, 8)], lsend.at[k])
    drain(wall.at[pl.ds(0, OTHERS)], wsend)


def emit_kernel(dc, qs, qt, dz, loss, o_q1, o_q2, o_loss, o_z1, o_z2, o_zs, o_dc, sem):
    pairs = []
    for i in range(PARTS):
        for v, o in enumerate((o_q1, o_q2)):
            if i < PARTS - 1:
                pairs.append((qs.at[i, v], o.at[:, pl.ds(i * RW, RW)]))
            else:
                pairs.append((qt.at[v], o.at[:, pl.ds(i * RW, QT)]))
        rows = pl.ds(i * RW, RW if i < PARTS - 1 else QT)
        pairs.append((dc.at[rows], o_dc.at[rows]))
    pairs += [(loss, o_loss), (dz.at[0], o_z1), (dz.at[1], o_z2), (dz.at[CROPS], o_zs)]
    copies = [pltpu.make_async_copy(a, b, sem.at[i]) for i, (a, b) in enumerate(pairs)]
    for c in copies:
        c.start()
    for c in copies:
        c.wait()


def local_step(z_one, z_two, z_small, protos, live_mask):
    f32 = jnp.float32
    bf16 = jnp.bfloat16
    vmem = pl.BlockSpec(memory_space=pltpu.VMEM)
    anym = pl.BlockSpec(memory_space=pl.ANY)
    dma = pltpu.SemaphoreType.DMA
    vm = pltpu.VMEM
    dc, qs, qt, dz, loss = pl.pallas_call(
        kernel,
        out_shape=[vm((KPAD, D), f32), vm((PARTS, 2, ROWS, RW), f32), vm((2, ROWS, QT), f32),
                   vm((VIEWS, ROWS, D), f32), vm((1, 1), f32)],
        in_specs=[anym] * 5,
        out_specs=[vmem] * 5,
        scratch_shapes=[vm((KPAD, D), bf16), vm((2, SH, NS), f32), vm((NDEV, 1, LANE), f32), vm((7, NDEV, 4, LANE), f32), vm((NDEV, 32, LANE), f32),
                        vm((NDEV, 2, SH), f32), vm((VIEWS, NS, D), bf16), vm((8, NS), f32), vm((8, NS), f32),
                        vm((2, CB, 4 * NS), bf16), vm((CB, NS), f32),
                        vm((VIEWS * ROWS, RW), bf16), vm((NS, LANE), bf16), vm((3, 32, LANE), f32), vm((VIEWS * ROWS, 2 * D), bf16),
                        vm((2, LANE, 8), f32),
                        vm((VIEWS * ROWS + ROWS, D), f32),
                        vm((1, ROWS), jnp.int32),
                        dma((4,)), dma((2,)), dma, dma((3,)), dma((2,)), dma, dma, dma, dma((7,)), dma((7,)), dma((4,)), dma((4,)), dma, dma,
                        dma((STEPS, 3)), dma((STEPS, 3)), dma((STEPS, 3)), dma((STEPS, 3))],
        compiler_params=pltpu.CompilerParams(collective_id=0, has_side_effects=True, vmem_limit_bytes=VM),
        name="step",
    )(z_one, z_two, z_small, live_mask.reshape(1, ROWS), protos)
    q1, q2, loss, dz1, dz2, dzs, dc = pl.pallas_call(
        emit_kernel,
        out_shape=[jax.ShapeDtypeStruct((ROWS, KP), f32), jax.ShapeDtypeStruct((ROWS, KP), f32),
                   jax.ShapeDtypeStruct((1, 1), f32), jax.ShapeDtypeStruct((ROWS, D), f32),
                   jax.ShapeDtypeStruct((ROWS, D), f32), jax.ShapeDtypeStruct((6, ROWS, D), f32),
                   jax.ShapeDtypeStruct((KP, D), f32)],
        in_specs=[vmem] * 5,
        out_specs=[anym] * 7,
        scratch_shapes=[dma((3 * PARTS + 4,))],
        compiler_params=pltpu.CompilerParams(vmem_limit_bytes=1024 * 1024),
        name="emit",
    )(dc, qs, qt, dz, loss)
    return q1, q2, loss.reshape(()), dz1, dz2, dzs, dc


def solution(mesh):
    row_spec = P("data", None)
    crop_spec = P(None, "data", None)
    return jax.shard_map(local_step, mesh=mesh,
                         in_specs=(row_spec, row_spec, crop_spec, P(None, None), P("data")),
                         out_specs=(row_spec, row_spec, P(), row_spec, row_spec, crop_spec, P(None, None)),
                         check_vma=False)
```

```python
import jax
import jax.numpy as jnp
from jax import lax
from jax.experimental import pallas as pl
from jax.experimental.pallas import tpu as pltpu
from jax.sharding import PartitionSpec as P

TAU = 0.1
LOG2E = 1.4426950408889634
LN2 = 0.6931471805599453
SCALE = LOG2E / TAU
NDEV = 16
ROWS = 32
NS = 512
VIEWS = 8
D = 128
KP = 30000
SH = 1920
KPAD = SH * NDEV
LAST = KP - SH * (NDEV - 1)
CB = 384
NCH = SH // CB
PAIRS = 14.0
LOGICAL = pl.DeviceIdType.LOGICAL
VM = 36 * 1024 * 1024
RB = 512
NQ = 1
N2 = 2 * (NCH - NQ)
STEPS = N2 + 4 * NQ
PARTS = 15
ALONE = 3
RPI = KPAD // RB // PARTS
RW = RPI * RB
QT = KP - RW * (PARTS - 1)
LAG2, LAG3 = 3, 7
LANE = 128
OTHERS = NDEV - 1
CROPS = pl.ds(2, 6)
SMALL = range(2, VIEWS)
PEERS = range(1, NDEV)
PEERS_HALF = range(1, NDEV // 2)
QR, LW = 32, 256


def dot_nt(a, b):
    return lax.dot_general(a, b, (((1,), (1,)), ((), ())), preferred_element_type=jnp.float32)


def dot_nn(a, b):
    return lax.dot_general(a, b, (((1,), (0,)), ((), ())), preferred_element_type=jnp.float32)


def fold8(x):
    return jnp.sum(x.reshape(x.shape[0] // 8, 8, x.shape[1]), axis=0)


def flip(me, bit):
    return me + bit - 2 * bit * lax.rem(me // bit, 2)


def send(src, dst, ssem, rsem, to):
    copy = pltpu.make_async_remote_copy(src_ref=src, dst_ref=dst, send_sem=ssem, recv_sem=rsem,
                                        device_id=to, device_id_type=LOGICAL)
    copy.start()


def drain(ref, sem):
    pltpu.make_async_copy(ref, ref, sem).wait()


def kernel(z1, z2, zs, mask, protos, dc, qs, qt, dz, loss,
           ca, ex, mrows, slots, lslots, wall, zall, arow, brow, gt, xsc, gr, zt, px, zl, cols, acc, mv,
           insem, msem, csem, zsend, zlrecv, zs1recv, zs2send, zs2recv, arsend, arrecv, lsend, lrecv, wsend, wrecv,
           ssem, r2, r3, rs):
    me = lax.axis_index("data")
    barrier = pltpu.get_barrier_semaphore()
    for d in PEERS:
        pl.semaphore_signal(barrier, inc=1, device_id=lax.rem(me + d, NDEV), device_id_type=LOGICAL)
    myrows = pl.ds(pl.multiple_of(me * ROWS, ROWS), ROWS)
    ins = [pltpu.make_async_copy(src, dst, insem.at[i]) for i, (src, dst) in enumerate((
        (mask, mv), (z1, zall.at[0, myrows]), (z2, zall.at[1, myrows]), (zs, zall.at[CROPS, myrows])))]
    for c in ins:
        c.start()
    cc = pltpu.make_async_copy(protos, ca.at[pl.ds(0, KP)], csem)
    cc.start()
    dims = (flip(me, 2), flip(me, 4), flip(me, 8))
    sib = flip(me, 1)
    ins[0].wait()
    mpad = jnp.concatenate([mv[...].astype(jnp.float32), jnp.zeros((1, LANE - ROWS), jnp.float32)], axis=1)
    mrows[me] = pltpu.roll(jnp.broadcast_to(mpad, (8, LANE)), ROWS * lax.rem(me, 4), 1)[0:1]
    for c in ins[1:]:
        c.wait()
    with jax.named_scope("barrier"):
        pl.semaphore_wait(barrier, OTHERS)

    def ar_send(t):
        for d in PEERS:
            send(slots.at[t, me], slots.at[t, me], arsend.at[t], arrecv.at[t], lax.rem(me + d, NDEV))

    def ar_total(t):
        drain(slots.at[t, pl.ds(0, OTHERS)], arrecv.at[t])
        tot = slots[t, 0]
        for i in PEERS:
            tot = tot + slots[t, i]
        return tot

    for d in PEERS:
        send(zall.at[0, myrows], zall.at[0, myrows], zsend.at[0], zlrecv.at[0], lax.rem(me + d, NDEV))
    for d in PEERS:
        send(mrows.at[me], mrows.at[me], msem.at[0], msem.at[1], lax.rem(me + d, NDEV))
    for d in PEERS:
        send(zall.at[1, myrows], zall.at[1, myrows], zsend.at[1], zlrecv.at[1], lax.rem(me + d, NDEV))
    for d in PEERS_HALF:
        send(zall.at[CROPS, myrows], zall.at[CROPS, myrows], zsend.at[2], zs1recv, lax.rem(me + 2 * d, NDEV))
    send(zall.at[CROPS, myrows], zall.at[CROPS, myrows], zs2send, zs2recv, sib)
    zl[pl.ds(0, ROWS), pl.ds(0, D)] = zall[0, myrows]
    zl[pl.ds(ROWS, ROWS), pl.ds(0, D)] = zall[1, myrows]
    zl[pl.ds(2 * ROWS, 6 * ROWS), pl.ds(0, D)] = zall[CROPS, myrows].reshape(6 * ROWS, D)
    zl[pl.ds(0, 2 * ROWS), pl.ds(D, LANE)] = jnp.zeros((2 * ROWS, LANE), jnp.bfloat16)
    ca[pl.ds(KP, KPAD - KP), :] = jnp.zeros((KPAD - KP, D), jnp.bfloat16)
    acc[...] = jnp.zeros_like(acc)
    cc.wait()
    with jax.named_scope("mask"):
        drain(mrows.at[pl.ds(0, OTHERS)], msem.at[1])
        mask8 = [mrows[4 * j] + mrows[4 * j + 1] + mrows[4 * j + 2] + mrows[4 * j + 3] for j in range(4)]
    mask4 = jnp.concatenate(mask8, axis=0)
    mrow = jnp.concatenate(mask8, axis=1)
    live = jnp.sum(jnp.sum(mask4, axis=1, keepdims=True), axis=0, keepdims=True)

    def zwait(v):
        with jax.named_scope("zlarge"):
            drain(zall.at[0, pl.ds(0, NS - ROWS)], zlrecv.at[v])

    def shard(b):
        return ca[pl.ds(pl.multiple_of(me * SH + b * CB, LANE), CB)]

    def col_scale(c, b):
        k = me * SH + b * CB + lax.broadcasted_iota(jnp.int32, (CB, 1), 0)
        return jnp.where(k < KP, 1.0 / (KP * c), 0.0)

    zero8 = jnp.zeros((8, NS), jnp.float32)

    def first(v):
        ps, r = zero8, zero8
        for b in range(NCH):
            p = jnp.exp2(dot_nt(shard(b), zall[v]) * SCALE)
            ps = ps + fold8(p)
            e = p * p * mrow
            ex[v, pl.ds(b * CB, CB)] = e
            w = col_scale(jnp.sum(e, axis=1, keepdims=True), b)
            r = r + fold8(e * w)
        return ps, r

    def put(t, r):
        row = jnp.sum(r, axis=0, keepdims=True)
        for j in range(4):
            slots[t, me, pl.ds(j, 1)] = row[:, LANE * j:LANE * (j + 1)]

    def scale_row(tot):
        r = jnp.concatenate([tot[j:j + 1] for j in range(4)], axis=1)
        return mrow / (live * jnp.where(mrow > 0, r, 1.0))

    pad = jnp.where(me == OTHERS, float(SH - LAST), 0.0)

    def put_lse(v, ps):
        row = jnp.sum(ps, axis=0, keepdims=True) - pad
        for j in range(4):
            lslots[me, pl.ds(4 * v + j, 1)] = row[:, LANE * j:LANE * (j + 1)]

    def lse_send(k):
        ref = lslots.at[me, pl.ds(8 * k, 8)]
        for d in PEERS:
            send(ref, ref, lsend.at[k], lrecv.at[k], lax.rem(me + d, NDEV))

    for v in range(2):
        zwait(v)
        with jax.named_scope("first"):
            ps, r = first(v)
            put(v, r)
            ar_send(v)
        put_lse(v, ps)
    lse_send(0)
    with jax.named_scope("zsmall1"):
        drain(zall.at[CROPS, pl.ds(0, 7 * ROWS)], zs1recv)
    for d in PEERS_HALF:
        rows = pl.ds(pl.multiple_of(lax.rem(me + 2 * d, NDEV) * ROWS, ROWS), ROWS)
        send(zall.at[CROPS, rows], zall.at[CROPS, rows], zs2send, zs2recv, sib)

    def small(i, carry):
        v = 2 + i
        ps = zero8
        for b in range(NCH):
            ps = ps + fold8(jnp.exp2(dot_nt(shard(b), zall[v]) * SCALE))
        put_lse(v, ps)
        return carry

    def again(v, t):
        with jax.named_scope("ar%d" % t):
            u = scale_row(ar_total(t - 2))
        last = t > 3

        def step(b, r):
            rows = pl.ds(pl.multiple_of(b * CB, CB), CB)
            e = ex[v, rows]
            w = col_scale(jnp.sum(e * u, axis=1, keepdims=True), b)
            if last:
                for q in range(CB // LANE):
                    wt = jnp.broadcast_to(w[LANE * q:LANE * (q + 1)], (LANE, LANE)).T
                    wall[me, pl.ds(v, 1), pl.ds(pl.multiple_of(b * CB + LANE * q, LANE), LANE)] = wt[0:1]
            return r + fold8(e * w)

        with jax.named_scope("again%d" % t):
            put(t, lax.fori_loop(0, NCH, step, zero8))
            ar_send(t)

    again(0, 2)
    again(1, 3)
    with jax.named_scope("zsmall2"):
        drain(zall.at[CROPS, pl.ds(0, 8 * ROWS)], zs2recv)
    with jax.named_scope("small"):
        for k in range(1, 4):
            lax.fori_loop(2 * k - 2, 2 * k, small, 0)
            lse_send(k)
    again(0, 4)
    again(1, 5)
    for d in PEERS:
        send(wall.at[me], wall.at[me], wsend, wrecv, lax.rem(me + d, NDEV))
    gsc = 1.0 / (TAU * PAIRS * live)
    with jax.named_scope("lse"):
        for k in range(4):
            drain(lslots.at[pl.ds(0, OTHERS), pl.ds(0, 8)], lrecv.at[k])
        tot = lslots[0]
        for i in PEERS:
            tot = tot + lslots[i]
        logs = jnp.log(tot)
        inv = 1.0 / tot[0:8]
        for v in range(2):
            for j in range(4):
                arow[v:v + 1, LANE * j:LANE * (j + 1)] = gsc * (mask8[j] * inv[4 * v + j:4 * v + j + 1])
        lg2 = jnp.log(2.0 * gsc)
        lsum = jnp.sum(jnp.sum(jnp.concatenate([mask4] * 2, axis=0) * logs[0:8], axis=1, keepdims=True), axis=0, keepdims=True)
        lsum = lsum + (12.0 * live) * lg2
        rest_ = jnp.where(jnp.concatenate([mask4] * 8, axis=0) > 0, TAU * (lg2 - logs), -100.0)
        for k in range(3):
            piece_ = rest_.astype(jnp.bfloat16).astype(jnp.float32)
            px[k] = piece_
            rest_ = rest_ - piece_
        for j in range(4):
            block = jnp.concatenate([px[k, pl.ds(8 + j, 6, 4)] for k in range(3)] + [jnp.zeros((110, LANE), jnp.float32)], axis=0)
            zt[pl.ds(LANE * j, LANE)] = block.T.astype(jnp.bfloat16)
        lane = lax.broadcasted_iota(jnp.int32, (ROWS, LANE), 1)
        own_rows = zt[myrows].astype(jnp.float32)
        for v in SMALL:
            pick = jnp.where(jnp.logical_and(lax.rem(lane, 6) == v - 2, lane < 18), own_rows, 0.0)
            zl[pl.ds(v * ROWS, ROWS), pl.ds(D, LANE)] = pick.astype(jnp.bfloat16)
    def probs(c, v):
        if v < 2:
            return dot_nt(c, zall[v])
        lanes = lax.broadcasted_iota(jnp.int32, (CB, LANE), 1)
        sel = jnp.where(jnp.logical_and(lax.rem(lanes, 6) == v - 2, lanes < 18), 1.0, 0.0).astype(jnp.bfloat16)
        return dot_nt(jnp.concatenate([c, sel], axis=1), jnp.concatenate([zall[v], zt[...]], axis=1))

    with jax.named_scope("ahead"):
        for v in range(VIEWS):
            ex[v % 2, pl.ds(v // 2 * CB, CB)] = jnp.exp2(probs(shard(0), v) * SCALE)
    with jax.named_scope("ar3"):
        us = [scale_row(ar_total(4)), scale_row(ar_total(5))]
    for v in range(2):
        brow[v:v + 1] = live * us[v]
    brow[2:8] = jnp.zeros((6, NS), jnp.float32)
    arow[2:8] = jnp.zeros((6, NS), jnp.float32)
    tile = pl.ds(pl.multiple_of((me // 4) * LANE, LANE), LANE)
    cols[0] = arow[:, tile].T
    cols[1] = brow[:, tile].T
    mine = pl.ds(pl.multiple_of(lax.rem(me, 4) * ROWS, ROWS), ROWS)

    def piece_row(owner, t, a):
        return pl.multiple_of(owner * SH + t * CB + a * LANE, LANE)

    def parts_of(it):
        quad = (it + 8 - N2) // 8
        t = (1 - quad) * (it // 2) + quad * (NCH - NQ + (it - N2) // 4)
        par = (1 - quad) * lax.rem(it, 2) + quad * lax.rem(it + 4 - N2 % 4, 4)
        return t, par

    def push(owner, it, a, to, rsem):
        ref = dc.at[pl.ds(piece_row(owner, parts_of(it)[0], a), LANE)]
        send(ref, ref, ssem.at[it, a], rsem.at[it, a], to)

    def order(a):
        return dims[a], dims[(a + 1) % 3], dims[(a + 2) % 3]

    def owner_of(holder, a, it):
        d0, d1, _ = order(a)
        par = parts_of(it)[1]
        return holder + lax.rem(par, 2) * (d0 - me) + (par // 2) * (d1 - me)

    def chunk(it, ready=False):
        t = parts_of(it)[0]
        owners = [owner_of(me, a, it) for a in range(3)]
        c = jnp.concatenate([ca[pl.ds(piece_row(owners[a], t, a), LANE)] for a in range(3)], axis=0)
        wc = []
        for v in range(2):
            parts = []
            for a in range(3):
                off = pl.multiple_of(t * CB + a * LANE, LANE)
                row = wall[owners[a], pl.ds(v, 1), pl.ds(off, LANE)] * gsc
                parts.append(jnp.broadcast_to(row, (LANE, LANE)).T)
            wc.append(jnp.concatenate(parts, axis=0))
        HALF = CB // 2

        def prob_at(s, v, q, l):
            if ready:
                return ex[v % 2, pl.ds(v // 2 * CB + QR * q, QR), pl.ds(LW * l, LW)]
            return jnp.exp2(s[QR * q:QR * (q + 1), LW * l:LW * (l + 1)] * SCALE)

        def put_g(v, q, l, g):
            gt[v // 4, pl.ds(QR * q, QR), pl.ds((v % 4) * NS + LW * l, LW)] = g.astype(jnp.bfloat16)

        def dc_part(h):
            zz = zall[pl.ds(4 * h, 4)].reshape(4 * NS, D)
            return [dot_nn(gt[h, pl.ds(HALF * m, HALF)], zz) for m in range(2)]

        def rows_of(ref, v, l):
            return ref[v:v + 1, LW * l:LW * (l + 1)]

        e0 = probs(c, 0) if not ready else None
        e1 = probs(c, 1) if not ready else None
        for l in range(NS // LW):
            b0, b1, a0, a1 = rows_of(brow, 0, l), rows_of(brow, 1, l), rows_of(arow, 0, l), rows_of(arow, 1, l)
            for q in range(CB // QR):
                sl = slice(QR * q, QR * (q + 1))
                p0 = prob_at(e0, 0, q, l)
                p1 = prob_at(e1, 1, q, l)
                x0 = (p0 * p0) * b0 * jnp.concatenate([wc[0][sl]] * 2, axis=1)
                x1 = (p1 * p1) * b1 * jnp.concatenate([wc[1][sl]] * 2, axis=1)
                xsc[pl.ds(QR * q, QR), pl.ds(LW * l, LW)] = x0 + x1
                put_g(0, q, l, p0 * a0 - x1)
                put_g(1, q, l, p1 * a1 - x0)
        res = None
        for v in SMALL:
            e = probs(c, v) if not ready else None
            for l in range(NS // LW):
                for q in range(CB // QR):
                    put_g(v, q, l, prob_at(e, v, q, l) - xsc[pl.ds(QR * q, QR), pl.ds(LW * l, LW)])
            if v == 3:
                res = dc_part(0)
        more = dc_part(1)
        out = jnp.concatenate([res[0] + more[0], res[1] + more[1]], axis=0)
        for a in range(3):
            dc[pl.ds(piece_row(owners[a], t, a), LANE)] = out[LANE * a:LANE * (a + 1)]

    def rows_part(i):
        ac = cols[0, mine]
        bc = cols[1, mine]
        lanes = lax.broadcasted_iota(jnp.int32, (RB, LANE), 1)
        ones = jnp.where(lanes < 18, 1.0, 0.0).astype(jnp.bfloat16)
        for h in range(RPI):
            jb = i * RPI + h
            c = ca[pl.ds(pl.multiple_of(jb * RB, RB), RB)]
            s = dot_nt(zl[...], jnp.concatenate([c, ones], axis=1)) * SCALE
            wr = []
            for v in range(2):
                parts = []
                for q in range(RB // LANE):
                    b = jb * (RB // LANE) + q
                    parts.append(wall[b // (SH // LANE), pl.ds(v, 1), pl.ds(pl.multiple_of(lax.rem(b, SH // LANE) * LANE, LANE), LANE)])
                wr.append(jnp.concatenate(parts, axis=1))
            sv = [s[ROWS * v:ROWS * (v + 1)] for v in range(VIEWS)]
            p0 = jnp.exp2(sv[0])
            p1 = jnp.exp2(sv[1])
            o0 = (p0 * p0) * bc[:, 0:1] * wr[0]
            o1 = (p1 * p1) * bc[:, 1:2] * wr[1]
            col = pl.ds(h * RB, RB)
            qs[i, 0, :, col] = o0
            qs[i, 1, :, col] = o1
            x0 = o0 * gsc
            x1 = o1 * gsc
            xs = x0 + x1
            gr[pl.ds(0, ROWS), col] = (p0 * ac[:, 0:1] - x1).astype(jnp.bfloat16)
            gr[pl.ds(ROWS, ROWS), col] = (p1 * ac[:, 1:2] - x0).astype(jnp.bfloat16)
            ssum = sv[2]
            for v in range(3, VIEWS):
                ssum = ssum + sv[v]
            for v in SMALL:
                gr[pl.ds(v * ROWS, ROWS), col] = (jnp.exp2(sv[v]) - xs).astype(jnp.bfloat16)
            ls = x1 * sv[0] + x0 * sv[1] + xs * ssum
            part = ls[:, 0:LANE]
            for q in range(1, RB // LANE):
                part = part + ls[:, LANE * q:LANE * (q + 1)]
            acc[pl.ds(VIEWS * ROWS, ROWS)] += part
        cs = ca[pl.ds(pl.multiple_of(i * RW, RW), RW)]
        acc[pl.ds(0, VIEWS * ROWS)] += dot_nn(gr[...], cs)

    def own(it):
        for a in range(3):
            o = owner_of(me, a, it)
            push(o, it, a, order(a)[2], r3)
            push(o, it, a, sib, rs)

    def own1(it):
        for a in range(3):
            push(owner_of(me, a, it), it, a, order(a)[1], r2)

    def serve2(it):
        for a in range(3):
            d0, d1, d2 = order(a)
            drain(dc.at[pl.ds(0, LANE)], r2.at[it, a])
            o = owner_of(d1, a, it)
            push(o, it, a, d2, r3)
            push(o, it, a, sib, rs)

    def serve3(it):
        @pl.when(it < N2)
        def _():
            for a in range(3):
                d0, d1, d2 = order(a)
                drain(dc.at[pl.ds(0, 256)], r3.at[it, a])
                for holder in (d2, d2 + d1 - me):
                    push(owner_of(holder, a, it), it, a, sib, rs)

        @pl.when(it >= N2)
        def _():
            for a in range(3):
                drain(dc.at[pl.ds(0, LANE)], r3.at[it, a])
                push(owner_of(order(a)[2], a, it), it, a, sib, rs)

    with jax.named_scope("chunk0"):
        chunk(0, ready=True)
    own1(0)
    own(0)
    with jax.named_scope("wait_w"):
        drain(wall.at[pl.ds(0, OTHERS)], wrecv)

    def main(it, with_rows):
        with jax.named_scope("compute"):
            chunk(it)
            if with_rows:
                rows_part(it - ALONE)

        @pl.when(it < N2)
        def _():
            own1(it)

        own(it)

        @pl.when(jnp.logical_and(it >= LAG2, it < LAG2 + N2))
        def _():
            with jax.named_scope("serve2"):
                serve2(it - LAG2)

        @pl.when(it >= LAG3)
        def _():
            with jax.named_scope("serve3"):
                serve3(it - LAG3)

    def main_alone(it, carry):
        main(it, False)
        return carry

    def main_rows(it, carry):
        main(it, True)
        return carry

    lax.fori_loop(1, ALONE, main_alone, 0)
    lax.fori_loop(ALONE, STEPS, main_rows, 0)

    def rest(i, carry):
        with jax.named_scope("rows"):
            rows_part(i)
        return carry

    lax.fori_loop(STEPS - ALONE, PARTS, rest, 0)
    total = jnp.sum(jnp.sum(acc[pl.ds(VIEWS * ROWS, ROWS)], axis=1, keepdims=True), axis=0, keepdims=True)
    slots[6, me] = jnp.broadcast_to(total, (4, LANE))
    ar_send(6)
    for v in range(2):
        qt[v] = qs[PARTS - 1, v, :, pl.ds(0, QT)]

    def last(it, carry):
        with jax.named_scope("serve3"):
            serve3(it)
        return carry

    lax.fori_loop(STEPS - LAG3, STEPS, last, 0)
    dz[...] = acc[pl.ds(0, VIEWS * ROWS)].reshape(VIEWS, ROWS, D)
    with jax.named_scope("loss"):
        tot = ar_total(6)
    cross = tot[0:1, 0:1] * (LN2 * TAU * PAIRS) * live - lsum
    loss[...] = -cross / (live * PAIRS)

    def finish(it, carry):
        @pl.when(it < N2)
        def _():
            for a in range(3):
                drain(dc.at[pl.ds(0, 4 * LANE)], rs.at[it, a])
                drain(dc.at[pl.ds(0, 7 * LANE)], ssem.at[it, a])

        @pl.when(it >= N2)
        def _():
            for a in range(3):
                drain(dc.at[pl.ds(0, 2 * LANE)], rs.at[it, a])
                drain(dc.at[pl.ds(0, 3 * LANE)], ssem.at[it, a])
        return carry

    with jax.named_scope("finish"):
        lax.fori_loop(0, STEPS, finish, 0)
    for v in range(2):
        drain(zall.at[0, pl.ds(0, NS - ROWS)], zsend.at[v])
    drain(zall.at[CROPS, pl.ds(0, 7 * ROWS)], zsend.at[2])
    drain(zall.at[CROPS, pl.ds(0, 8 * ROWS)], zs2send)
    drain(mrows.at[pl.ds(0, OTHERS)], msem.at[0])
    for t in range(7):
        drain(slots.at[t, pl.ds(0, OTHERS)], arsend.at[t])
    for k in range(4):
        drain(lslots.at[pl.ds(0, OTHERS), pl.ds(0, 8)], lsend.at[k])
    drain(wall.at[pl.ds(0, OTHERS)], wsend)


def emit_kernel(dc, qs, qt, dz, loss, o_q1, o_q2, o_loss, o_z1, o_z2, o_zs, o_dc, sem):
    pairs = []
    for i in range(PARTS):
        for v, o in enumerate((o_q1, o_q2)):
            if i < PARTS - 1:
                pairs.append((qs.at[i, v], o.at[:, pl.ds(i * RW, RW)]))
            else:
                pairs.append((qt.at[v], o.at[:, pl.ds(i * RW, QT)]))
        rows = pl.ds(i * RW, RW if i < PARTS - 1 else QT)
        pairs.append((dc.at[rows], o_dc.at[rows]))
    pairs += [(loss, o_loss), (dz.at[0], o_z1), (dz.at[1], o_z2), (dz.at[CROPS], o_zs)]
    copies = [pltpu.make_async_copy(a, b, sem.at[i]) for i, (a, b) in enumerate(pairs)]
    for c in copies:
        c.start()
    for c in copies:
        c.wait()


def local_step(z_one, z_two, z_small, protos, live_mask):
    f32 = jnp.float32
    bf16 = jnp.bfloat16
    vmem = pl.BlockSpec(memory_space=pltpu.VMEM)
    anym = pl.BlockSpec(memory_space=pl.ANY)
    dma = pltpu.SemaphoreType.DMA
    vm = pltpu.VMEM
    dc, qs, qt, dz, loss = pl.pallas_call(
        kernel,
        out_shape=[vm((KPAD, D), f32), vm((PARTS, 2, ROWS, RW), f32), vm((2, ROWS, QT), f32),
                   vm((VIEWS, ROWS, D), f32), vm((1, 1), f32)],
        in_specs=[anym] * 5,
        out_specs=[vmem] * 5,
        scratch_shapes=[vm((KPAD, D), bf16), vm((2, SH, NS), f32), vm((NDEV, 1, LANE), f32), vm((7, NDEV, 4, LANE), f32), vm((NDEV, 32, LANE), f32),
                        vm((NDEV, 2, SH), f32), vm((VIEWS, NS, D), bf16), vm((8, NS), f32), vm((8, NS), f32),
                        vm((2, CB, 4 * NS), bf16), vm((CB, NS), f32),
                        vm((VIEWS * ROWS, RW), bf16), vm((NS, LANE), bf16), vm((3, 32, LANE), f32), vm((VIEWS * ROWS, 2 * D), bf16),
                        vm((2, LANE, 8), f32),
                        vm((VIEWS * ROWS + ROWS, D), f32),
                        vm((1, ROWS), jnp.int32),
                        dma((4,)), dma((2,)), dma, dma((3,)), dma((2,)), dma, dma, dma, dma((7,)), dma((7,)), dma((4,)), dma((4,)), dma, dma,
                        dma((STEPS, 3)), dma((STEPS, 3)), dma((STEPS, 3)), dma((STEPS, 3))],
        compiler_params=pltpu.CompilerParams(collective_id=0, has_side_effects=True, vmem_limit_bytes=VM),
        name="step",
    )(z_one, z_two, z_small, live_mask.reshape(1, ROWS), protos)
    q1, q2, loss, dz1, dz2, dzs, dc = pl.pallas_call(
        emit_kernel,
        out_shape=[jax.ShapeDtypeStruct((ROWS, KP), f32), jax.ShapeDtypeStruct((ROWS, KP), f32),
                   jax.ShapeDtypeStruct((1, 1), f32), jax.ShapeDtypeStruct((ROWS, D), f32),
                   jax.ShapeDtypeStruct((ROWS, D), f32), jax.ShapeDtypeStruct((6, ROWS, D), f32),
                   jax.ShapeDtypeStruct((KP, D), f32)],
        in_specs=[vmem] * 5,
        out_specs=[anym] * 7,
        scratch_shapes=[dma((3 * PARTS + 4,))],
        compiler_params=pltpu.CompilerParams(vmem_limit_bytes=1024 * 1024),
        name="emit",
    )(dc, qs, qt, dz, loss)
    return q1, q2, loss.reshape(()), dz1, dz2, dzs, dc


def solution(mesh):
    row_spec = P("data", None)
    crop_spec = P(None, "data", None)
    return jax.shard_map(local_step, mesh=mesh,
                         in_specs=(row_spec, row_spec, crop_spec, P(None, None), P("data")),
                         out_specs=(row_spec, row_spec, P(), row_spec, row_spec, crop_spec, P(None, None)),
                         check_vma=False)
```
